8 devices in a mesh: dp: 1 (over z), ff: 2 (over y), hd: 4 (over x, core).
Axes of the slice: x: 2, y: 2, z: 1, core: 2. Of those that a mesh axis runs over, the one named last changes fastest.
Arguments:
- x_in: bfloat16 [128, 4096], P('dp', 'hd')
- w_up: bfloat16 [4096, 20480], P('hd', 'ff')
- b_up: float32 [20480], P('ff')
- w_down: bfloat16 [10240, 4096], P('ff', 'hd')
- b_down: float32 [4096], P('hd')
- ln_gain: float32 [4096], P('hd')
- ln_bias: float32 [4096], P('hd')
- dy_in: bfloat16 [128, 4096], P('dp', 'hd')
Outputs:
- output 1: bfloat16 [128, 4096], P('dp', 'hd')
- output 2: bfloat16 [128, 4096], P('dp', 'hd')
- output 3: float32 [4096, 20480], P(('dp', 'hd'), 'ff')
- output 4: float32 [10240, 4096], P(('dp', 'ff'), 'hd')
- output 5: float32 [20480], P(('dp', 'ff'))
- output 6: float32 [4096], P(('dp', 'hd'))
- output 7: float32 [4096], P(('dp', 'hd'))
- output 8: float32 [4096], P(('dp', 'hd'))
All inputs are finite; a program needn't handle non-finite values.
Results may differ from the reference program's by a relative error of at most 0.0181239.
Values are sent between devices in bfloat16 or wider.
A program may use at most 1 GiB of HBM per device.

```python
import math
import jax
import jax.numpy as jnp
from jax import lax

TOKENS = 128
HIDDEN = 4096
FFN = 10240
PAIR = 128
COARSE = 16
ALPHA = math.sqrt(140.0)
LN_EPS = 1e-5


def setup_inputs(seed: int = 0, part: int = 0) -> dict:
    part_keys = jax.random.split(jax.random.fold_in(jax.random.key(seed), part), 7)
    shared_keys = jax.random.split(jax.random.key(seed + 1), 6)
    seg_width = HIDDEN // COARSE
    row_shift = 0.7 * jax.random.normal(part_keys[0], (TOKENS, 1, 1), jnp.float32)
    seg_shift = 0.8 * jax.random.normal(part_keys[1], (1, COARSE, 1), jnp.float32)
    seg_scale = jnp.exp(0.4 * jax.random.normal(part_keys[2], (1, COARSE, 1), jnp.float32))
    x_noise = jax.random.normal(part_keys[3], (TOKENS, COARSE, seg_width), jnp.float32)
    x_vals = (row_shift + seg_shift + seg_scale * x_noise).reshape(TOKENS, HIDDEN)
    dy_noise = jax.random.normal(part_keys[4], (TOKENS, COARSE, seg_width), jnp.float32)
    dy_shift = 0.8 * jax.random.normal(part_keys[5], (TOKENS, 1, 1), jnp.float32)
    dy_tilt = jax.random.normal(part_keys[6], (TOKENS, 1, 1), jnp.float32)
    dy_vals = (dy_noise + dy_shift + dy_tilt * seg_shift).reshape(TOKENS, HIDDEN)
    w_up = jax.random.normal(shared_keys[0], (HIDDEN, 2 * FFN), jnp.float32) * HIDDEN ** -0.5
    b_up = 0.5 * jax.random.normal(shared_keys[1], (2 * FFN,), jnp.float32)
    w_down = jax.random.normal(shared_keys[2], (FFN, HIDDEN), jnp.float32) * (ALPHA * FFN ** -0.5)
    b_down = 3.0 * jax.random.normal(shared_keys[3], (HIDDEN,), jnp.float32)
    ln_gain = 1.0 + 0.3 * jax.random.normal(shared_keys[4], (HIDDEN,), jnp.float32)
    ln_bias = 0.3 * jax.random.normal(shared_keys[5], (HIDDEN,), jnp.float32)
    return {'x_in': x_vals.astype(jnp.bfloat16), 'w_up': w_up.astype(jnp.bfloat16), 'b_up': b_up, 'w_down': w_down.astype(jnp.bfloat16), 'b_down': b_down, 'ln_gain': ln_gain, 'ln_bias': ln_bias, 'dy_in': dy_vals.astype(jnp.bfloat16)}


def gelu_tanh(z_val):
    return jax.nn.gelu(z_val, approximate=True)


def reference(x_in, w_up, b_up, w_down, b_down, ln_gain, ln_bias, dy_in):
    n_blocks = FFN // PAIR
    u_acc = jnp.dot(x_in, w_up, preferred_element_type=jnp.float32) + b_up
    u_act = u_acc.astype(jnp.bfloat16).reshape(TOKENS, n_blocks, 2, PAIR)
    val_half = u_act[:, :, 0, :].astype(jnp.float32)
    gate_half = u_act[:, :, 1, :].astype(jnp.float32)
    gelu_out, gelu_vjp = jax.vjp(gelu_tanh, gate_half)
    m_act = (val_half * gelu_out).astype(jnp.bfloat16).reshape(TOKENS, FFN)
    f_out = jnp.dot(m_act, w_down, preferred_element_type=jnp.float32)
    residual = ALPHA * x_in.astype(jnp.float32) + f_out + b_down
    row_mean = jnp.mean(residual, axis=1, keepdims=True)
    centered = residual - row_mean
    row_var = jnp.mean(centered * centered, axis=1, keepdims=True)
    inv_std = lax.rsqrt(row_var + LN_EPS)
    normed = centered * inv_std
    y_out = (ln_gain * normed + ln_bias).astype(jnp.bfloat16)
    dy_f = dy_in.astype(jnp.float32)
    g_dy = dy_f * ln_gain
    d_resid = inv_std * (g_dy - jnp.mean(g_dy, axis=1, keepdims=True) - normed * jnp.mean(g_dy * normed, axis=1, keepdims=True))
    dr_b = d_resid.astype(jnp.bfloat16)
    d_mact = jnp.dot(dr_b, w_down.T, preferred_element_type=jnp.float32).reshape(TOKENS, n_blocks, PAIR)
    d_val = d_mact * gelu_out
    d_gate = gelu_vjp(d_mact * val_half)[0]
    du_f = jnp.stack([d_val, d_gate], axis=2).reshape(TOKENS, 2 * FFN)
    du_b = du_f.astype(jnp.bfloat16)
    dw_up = jnp.dot(x_in.T, du_b, preferred_element_type=jnp.float32)
    dw_down = jnp.dot(m_act.T, dr_b, preferred_element_type=jnp.float32)
    dx_out = (ALPHA * d_resid + jnp.dot(du_b, w_up.T, preferred_element_type=jnp.float32)).astype(jnp.bfloat16)
    return (y_out, dx_out, dw_up, dw_down, jnp.sum(du_f, axis=0), jnp.sum(d_resid, axis=0), jnp.sum(dy_f * normed, axis=0), jnp.sum(dy_f, axis=0))
```

```python
import functools
import math
import jax
import jax.numpy as jnp
from jax import lax
from jax.experimental import pallas as pl
from jax.experimental.pallas import tpu as pltpu
from jax.sharding import PartitionSpec as P

PAIR = 128
ALPHA = math.sqrt(140.0)
LN_EPS = 1e-5
C0 = math.sqrt(2.0 / math.pi)
C1 = 0.044715
MESH = pl.DeviceIdType.MESH
F32 = jnp.float32
BF = jnp.bfloat16
T = 128
H = 1024
NC = 5
Q = 256
S = 2
VLIM = 62 * 1024 * 1024

VMEM = pl.BlockSpec(memory_space=pltpu.VMEM)
ANY = pl.BlockSpec(memory_space=pl.ANY)


def sds(shape, dtype):
    return jax.ShapeDtypeStruct(shape, dtype)


def dot(a, b):
    return jnp.dot(a, b, preferred_element_type=F32)


def dot_t(a, b):
    return lax.dot_general(a, b, (((1,), (1,)), ((), ())), preferred_element_type=F32)


def split_u(u):
    v = jnp.concatenate([u[:, 0:128], u[:, 256:384]], axis=1)
    g = jnp.concatenate([u[:, 128:256], u[:, 384:512]], axis=1)
    return v, g


def gelu(g):
    t = jnp.tanh(C0 * (g + C1 * (g * g * g)))
    return g * (0.5 * (1.0 + t))


def gelu_both(g):
    g2 = g * g
    t = jnp.tanh(C0 * (g + C1 * (g2 * g)))
    cdf = 0.5 * (1.0 + t)
    slope = cdf + (0.5 * g) * (1.0 - t * t) * (C0 * (1.0 + (3.0 * C1) * g2))
    return g * cdf, slope


def grad_u(u, dm):
    v, g = split_u(u.astype(F32))
    val, slope = gelu_both(g)
    dv = dm * val
    dg = dm * v * slope
    return jnp.concatenate([dv[:, 0:128], dg[:, 0:128], dv[:, 128:256], dg[:, 128:256]], axis=1)


def places():
    h = lax.axis_index("hd")
    y = lax.axis_index("ff")
    c = lax.rem(h, 2)
    sib = h + 1 - 2 * c
    xn = lax.rem(h + 2, 4)
    xs = lax.rem(sib + 2, 4)
    return h, y, c, sib, xn, xs


def remote(src, dst, sems, k, dev):
    return pltpu.make_async_remote_copy(src_ref=src, dst_ref=dst, send_sem=sems[0].at[k], recv_sem=sems[1].at[k],
                                        device_id=dev, device_id_type=MESH)


def w1_cols(w1_ref, j, q):
    return w1_ref.at[:, pl.ds(pl.multiple_of(j * 4 * 512 + q * 512, 512), 512)]


N_SEM = {"ud": 2 * NC, "ux": NC, "mx": NC, "md": NC, "mf": NC, "gx": NC, "gd": NC, "gf": NC, "fy": 2, "st": 3,
         "dd": 2 * NC, "dx": NC, "df": 2 * NC}
SEM_NAMES = list(N_SEM)


def forward_kernel(x_ref, w1_ref, b1_ref, w2_ref, b2_ref, gam_ref, dy_ref,
                   m_ref, u_ref, d_ref, dr_ref, nrm_ref, dmf_ref, dms_ref,
                   w1b, w2b, ub, rb, xsb, xrb, facc, fs, fr, stb, dmb, dmr, dsum, dxr,
                   ls1, ls2, *sem_list):
    sems = {n: (sem_list[2 * i], sem_list[2 * i + 1]) for i, n in enumerate(SEM_NAMES)}
    h, y, c, sib, xn, xs = places()
    dev_sib, dev_x, dev_xs, dev_y = (0, y, sib), (0, y, xn), (0, y, xs), (0, 1 - y, h)
    order = [xs, xn, sib, h]
    for j in range(NC):
        for k in range(4):
            pltpu.make_async_copy(w1_cols(w1_ref, j, order[k]), w1b.at[j, k], ls1.at[j, k]).start()
    for j in range(NC):
        pltpu.make_async_copy(w2_ref.at[j * 1024:(j + 1) * 1024, :], w2b.at[j], ls2.at[j]).start()
    bar = pltpu.get_barrier_semaphore()
    for dev in (dev_sib, dev_x, dev_xs, dev_y):
        pl.semaphore_signal(bar, inc=1, device_id=dev, device_id_type=MESH)
    pl.semaphore_wait(bar, 4)

    live = []

    def send(src, dst, name, k, dev):
        cp = remote(src, dst, sems[name], k, dev)
        cp.start()
        live.append(cp)
        return cp

    def u_part(j):
        for k in range(4):
            pltpu.make_async_copy(w1_cols(w1_ref, j, order[k]), w1b.at[j, k], ls1.at[j, k]).wait()
            ub[j, k] = dot(x_ref[...], w1b[j, k]).astype(BF)
            if k == 0:
                c_ud[j, 1] = send(ub.at[j, 0], rb.at[j, 1], "ud", 2 * j + 1, dev_sib)
            if k == 2:
                c_ud[j, 0] = send(ub.at[j, 2], rb.at[j, 0], "ud", 2 * j, dev_sib)

    def s1(j):
        c_ud[j, 1].wait_recv()
        xsb[j] = (ub[j, 1].astype(F32) + rb[j, 1].astype(F32)).astype(BF)
        c_ux[j] = send(xsb.at[j], xrb.at[j], "ux", j, dev_x)

    def s2(j):
        c_ud[j, 0].wait_recv()
        c_ux[j].wait_recv()
        u = ub[j, 3].astype(F32) + rb[j, 0].astype(F32) + xrb[j].astype(F32) + b1_ref[j * 4 + h]
        u = u.astype(BF)
        u_ref[j, h] = u
        v, g = split_u(u.astype(F32))
        m_ref[j, h] = (v * gelu(g)).astype(BF)
        c_mx[j] = send(m_ref.at[j, h], m_ref.at[j, h], "mx", j, dev_x)
        c_md[j] = send(m_ref.at[j, h], m_ref.at[j, h], "md", j, dev_sib)

    def s3(j):
        c_mx[j].wait_recv()
        c_mf[j] = send(m_ref.at[j, xn], m_ref.at[j, xn], "mf", j, dev_sib)

    def s4(j):
        c_md[j].wait_recv()
        c_mf[j].wait_recv()
        pltpu.make_async_copy(w2_ref.at[j * 1024:(j + 1) * 1024, :], w2b.at[j], ls2.at[j]).wait()
        m = jnp.concatenate([m_ref[j, q] for q in range(4)], axis=1)
        for n in range(2):
            cols = slice(n * 512, (n + 1) * 512)
            part = dot(m, w2b[j, :, cols])
            if j > 0:
                part = facc[:, cols] + part
            if j < NC - 1:
                facc[:, cols] = part
            else:
                fs[n] = part.astype(BF)
                c_fy.append(send(fs.at[n], fr.at[n], "fy", n, dev_y))

    def gather_u(j):
        c_gx[j] = send(u_ref.at[j, h], u_ref.at[j, h], "gx", j, dev_x)
        c_gd[j] = send(u_ref.at[j, h], u_ref.at[j, h], "gd", j, dev_sib)

    def forward_u(j):
        c_gx[j].wait_recv()
        c_gf[j] = send(u_ref.at[j, xn], u_ref.at[j, xn], "gf", j, dev_sib)

    c_ud, c_ux, c_mx, c_md, c_mf, c_fy, c_gx, c_gd, c_gf = {}, {}, {}, {}, {}, [], {}, {}, {}
    u_part(0)
    u_part(1)
    s1(0)
    u_part(2)
    s1(1)
    u_part(3)
    s1(2)
    s2(0)
    u_part(4)
    s1(3)
    s1(4)
    s2(1)
    s2(2)
    s2(3)
    s3(0)
    s4(0)
    s2(4)
    for j in range(NC):
        gather_u(j)
    for j in range(1, NC):
        s3(j)
        if j > 1:
            s4(j - 1)
    s4(NC - 1)

    for n in range(2):
        cols = slice(n * 512, (n + 1) * 512)
        c_fy[n].wait_recv()
        f = fs[n].astype(F32) + fr[n].astype(F32)
        nrm_ref[:, cols] = ALPHA * x_ref[:, cols].astype(F32) + f + b2_ref[:, cols]
    r = nrm_ref[...]
    gdy = dy_ref[...].astype(F32) * gam_ref[...]
    m_loc = jnp.sum(r, axis=1, keepdims=True) * (1.0 / H)
    cen = r - m_loc
    m2 = jnp.sum(cen * cen, axis=1, keepdims=True)
    sg = jnp.sum(gdy, axis=1, keepdims=True)
    cg = jnp.sum(gdy * cen, axis=1, keepdims=True)
    lane = lax.broadcasted_iota(jnp.int32, (T, 128), 1)
    pack = jnp.where(lane == 0, m_loc, jnp.where(lane == 1, m2, jnp.where(lane == 2, sg, cg)))
    stb[h] = pack.T[0:8]
    c_st = [send(stb.at[h], stb.at[h], "st", i, dev) for i, dev in enumerate((dev_sib, dev_x, dev_xs))]
    for cp in c_st:
        cp.wait_recv()
    st = [stb[i] for i in range(4)]
    mu = ((st[0][0:1] + st[1][0:1]) + (st[2][0:1] + st[3][0:1])) * 0.25
    m2t = jnp.zeros_like(mu)
    sgt = jnp.zeros_like(mu)
    cgt = jnp.zeros_like(mu)
    for i in range(4):
        delta = st[i][0:1] - mu
        m2t += st[i][1:2] + (H * delta) * delta
        sgt += st[i][2:3]
        cgt += st[i][3:4] + delta * st[i][2:3]
    rho = lax.rsqrt(m2t * (1.0 / (4 * H)) + LN_EPS)
    rows = jnp.concatenate([mu, rho, sgt * (1.0 / (4 * H)), cgt * rho * (1.0 / (4 * H)), jnp.zeros((124, T), F32)], axis=0)
    colst = rows.T
    mu_c, rho_c, mg_c, mgr_c = (colst[:, i:i + 1] for i in range(4))
    nrm = (r - mu_c) * rho_c
    dr = rho_c * (gdy - mg_c - nrm * mgr_c)
    nrm_ref[...] = nrm
    dr_ref[...] = dr
    d_ref[...] = dr.astype(BF)
    d_t = dr.T.astype(BF)

    c_dd, c_dx, c_df = {}, {}, {}
    mine, theirs = (c, c + 2), (1 - c, 3 - c)

    def dm_part(j):
        for i, q in enumerate(theirs + mine):
            rows_q = pl.ds(pl.multiple_of(q * Q, Q), Q)
            dmb[j, i] = dot(w2b[j, rows_q, :], d_t).T.astype(BF)
            if i < 2:
                c_dd[j, i] = send(dmb.at[j, i], dmr.at[j, i], "dd", 2 * j + i, dev_sib)

    def dm_sum(j):
        for i in range(2):
            c_dd[j, i].wait_recv()
            val = (dmb[j, 2 + i].astype(F32) + dmr[j, i].astype(F32)).astype(BF)
            if j < S:
                dsum[j, i] = val
            else:
                dms_ref[j - S, i] = val
        if j < S:
            c_dx[j] = send(dsum.at[j], dxr.at[j], "dx", j, dev_x)

    def dm_full(j):
        c_dx[j].wait_recv()
        for i in range(2):
            q = mine[i]
            dmf_ref[j, q] = (dsum[j, i].astype(F32) + dxr[j, i].astype(F32)).astype(BF)
            c_df[j, i] = send(dmf_ref.at[j, q], dmf_ref.at[j, q], "df", 2 * j + i, dev_sib)

    dm_part(0)
    dm_part(1)
    dm_sum(0)
    for j in range(2, NC):
        dm_part(j)
        dm_sum(j - 1)
        forward_u(j - 2)
    dm_sum(NC - 1)
    forward_u(NC - 2)
    forward_u(NC - 1)
    for j in range(S):
        dm_full(j)
    for cp in list(c_gd.values()) + list(c_gf.values()) + list(c_df.values()):
        cp.wait_recv()
    for cp in live:
        cp.wait_send()


def forward_call(x, w1, b1, w2, b2, gam, dy):
    scratch = [pltpu.VMEM((NC, 4, H, 512), BF), pltpu.VMEM((NC, 1024, H), BF),
               pltpu.VMEM((NC, 4, T, 512), BF), pltpu.VMEM((NC, 2, T, 512), BF),
               pltpu.VMEM((NC, T, 512), BF), pltpu.VMEM((NC, T, 512), BF),
               pltpu.VMEM((T, H), F32), pltpu.VMEM((2, T, 512), BF), pltpu.VMEM((2, T, 512), BF),
               pltpu.VMEM((4, 8, T), F32),
               pltpu.VMEM((NC, 4, T, Q), BF), pltpu.VMEM((NC, 2, T, Q), BF),
               pltpu.VMEM((S, 2, T, Q), BF), pltpu.VMEM((S, 2, T, Q), BF),
               pltpu.SemaphoreType.DMA((NC, 4)), pltpu.SemaphoreType.DMA((NC,))]
    for n in SEM_NAMES:
        scratch += [pltpu.SemaphoreType.DMA((N_SEM[n],)), pltpu.SemaphoreType.DMA((N_SEM[n],))]
    outs = [sds((NC, 4, T, Q), BF), sds((NC, 4, T, 512), BF), sds((T, H), BF), sds((T, H), F32), sds((T, H), F32),
            sds((S, 4, T, Q), BF), sds((NC - S, 2, T, Q), BF)]
    return pl.pallas_call(
        forward_kernel, out_shape=outs, name="fwd",
        in_specs=[VMEM, ANY, VMEM, ANY, VMEM, VMEM, VMEM], out_specs=[VMEM] * len(outs), scratch_shapes=scratch,
        compiler_params=pltpu.CompilerParams(collective_id=0, has_side_effects=True, vmem_limit_bytes=VLIM),
        cost_estimate=pl.CostEstimate(flops=5 * 10 ** 9, bytes_accessed=32 << 20, transcendentals=0),
    )(x, w1, b1, w2, b2, gam, dy)


NB2 = 6
NB1 = 4


def first_grads_kernel(m_ref, u_ref, d_ref, dr_ref, nrm_ref, dmf_ref, x_ref, gam_ref, beta_ref, dy_ref, w1_ref,
                       dw1_ref, dw2_ref, y_ref, db2_ref, dgam_ref, dbeta_ref, db1_ref, dxt_ref,
                       w1b, ob2, ob1, xt, ls1, so2, so1):
    def w1_load(j, q):
        return pltpu.make_async_copy(w1_ref.at[:, (j * 4 + q) * 512:(j * 4 + q + 1) * 512], w1b.at[j, q], ls1.at[j, q])

    for j in range(S):
        for q in range(4):
            w1_load(j, q).start()

    def put2(t):
        return pltpu.make_async_copy(ob2.at[t % NB2], dw2_ref.at[t * Q:(t + 1) * Q, :], so2.at[t % NB2])

    for t in range(NC * 4):
        if t >= NB2:
            put2(t - NB2).wait()
        ob2[t % NB2] = dot(m_ref[t // 4, t % 4].T, d_ref[...])
        put2(t).start()

    dy = dy_ref[...].astype(F32)
    y_ref[...] = (gam_ref[...] * nrm_ref[...] + beta_ref[...]).astype(BF)
    db2_ref[...] = jnp.sum(dr_ref[...], axis=0, keepdims=True)
    dgam_ref[...] = jnp.sum(dy * nrm_ref[...], axis=0, keepdims=True)
    dbeta_ref[...] = jnp.sum(dy, axis=0, keepdims=True)
    xt[...] = x_ref[...].T

    def put1(t):
        return pltpu.make_async_copy(ob1.at[t % NB1], dw1_ref.at[:, t * 512:(t + 1) * 512], so1.at[t % NB1])

    for t in range(S * 4):
        j, q = t // 4, t % 4
        du_f = grad_u(u_ref[j, q], dmf_ref[j, q].astype(F32))
        db1_ref[j, q] = jnp.sum(du_f, axis=0, keepdims=True)
        du = du_f.astype(BF)
        if t >= NB1:
            put1(t - NB1).wait()
        ob1[t % NB1] = dot(xt[...], du)
        put1(t).start()
        w1_load(j, q).wait()
        part = dot(w1b[j, q], du_f.T.astype(BF))
        dxt_ref[...] = part if t == 0 else dxt_ref[...] + part
    for t in range(NC * 4 - NB2, NC * 4):
        put2(t).wait()
    for t in range(max(0, S * 4 - NB1), S * 4):
        put1(t).wait()


def first_grads_call(m, u, d, dr, nrm, dmf, x, gam, beta, dy, w1):
    outs = [sds((H, NC * 2048), F32), sds((NC * 1024, H), F32), sds((T, H), BF), sds((1, H), F32), sds((1, H), F32),
            sds((1, H), F32), sds((S, 4, 1, 512), F32), sds((H, T), F32)]
    return pl.pallas_call(
        first_grads_kernel, out_shape=outs, name="ga",
        in_specs=[VMEM] * 10 + [ANY], out_specs=[ANY, ANY] + [VMEM] * 6,
        scratch_shapes=[pltpu.VMEM((S, 4, H, 512), BF), pltpu.VMEM((NB2, Q, H), F32), pltpu.VMEM((NB1, H, 512), F32),
                        pltpu.VMEM((H, T), BF), pltpu.SemaphoreType.DMA((S, 4)), pltpu.SemaphoreType.DMA((NB2,)),
                        pltpu.SemaphoreType.DMA((NB1,))],
        compiler_params=pltpu.CompilerParams(vmem_limit_bytes=48 * 1024 * 1024),
        cost_estimate=pl.CostEstimate(flops=3 * 10 ** 9, bytes_accessed=44 << 20, transcendentals=0),
    )(m, u, d, dr, nrm, dmf, x, gam, beta, dy, w1)


B = NC - S


def second_kernel(dms_ref, dmx_ref, u_ref, dxt_ref, w1_ref, du_ref, db1_ref, dxp_ref,
                  w1b, dmf, acc, ls1, ss, rs):
    h, y, c, sib, xn, xs = places()
    mine, theirs = (c, c + 2), (1 - c, 3 - c)
    dev_sib = (0, y, sib)

    def w1_load(j, k, q):
        return pltpu.make_async_copy(w1_cols(w1_ref, S + j, q), w1b.at[j, k], ls1.at[j, k])

    steps = [(j, i, mine[i]) for j in range(B) for i in range(2)] + [(j, 2 + i, theirs[i]) for j in range(B) for i in range(2)]
    for j, k, q in steps:
        w1_load(j, k, q).start()
    bar = pltpu.get_barrier_semaphore()
    pl.semaphore_signal(bar, inc=1, device_id=dev_sib, device_id_type=MESH)
    pl.semaphore_wait(bar, 1)
    cps = {}
    for j in range(B):
        for i in range(2):
            q = mine[i]
            dmf[j, q] = (dms_ref[j, i].astype(F32) + dmx_ref[j, i].astype(F32)).astype(BF)
            cps[j, i] = remote(dmf.at[j, q], dmf.at[j, q], (ss, rs), 2 * j + i, dev_sib)
            cps[j, i].start()
    for n, (j, k, q) in enumerate(steps):
        if k >= 2:
            cps[j, k - 2].wait_recv()
        du_f = grad_u(u_ref[S + j, q], dmf[j, q].astype(F32))
        db1_ref[j, q] = jnp.sum(du_f, axis=0, keepdims=True)
        du_ref[j, q] = du_f.astype(BF)
        w1_load(j, k, q).wait()
        part = dot(w1b[j, k], du_f.T.astype(BF))
        acc[...] = (dxt_ref[...] if n == 0 else acc[...]) + part
    dxp_ref[...] = acc[...].T.astype(BF)
    for cp in cps.values():
        cp.wait_send()


def second_call(dms, dmx, u, dxt, w1):
    outs = [sds((B, 4, T, 512), BF), sds((B, 4, 1, 512), F32), sds((T, H), BF)]
    return pl.pallas_call(
        second_kernel, out_shape=outs, name="mid",
        in_specs=[VMEM] * 4 + [ANY], out_specs=[VMEM] * 3,
        scratch_shapes=[pltpu.VMEM((B, 4, H, 512), BF), pltpu.VMEM((B, 4, T, Q), BF), pltpu.VMEM((H, T), F32),
                        pltpu.SemaphoreType.DMA((B, 4)), pltpu.SemaphoreType.DMA((2 * B,)), pltpu.SemaphoreType.DMA((2 * B,))],
        compiler_params=pltpu.CompilerParams(collective_id=1, has_side_effects=True, vmem_limit_bytes=32 * 1024 * 1024),
        cost_estimate=pl.CostEstimate(flops=2 * 10 ** 9, bytes_accessed=14 << 20, transcendentals=0),
    )(dms, dmx, u, dxt, w1)


def last_grads_kernel(x_ref, du_ref, dba_ref, dbb_ref, dw1_in, dw1_ref, db1_ref, ob1, xt, so1):
    xt[...] = x_ref[...].T

    def put1(t):
        return pltpu.make_async_copy(ob1.at[t % NB1], dw1_ref.at[:, (S * 4 + t) * 512:(S * 4 + t + 1) * 512], so1.at[t % NB1])

    for t in range(B * 4):
        if t >= NB1:
            put1(t - NB1).wait()
        ob1[t % NB1] = dot(xt[...], du_ref[t // 4, t % 4])
        put1(t).start()
    for j in range(NC):
        for q in range(4):
            src = dba_ref[j, q] if j < S else dbb_ref[j - S, q]
            db1_ref[:, (j * 4 + q) * 512:(j * 4 + q + 1) * 512] = src
    for t in range(B * 4 - NB1, B * 4):
        put1(t).wait()


def last_grads_call(x, du, dba, dbb, dw1):
    outs = [sds((H, NC * 2048), F32), sds((1, NC * 2048), F32)]
    return pl.pallas_call(
        last_grads_kernel, out_shape=outs, name="gb",
        in_specs=[VMEM] * 4 + [ANY], out_specs=[ANY, VMEM],
        scratch_shapes=[pltpu.VMEM((NB1, H, 512), F32), pltpu.VMEM((H, T), BF), pltpu.SemaphoreType.DMA((NB1,))],
        input_output_aliases={4: 0},
        compiler_params=pltpu.CompilerParams(vmem_limit_bytes=24 * 1024 * 1024),
        cost_estimate=pl.CostEstimate(flops=10 ** 9, bytes_accessed=26 << 20, transcendentals=0),
    )(x, du, dba, dbb, dw1)


def solution(mesh):
    data_spec = P('dp', 'hd')
    hid_spec = P('hd')
    in_specs = (data_spec, P('hd', 'ff'), P('ff'), P('ff', 'hd'), hid_spec, hid_spec, hid_spec, data_spec)
    out_specs = (data_spec, data_spec, P(('dp', 'hd'), 'ff'), P(('dp', 'ff'), 'hd'), P(('dp', 'ff')), P(('dp', 'hd')), P(('dp', 'hd')), P(('dp', 'hd')))

    def device_step(x, w1, b1, w2, b2, gam, beta, dy):
        b2, gam, beta = (a.reshape(1, H) for a in (b2, gam, beta))
        m, u, d, dr, nrm, dmf, dms = forward_call(x, w1, b1.reshape(NC * 4, 1, 512), w2, b2, gam, dy)
        dmx = lax.ppermute(dms, 'hd', [(0, 2), (2, 0), (1, 3), (3, 1)])
        dw1, dw2, y, db2, dgam, dbeta, dba, dxt = first_grads_call(m, u, d, dr, nrm, dmf, x, gam, beta, dy, w1)
        du, dbb, dxp = second_call(dms, dmx, u, dxt, w1)
        dxr = lax.ppermute(dxp, 'ff', [(0, 1), (1, 0)])
        dw1, db1 = last_grads_call(x, du, dba, dbb, dw1)
        dx = (ALPHA * dr + (dxp.astype(F32) + dxr.astype(F32))).astype(BF)
        return y, dx, dw1, dw2, db1.reshape(-1), db2.reshape(-1), dgam.reshape(-1), dbeta.reshape(-1)

    return jax.shard_map(device_step, mesh=mesh, in_specs=in_specs, out_specs=out_specs, check_vma=False)
```

```python
import functools
import math
import jax
import jax.numpy as jnp
from jax import lax
from jax.experimental import pallas as pl
from jax.experimental.pallas import tpu as pltpu
from jax.sharding import PartitionSpec as P

PAIR = 128
ALPHA = math.sqrt(140.0)
LN_EPS = 1e-5
C0 = math.sqrt(2.0 / math.pi)
C1 = 0.044715
MESH = pl.DeviceIdType.MESH
F32 = jnp.float32
BF = jnp.bfloat16
T = 128
H = 1024
NU = 10
CH = ((0, 1), (1, 3), (3, 5), (5, 7), (7, 9), (9, 10))
NC = len(CH)
VLIM = 62 * 1024 * 1024

VMEM = pl.BlockSpec(memory_space=pltpu.VMEM)
ANY = pl.BlockSpec(memory_space=pl.ANY)


def sds(shape, dtype):
    return jax.ShapeDtypeStruct(shape, dtype)


def dot(a, b):
    return jnp.dot(a, b, preferred_element_type=F32)


def gelu(g):
    t = jnp.tanh(C0 * (g + C1 * (g * g * g)))
    return g * (0.5 * (1.0 + t))


def gelu_both(g):
    g2 = g * g
    t = jnp.tanh(C0 * (g + C1 * (g2 * g)))
    cdf = 0.5 * (1.0 + t)
    slope = cdf + (0.5 * g) * (1.0 - t * t) * (C0 * (1.0 + (3.0 * C1) * g2))
    return g * cdf, slope


def grad_u(u, dm):
    u = u.astype(F32)
    v, g = u[:, :PAIR], u[:, PAIR:]
    val, slope = gelu_both(g)
    return jnp.concatenate([dm * val, dm * v * slope], axis=1)


def places():
    h = lax.axis_index("hd")
    y = lax.axis_index("ff")
    c = lax.rem(h, 2)
    sib = h + 1 - 2 * c
    xn = lax.rem(h + 2, 4)
    xs = lax.rem(sib + 2, 4)
    return h, y, c, sib, xn, xs


def remote(src, dst, sems, k, dev):
    return pltpu.make_async_remote_copy(src_ref=src, dst_ref=dst, send_sem=sems[0].at[k], recv_sem=sems[1].at[k],
                                        device_id=dev, device_id_type=MESH)


def unit(j, q):
    u0, u1 = CH[j]
    return 4 * u0 + q * (u1 - u0)


def aligned(start, size, tile):
    return pl.ds(pl.multiple_of(start * tile, tile), size * tile)


N_SEM = {"ud": 2 * NC, "ux": NC, "mx": NC, "md": NC, "mf": NC, "gx": NC, "gd": NC, "gf": NC, "fy": 2, "st": 3,
         "dd": 2 * NC, "dx": NC, "df": 2 * NC}
SEM_NAMES = list(N_SEM)


def comm_kernel(x_ref, w1_ref, b1_ref, w2_ref, b2_ref, gam_ref, dy_ref,
                m_out, du_out, d_out, dr_out, nrm_out, db1_ref, dxp_ref,
                w1b, w2b, ub, rb, xsb, xrb, facc, fs, fr, stb, dmb, dmr, dsum, dxr, m_ref, u_ref, dmf, du_ref,
                d_ref, dr_ref, nrm_ref, acc,
                ls1, ls2, os, *sem_list):
    sems = {n: (sem_list[2 * i], sem_list[2 * i + 1]) for i, n in enumerate(SEM_NAMES)}
    h, y, c, sib, xn, xs = places()
    dev_sib, dev_x, dev_xs, dev_y = (0, y, sib), (0, y, xn), (0, y, xs), (0, 1 - y, h)
    order = [xs, xn, sib, h]
    outs = []

    def w1_load(j, k):
        u0, u1 = CH[j]
        n = u1 - u0
        return pltpu.make_async_copy(w1_ref.at[:, aligned(unit(j, order[k]), n, 256)], w1b.at[k, :, u0 * 256:u1 * 256],
                                     ls1.at[j, k])

    def w2_load(j):
        rows = slice(4 * 128 * CH[j][0], 4 * 128 * CH[j][1])
        return pltpu.make_async_copy(w2_ref.at[rows, :], w2b.at[rows, :], ls2.at[j])

    def put(src, dst):
        cp = pltpu.make_async_copy(src, dst, os.at[len(outs)])
        cp.start()
        outs.append(cp)

    for j in range(NC + 1):
        for k in (0, 1):
            if j < NC:
                w1_load(j, k).start()
        for k in (2, 3):
            if j > 0:
                w1_load(j - 1, k).start()
    bar = pltpu.get_barrier_semaphore()
    for dev in (dev_sib, dev_x, dev_xs, dev_y):
        pl.semaphore_signal(bar, inc=1, device_id=dev, device_id_type=MESH)
    pl.semaphore_wait(bar, 4)

    live = []

    def send(src, dst, name, k, dev):
        cp = remote(src, dst, sems[name], k, dev)
        cp.start()
        live.append(cp)
        return cp

    def u_part(j, ks):
        u0, u1 = CH[j]
        us = slice(u0, u1)
        for k in ks:
            w1_load(j, k).wait()
            r = dot(x_ref[...], w1b[k, :, u0 * 256:u1 * 256]).astype(BF)
            for i in range(u1 - u0):
                ub[k, u0 + i] = r[:, i * 256:(i + 1) * 256]
            if k == 0:
                c_ud[j, 1] = send(ub.at[0, us], rb.at[1, us], "ud", 2 * j + 1, dev_sib)
            if k == 2:
                c_ud[j, 0] = send(ub.at[2, us], rb.at[0, us], "ud", 2 * j, dev_sib)

    def ux(j):
        u_part(j, (0, 1))

    def uo(j):
        u_part(j, (2, 3))

    def s1(j):
        us = slice(*CH[j])
        c_ud[j, 1].wait_recv()
        xsb[us] = (ub[1, us].astype(F32) + rb[1, us].astype(F32)).astype(BF)
        c_ux[j] = send(xsb.at[us], xrb.at[us], "ux", j, dev_x)

    def s2(j):
        u0, u1 = CH[j]
        us = slice(u0, u1)
        c_ud[j, 0].wait_recv()
        c_ux[j].wait_recv()
        for i in range(u1 - u0):
            a = u0 + i
            u = ub[3, a].astype(F32) + rb[0, a].astype(F32) + xrb[a].astype(F32) + b1_ref[unit(j, h) + i]
            u = u.astype(BF)
            u_ref[h, a] = u
            u = u.astype(F32)
            m_ref[h, a] = (u[:, :PAIR] * gelu(u[:, PAIR:])).astype(BF)
        c_mx[j] = send(m_ref.at[h, us], m_ref.at[h, us], "mx", j, dev_x)
        c_md[j] = send(m_ref.at[h, us], m_ref.at[h, us], "md", j, dev_sib)

    def s3(j):
        us = slice(*CH[j])
        c_mx[j].wait_recv()
        c_mf[j] = send(m_ref.at[xn, us], m_ref.at[xn, us], "mf", j, dev_sib)

    def s4(j):
        u0, u1 = CH[j]
        c_md[j].wait_recv()
        c_mf[j].wait_recv()
        w2_load(j).wait()
        m = jnp.concatenate([m_ref[q, a] for q in range(4) for a in range(u0, u1)], axis=1)
        for n in range(2):
            cols = slice(n * 512, (n + 1) * 512)
            part = dot(m, w2b[4 * 128 * u0:4 * 128 * u1, cols])
            if j > 0:
                part = facc[:, cols] + part
            if j < NC - 1:
                facc[:, cols] = part
            else:
                fs[n] = part.astype(BF)
                c_fy.append(send(fs.at[n], fr.at[n], "fy", n, dev_y))

    def gather_u(j):
        us = slice(*CH[j])
        c_gx[j] = send(u_ref.at[h, us], u_ref.at[h, us], "gx", j, dev_x)
        c_gd[j] = send(u_ref.at[h, us], u_ref.at[h, us], "gd", j, dev_sib)

    def forward_u(j):
        us = slice(*CH[j])
        c_gx[j].wait_recv()
        c_gf[j] = send(u_ref.at[xn, us], u_ref.at[xn, us], "gf", j, dev_sib)

    c_ud, c_ux, c_mx, c_md, c_mf, c_fy, c_gx, c_gd, c_gf = {}, {}, {}, {}, {}, [], {}, {}, {}
    ux(0)
    ux(1)
    s1(0)
    uo(0)
    ux(2)
    s1(1)
    uo(1)
    ux(3)
    s1(2)
    for j in range(NC):
        w2_load(j).start()
    uo(2)
    ux(4)
    s1(3)
    s2(0)
    ux(5)
    s1(4)
    uo(3)
    s1(5)
    uo(4)
    s2(1)
    uo(5)
    s2(2)
    s2(3)
    s2(4)
    s3(0)
    s4(0)
    s2(5)
    for j in range(NC):
        gather_u(j)
    for j in range(1, NC):
        s3(j)
        if j > 1:
            s4(j - 1)
    s4(NC - 1)
    put(m_ref, m_out)

    for n in range(2):
        cols = slice(n * 512, (n + 1) * 512)
        c_fy[n].wait_recv()
        f = fs[n].astype(F32) + fr[n].astype(F32)
        nrm_ref[:, cols] = ALPHA * x_ref[:, cols].astype(F32) + f + b2_ref[:, cols]
    r = nrm_ref[...]
    gdy = dy_ref[...].astype(F32) * gam_ref[...]
    m_loc = jnp.sum(r, axis=1, keepdims=True) * (1.0 / H)
    cen = r - m_loc
    m2 = jnp.sum(cen * cen, axis=1, keepdims=True)
    sg = jnp.sum(gdy, axis=1, keepdims=True)
    cg = jnp.sum(gdy * cen, axis=1, keepdims=True)
    lane = lax.broadcasted_iota(jnp.int32, (T, 128), 1)
    pack = jnp.where(lane == 0, m_loc, jnp.where(lane == 1, m2, jnp.where(lane == 2, sg, cg)))
    stb[h] = pack.T[0:8]
    c_st = [send(stb.at[h], stb.at[h], "st", i, dev) for i, dev in enumerate((dev_sib, dev_x, dev_xs))]
    for cp in c_st:
        cp.wait_recv()
    st = [stb[i] for i in range(4)]
    mu = ((st[0][0:1] + st[1][0:1]) + (st[2][0:1] + st[3][0:1])) * 0.25
    m2t = jnp.zeros_like(mu)
    sgt = jnp.zeros_like(mu)
    cgt = jnp.zeros_like(mu)
    for i in range(4):
        delta = st[i][0:1] - mu
        m2t += st[i][1:2] + (H * delta) * delta
        sgt += st[i][2:3]
        cgt += st[i][3:4] + delta * st[i][2:3]
    rho = lax.rsqrt(m2t * (1.0 / (4 * H)) + LN_EPS)
    rows = jnp.concatenate([mu, rho, sgt * (1.0 / (4 * H)), cgt * rho * (1.0 / (4 * H)), jnp.zeros((124, T), F32)], axis=0)
    colst = rows.T
    mu_c, rho_c, mg_c, mgr_c = (colst[:, i:i + 1] for i in range(4))
    nrm = (r - mu_c) * rho_c
    dr = rho_c * (gdy - mg_c - nrm * mgr_c)
    nrm_ref[...] = nrm
    dr_ref[...] = dr
    d_ref[...] = dr.astype(BF)
    d_t = dr.T.astype(BF)
    put(nrm_ref, nrm_out)
    put(dr_ref, dr_out)
    put(d_ref, d_out)

    c_dd, c_dx, c_df = {}, {}, {}
    mine, mine_k, theirs, theirs_k = (h, xn), (3, 1), (sib, xs), (2, 0)

    def dm_part(j):
        u0, u1 = CH[j]
        n = u1 - u0
        for i, q in enumerate(theirs + mine):
            r = dot(w2b[aligned(unit(j, q), n, 128), :], d_t).T.astype(BF)
            for a in range(n):
                dmb[i, u0 + a] = r[:, a * 128:(a + 1) * 128]
            if i < 2:
                c_dd[j, i] = send(dmb.at[i, u0:u1], dmr.at[i, u0:u1], "dd", 2 * j + i, dev_sib)

    def dm_sum(j):
        us = slice(*CH[j])
        for i in range(2):
            c_dd[j, i].wait_recv()
            dsum[i, us] = (dmb[2 + i, us].astype(F32) + dmr[i, us].astype(F32)).astype(BF)
        c_dx[j] = send(dsum.at[:, us], dxr.at[:, us], "dx", j, dev_x)

    def dm_full(j):
        us = slice(*CH[j])
        c_dx[j].wait_recv()
        for i in range(2):
            q = mine[i]
            dmf[q, us] = (dsum[i, us].astype(F32) + dxr[1 - i, us].astype(F32)).astype(BF)
            c_df[j, i] = send(dmf.at[q, us], dmf.at[q, us], "df", 2 * j + i, dev_sib)

    def grads(j, qs, ks, first):
        u0, u1 = CH[j]
        for q, k in zip(qs, ks):
            parts = []
            for a in range(u0, u1):
                du_f = grad_u(u_ref[q, a], dmf[q, a].astype(F32))
                db1_ref[unit(j, q) + a - u0] = jnp.sum(du_f, axis=0, keepdims=True)
                du_ref[q, a] = du_f.astype(BF)
                parts.append(du_f)
            du_t = jnp.concatenate(parts, axis=1).T.astype(BF)
            part = dot(w1b[k, :, u0 * 256:u1 * 256], du_t)
            acc[...] = part if first else acc[...] + part
            first = False

    def grads_mine(j):
        dm_full(j)
        grads(j, mine, mine_k, j == 0)

    def grads_theirs(j):
        us = slice(*CH[j])
        for i in range(2):
            c_df[j, i].wait_recv()
        grads(j, theirs, theirs_k, False)
        put(du_ref.at[:, us], du_out.at[:, us])

    dm_part(0)
    dm_part(1)
    dm_sum(0)
    for j in range(2, NC):
        dm_part(j)
        dm_sum(j - 1)
        forward_u(j - 2)
    dm_sum(NC - 1)
    forward_u(NC - 2)
    forward_u(NC - 1)
    for cp in list(c_gd.values()) + list(c_gf.values()):
        cp.wait_recv()
    for j in range(NC):
        grads_mine(j)
        if j > 0:
            grads_theirs(j - 1)
    grads_theirs(NC - 1)
    dxp_ref[...] = acc[...].T.astype(BF)
    for cp in live:
        cp.wait_send()
    for cp in outs:
        cp.wait()


def comm_call(x, w1, b1, w2, b2, gam, dy):
    scratch = [pltpu.VMEM((4, H, NU * 256), BF), pltpu.VMEM((4 * NU * 128, H), BF),
               pltpu.VMEM((4, NU, T, 256), BF), pltpu.VMEM((2, NU, T, 256), BF),
               pltpu.VMEM((NU, T, 256), BF), pltpu.VMEM((NU, T, 256), BF),
               pltpu.VMEM((T, H), F32), pltpu.VMEM((2, T, 512), BF), pltpu.VMEM((2, T, 512), BF),
               pltpu.VMEM((4, 8, T), F32),
               pltpu.VMEM((4, NU, T, 128), BF), pltpu.VMEM((2, NU, T, 128), BF),
               pltpu.VMEM((2, NU, T, 128), BF), pltpu.VMEM((2, NU, T, 128), BF),
               pltpu.VMEM((4, NU, T, 128), BF), pltpu.VMEM((4, NU, T, 256), BF), pltpu.VMEM((4, NU, T, 128), BF),
               pltpu.VMEM((4, NU, T, 256), BF),
               pltpu.VMEM((T, H), BF), pltpu.VMEM((T, H), F32), pltpu.VMEM((T, H), F32), pltpu.VMEM((H, T), F32),
               pltpu.SemaphoreType.DMA((NC, 4)), pltpu.SemaphoreType.DMA((NC,)), pltpu.SemaphoreType.DMA((NC + 4,))]
    for n in SEM_NAMES:
        scratch += [pltpu.SemaphoreType.DMA((N_SEM[n],)), pltpu.SemaphoreType.DMA((N_SEM[n],))]
    outs = [sds((4, NU, T, 128), BF), sds((4, NU, T, 256), BF), sds((T, H), BF), sds((T, H), F32), sds((T, H), F32),
            sds((4 * NU, 1, 256), F32), sds((T, H), BF)]
    return pl.pallas_call(
        comm_kernel, out_shape=outs, name="comm",
        in_specs=[VMEM, ANY, VMEM, ANY, VMEM, VMEM, VMEM], out_specs=[ANY] * 5 + [VMEM] * 2, scratch_shapes=scratch,
        compiler_params=pltpu.CompilerParams(collective_id=0, has_side_effects=True, vmem_limit_bytes=VLIM),
        cost_estimate=pl.CostEstimate(flops=8 * 10 ** 9, bytes_accessed=32 << 20, transcendentals=0),
    )(x, w1, b1, w2, b2, gam, dy)


NB2 = 6
NB1 = 6


def grads_kernel(m_hbm, du_hbm, d_hbm, nrm_hbm, dr_hbm, db1_in, x_ref, gam_ref, beta_ref, dy_ref,
                 dw1_ref, dw2_ref, y_ref, db1_ref, db2_ref, dgam_ref, dbeta_ref,
                 m_ref, du_ref, d_ref, nrm_ref, dr_ref, ob2, ob1, xt, ls, so2, so1):
    loads = [pltpu.make_async_copy(a, b, ls.at[i]) for i, (a, b) in enumerate(
        ((d_hbm, d_ref), (m_hbm, m_ref), (du_hbm, du_ref), (nrm_hbm, nrm_ref), (dr_hbm, dr_ref)))]
    for cp in loads:
        cp.start()
    tiles = [(j, q) for j in range(NC) for q in range(4)]

    def put2(t):
        j, q = tiles[t]
        n = CH[j][1] - CH[j][0]
        r0 = unit(j, q) * 128
        return pltpu.make_async_copy(ob2.at[t % NB2, :n * 128], dw2_ref.at[r0:r0 + n * 128, :], so2.at[t % NB2])

    def put1(t):
        j, q = tiles[t]
        n = CH[j][1] - CH[j][0]
        c0 = unit(j, q) * 256
        return pltpu.make_async_copy(ob1.at[t % NB1, :, :n * 256], dw1_ref.at[:, c0:c0 + n * 256], so1.at[t % NB1])

    loads[0].wait()
    loads[1].wait()
    for t, (j, q) in enumerate(tiles):
        if t >= NB2:
            put2(t - NB2).wait()
        for i, a in enumerate(range(*CH[j])):
            ob2[t % NB2, i * 128:(i + 1) * 128] = dot(m_ref[q, a].T, d_ref[...])
        put2(t).start()
        if t == 0:
            xt[...] = x_ref[...].T
    loads[2].wait()
    for t, (j, q) in enumerate(tiles):
        if t >= NB1:
            put1(t - NB1).wait()
        for i, a in enumerate(range(*CH[j])):
            ob1[t % NB1, :, i * 256:(i + 1) * 256] = dot(xt[...], du_ref[q, a])
        put1(t).start()
    loads[3].wait()
    loads[4].wait()
    dy = dy_ref[...].astype(F32)
    y_ref[...] = (gam_ref[...] * nrm_ref[...] + beta_ref[...]).astype(BF)
    db2_ref[...] = jnp.sum(dr_ref[...], axis=0, keepdims=True)
    dgam_ref[...] = jnp.sum(dy * nrm_ref[...], axis=0, keepdims=True)
    dbeta_ref[...] = jnp.sum(dy, axis=0, keepdims=True)
    for i in range(4 * NU):
        db1_ref[:, i * 256:(i + 1) * 256] = db1_in[i]
    last = len(tiles)
    for t in range(last - NB2, last):
        put2(t).wait()
    for t in range(last - NB1, last):
        put1(t).wait()


def grads_call(m, du, d, nrm, dr, db1, x, gam, beta, dy):
    outs = [sds((H, 4 * NU * 256), F32), sds((4 * NU * 128, H), F32), sds((T, H), BF), sds((1, 4 * NU * 256), F32),
            sds((1, H), F32), sds((1, H), F32), sds((1, H), F32)]
    return pl.pallas_call(
        grads_kernel, out_shape=outs, name="grads",
        in_specs=[ANY] * 5 + [VMEM] * 5, out_specs=[ANY, ANY] + [VMEM] * 5,
        scratch_shapes=[pltpu.VMEM((4, NU, T, 128), BF), pltpu.VMEM((4, NU, T, 256), BF), pltpu.VMEM((T, H), BF),
                        pltpu.VMEM((T, H), F32), pltpu.VMEM((T, H), F32),
                        pltpu.VMEM((NB2, 256, H), F32), pltpu.VMEM((NB1, H, 512), F32), pltpu.VMEM((H, T), BF),
                        pltpu.SemaphoreType.DMA((5,)), pltpu.SemaphoreType.DMA((NB2,)), pltpu.SemaphoreType.DMA((NB1,))],
        compiler_params=pltpu.CompilerParams(vmem_limit_bytes=40 * 1024 * 1024),
        cost_estimate=pl.CostEstimate(flops=4 * 10 ** 9, bytes_accessed=66 << 20, transcendentals=0),
    )(m, du, d, nrm, dr, db1, x, gam, beta, dy)


def solution(mesh):
    data_spec = P('dp', 'hd')
    hid_spec = P('hd')
    in_specs = (data_spec, P('hd', 'ff'), P('ff'), P('ff', 'hd'), hid_spec, hid_spec, hid_spec, data_spec)
    out_specs = (data_spec, data_spec, P(('dp', 'hd'), 'ff'), P(('dp', 'ff'), 'hd'), P(('dp', 'ff')), P(('dp', 'hd')), P(('dp', 'hd')), P(('dp', 'hd')))

    def device_step(x, w1, b1, w2, b2, gam, beta, dy):
        b2, gam, beta = (a.reshape(1, H) for a in (b2, gam, beta))
        m, du, d, dr, nrm, db1, dxp = comm_call(x, w1, b1.reshape(4 * NU, 1, 256), w2, b2, gam, dy)
        dxr = lax.ppermute(dxp, 'ff', [(0, 1), (1, 0)])
        dw1, dw2, y, db1, db2, dgam, dbeta = grads_call(m, du, d, nrm, dr, db1, x, gam, beta, dy)
        dx = (ALPHA * dr + (dxp.astype(F32) + dxr.astype(F32))).astype(BF)
        return y, dx, dw1, dw2, db1.reshape(-1), db2.reshape(-1), dgam.reshape(-1), dbeta.reshape(-1)

    return jax.shard_map(device_step, mesh=mesh, in_specs=in_specs, out_specs=out_specs, check_vma=False)
```

```python
import functools
import math
import jax
import jax.numpy as jnp
from jax import lax
from jax.experimental import pallas as pl
from jax.experimental.pallas import tpu as pltpu
from jax.sharding import PartitionSpec as P

PAIR = 128
ALPHA = math.sqrt(140.0)
LN_EPS = 1e-5
C0 = math.sqrt(2.0 / math.pi)
C1 = 0.044715
MESH = pl.DeviceIdType.MESH
F32 = jnp.float32
BF = jnp.bfloat16
T = 128
H = 1024
NU = 10
CH = ((0, 1), (1, 3), (3, 5), (5, 7), (7, 9), (9, 10))
NC = len(CH)
VLIM = 62 * 1024 * 1024

VMEM = pl.BlockSpec(memory_space=pltpu.VMEM)
ANY = pl.BlockSpec(memory_space=pl.ANY)


def sds(shape, dtype):
    return jax.ShapeDtypeStruct(shape, dtype)


def dot(a, b):
    return jnp.dot(a, b, preferred_element_type=F32)


def gelu(g):
    t = jnp.tanh(C0 * (g + C1 * (g * g * g)))
    return g * (0.5 * (1.0 + t))


def gelu_both(g):
    g2 = g * g
    t = jnp.tanh(C0 * (g + C1 * (g2 * g)))
    cdf = 0.5 * (1.0 + t)
    slope = cdf + (0.5 * g) * (1.0 - t * t) * (C0 * (1.0 + (3.0 * C1) * g2))
    return g * cdf, slope


def grad_u(u, dm):
    u = u.astype(F32)
    v, g = u[:, :PAIR], u[:, PAIR:]
    val, slope = gelu_both(g)
    return jnp.concatenate([dm * val, dm * v * slope], axis=1)


def places():
    h = lax.axis_index("hd")
    y = lax.axis_index("ff")
    c = lax.rem(h, 2)
    sib = h + 1 - 2 * c
    xn = lax.rem(h + 2, 4)
    xs = lax.rem(sib + 2, 4)
    return h, y, c, sib, xn, xs


def remote(src, dst, sems, k, dev):
    return pltpu.make_async_remote_copy(src_ref=src, dst_ref=dst, send_sem=sems[0].at[k], recv_sem=sems[1].at[k],
                                        device_id=dev, device_id_type=MESH)


def unit(j, q):
    u0, u1 = CH[j]
    return 4 * u0 + q * (u1 - u0)


def aligned(start, size, tile):
    return pl.ds(pl.multiple_of(start * tile, tile), size * tile)


N_SEM = {"ud": 2 * NC, "ux": NC, "mx": NC, "md": NC, "mf": NC, "gx": NC, "gd": NC, "gf": NC, "fy": 2, "st": 3,
         "dd": 2 * NC, "dx": NC, "df": 2 * NC}
SEM_NAMES = list(N_SEM)


def comm_kernel(x_ref, w1_ref, b1_ref, w2_ref, b2_ref, gam_ref, dy_ref,
                m_out, du_out, d_out, dr_out, nrm_out, db1_ref, dxp_ref,
                w1b, w2b, ub, rb, xsb, xrb, facc, fs, fr, stb, dmb, dmr, dsum, dxr, m_ref, u_ref, dmf, du_ref,
                d_ref, dr_ref, nrm_ref, acc,
                ls1, ls2, os, *sem_list):
    sems = {n: (sem_list[2 * i], sem_list[2 * i + 1]) for i, n in enumerate(SEM_NAMES)}
    h, y, c, sib, xn, xs = places()
    dev_sib, dev_x, dev_xs, dev_y = (0, y, sib), (0, y, xn), (0, y, xs), (0, 1 - y, h)
    order = [xs, xn, sib, h]
    outs = []

    def w1_load(j, k):
        u0, u1 = CH[j]
        n = u1 - u0
        return pltpu.make_async_copy(w1_ref.at[:, aligned(unit(j, order[k]), n, 256)], w1b.at[k, :, u0 * 256:u1 * 256],
                                     ls1.at[j, k])

    def w2_load(j):
        rows = slice(4 * 128 * CH[j][0], 4 * 128 * CH[j][1])
        return pltpu.make_async_copy(w2_ref.at[rows, :], w2b.at[rows, :], ls2.at[j])

    def put(src, dst):
        cp = pltpu.make_async_copy(src, dst, os.at[len(outs)])
        cp.start()
        outs.append(cp)

    for j in range(NC + 1):
        for k in (0, 1):
            if j < NC:
                w1_load(j, k).start()
        for k in (2, 3):
            if j > 0:
                w1_load(j - 1, k).start()
    bar = pltpu.get_barrier_semaphore()
    for dev in (dev_sib, dev_x, dev_xs, dev_y):
        pl.semaphore_signal(bar, inc=1, device_id=dev, device_id_type=MESH)
    pl.semaphore_wait(bar, 4)

    live = []

    def send(src, dst, name, k, dev):
        cp = remote(src, dst, sems[name], k, dev)
        cp.start()
        live.append(cp)
        return cp

    def u_part(j, ks):
        u0, u1 = CH[j]
        us = slice(u0, u1)
        for k in ks:
            w1_load(j, k).wait()
            r = dot(x_ref[...], w1b[k, :, u0 * 256:u1 * 256]).astype(BF)
            for i in range(u1 - u0):
                ub[k, u0 + i] = r[:, i * 256:(i + 1) * 256]
            if k == 0:
                c_ud[j, 1] = send(ub.at[0, us], rb.at[1, us], "ud", 2 * j + 1, dev_sib)
            if k == 2:
                c_ud[j, 0] = send(ub.at[2, us], rb.at[0, us], "ud", 2 * j, dev_sib)

    def ux(j):
        u_part(j, (0, 1))

    def uo(j):
        u_part(j, (2, 3))

    def s1(j):
        us = slice(*CH[j])
        c_ud[j, 1].wait_recv()
        xsb[us] = (ub[1, us].astype(F32) + rb[1, us].astype(F32)).astype(BF)
        c_ux[j] = send(xsb.at[us], xrb.at[us], "ux", j, dev_x)

    def s2(j):
        u0, u1 = CH[j]
        us = slice(u0, u1)
        c_ud[j, 0].wait_recv()
        c_ux[j].wait_recv()
        for i in range(u1 - u0):
            a = u0 + i
            u = ub[3, a].astype(F32) + rb[0, a].astype(F32) + xrb[a].astype(F32) + b1_ref[unit(j, h) + i]
            u = u.astype(BF)
            u_ref[h, a] = u
            u = u.astype(F32)
            m_ref[h, a] = (u[:, :PAIR] * gelu(u[:, PAIR:])).astype(BF)
        c_mx[j] = send(m_ref.at[h, us], m_ref.at[h, us], "mx", j, dev_x)
        c_md[j] = send(m_ref.at[h, us], m_ref.at[h, us], "md", j, dev_sib)

    def s3(j):
        us = slice(*CH[j])
        c_mx[j].wait_recv()
        c_mf[j] = send(m_ref.at[xn, us], m_ref.at[xn, us], "mf", j, dev_sib)

    def s4(j):
        u0, u1 = CH[j]
        c_md[j].wait_recv()
        c_mf[j].wait_recv()
        w2_load(j).wait()
        m = jnp.concatenate([m_ref[q, a] for q in range(4) for a in range(u0, u1)], axis=1)
        for n in range(2):
            cols = slice(n * 512, (n + 1) * 512)
            part = dot(m, w2b[4 * 128 * u0:4 * 128 * u1, cols])
            if j > 0:
                part = facc[:, cols] + part
            if j < NC - 1:
                facc[:, cols] = part
            else:
                fs[n] = part.astype(BF)
                c_fy.append(send(fs.at[n], fr.at[n], "fy", n, dev_y))

    def gather_u(j):
        us = slice(*CH[j])
        c_gx[j] = send(u_ref.at[h, us], u_ref.at[h, us], "gx", j, dev_x)
        c_gd[j] = send(u_ref.at[h, us], u_ref.at[h, us], "gd", j, dev_sib)

    def forward_u(j):
        us = slice(*CH[j])
        c_gx[j].wait_recv()
        c_gf[j] = send(u_ref.at[xn, us], u_ref.at[xn, us], "gf", j, dev_sib)

    c_ud, c_ux, c_mx, c_md, c_mf, c_fy, c_gx, c_gd, c_gf = {}, {}, {}, {}, {}, [], {}, {}, {}
    ux(0)
    ux(1)
    s1(0)
    uo(0)
    ux(2)
    s1(1)
    uo(1)
    ux(3)
    s1(2)
    for j in range(NC):
        w2_load(j).start()
    uo(2)
    ux(4)
    s1(3)
    s2(0)
    ux(5)
    s1(4)
    uo(3)
    s1(5)
    uo(4)
    s2(1)
    uo(5)
    s2(2)
    s2(3)
    s2(4)
    s3(0)
    s4(0)
    s2(5)
    for j in range(NC):
        gather_u(j)
    for j in range(1, NC):
        s3(j)
        if j > 1:
            s4(j - 1)
    s4(NC - 1)
    put(m_ref, m_out)

    for n in range(2):
        cols = slice(n * 512, (n + 1) * 512)
        c_fy[n].wait_recv()
        f = fs[n].astype(F32) + fr[n].astype(F32)
        nrm_ref[:, cols] = ALPHA * x_ref[:, cols].astype(F32) + f + b2_ref[:, cols]
    r = nrm_ref[...]
    gdy = dy_ref[...].astype(F32) * gam_ref[...]
    m_loc = jnp.sum(r, axis=1, keepdims=True) * (1.0 / H)
    cen = r - m_loc
    m2 = jnp.sum(cen * cen, axis=1, keepdims=True)
    sg = jnp.sum(gdy, axis=1, keepdims=True)
    cg = jnp.sum(gdy * cen, axis=1, keepdims=True)
    lane = lax.broadcasted_iota(jnp.int32, (T, 128), 1)
    pack = jnp.where(lane == 0, m_loc, jnp.where(lane == 1, m2, jnp.where(lane == 2, sg, cg)))
    stb[h] = pack.T[0:8]
    c_st = [send(stb.at[h], stb.at[h], "st", i, dev) for i, dev in enumerate((dev_sib, dev_x, dev_xs))]
    for cp in c_st:
        cp.wait_recv()
    st = [stb[i] for i in range(4)]
    mu = ((st[0][0:1] + st[1][0:1]) + (st[2][0:1] + st[3][0:1])) * 0.25
    m2t = jnp.zeros_like(mu)
    sgt = jnp.zeros_like(mu)
    cgt = jnp.zeros_like(mu)
    for i in range(4):
        delta = st[i][0:1] - mu
        m2t += st[i][1:2] + (H * delta) * delta
        sgt += st[i][2:3]
        cgt += st[i][3:4] + delta * st[i][2:3]
    rho = lax.rsqrt(m2t * (1.0 / (4 * H)) + LN_EPS)
    rows = jnp.concatenate([mu, rho, sgt * (1.0 / (4 * H)), cgt * rho * (1.0 / (4 * H)), jnp.zeros((124, T), F32)], axis=0)
    colst = rows.T
    mu_c, rho_c, mg_c, mgr_c = (colst[:, i:i + 1] for i in range(4))
    nrm = (r - mu_c) * rho_c
    dr = rho_c * (gdy - mg_c - nrm * mgr_c)
    nrm_ref[...] = nrm
    dr_ref[...] = dr
    d_ref[...] = dr.astype(BF)
    d_t = dr.T.astype(BF)
    put(nrm_ref, nrm_out)
    put(dr_ref, dr_out)
    put(d_ref, d_out)

    c_dd, c_dx, c_df = {}, {}, {}
    mine, mine_k, theirs, theirs_k = (h, xn), (3, 1), (sib, xs), (2, 0)

    def dm_part(j):
        u0, u1 = CH[j]
        n = u1 - u0
        for i, q in enumerate(theirs + mine):
            r = dot(w2b[aligned(unit(j, q), n, 128), :], d_t).T.astype(BF)
            for a in range(n):
                dmb[i, u0 + a] = r[:, a * 128:(a + 1) * 128]
            if i < 2:
                c_dd[j, i] = send(dmb.at[i, u0:u1], dmr.at[i, u0:u1], "dd", 2 * j + i, dev_sib)

    def dm_sum(j):
        us = slice(*CH[j])
        for i in range(2):
            c_dd[j, i].wait_recv()
            dsum[i, us] = (dmb[2 + i, us].astype(F32) + dmr[i, us].astype(F32)).astype(BF)
        c_dx[j] = send(dsum.at[:, us], dxr.at[:, us], "dx", j, dev_x)

    def dm_full(j):
        us = slice(*CH[j])
        c_dx[j].wait_recv()
        for i in range(2):
            q = mine[i]
            dmf[q, us] = (dsum[i, us].astype(F32) + dxr[1 - i, us].astype(F32)).astype(BF)
            c_df[j, i] = send(dmf.at[q, us], dmf.at[q, us], "df", 2 * j + i, dev_sib)

    def grads(j, qs, ks, first):
        u0, u1 = CH[j]
        for q, k in zip(qs, ks):
            parts = []
            for a in range(u0, u1):
                du_f = grad_u(u_ref[q, a], dmf[q, a].astype(F32))
                db1_ref[unit(j, q) + a - u0] = jnp.sum(du_f, axis=0, keepdims=True)
                du_ref[q, a] = du_f.astype(BF)
                parts.append(du_f)
            du_t = jnp.concatenate(parts, axis=1).T.astype(BF)
            part = dot(w1b[k, :, u0 * 256:u1 * 256], du_t)
            acc[...] = part if first else acc[...] + part
            first = False

    def grads_mine(j):
        dm_full(j)
        grads(j, mine, mine_k, j == 0)

    def grads_theirs(j):
        us = slice(*CH[j])
        for i in range(2):
            c_df[j, i].wait_recv()
        grads(j, theirs, theirs_k, False)
        put(du_ref.at[:, us], du_out.at[:, us])

    dm_part(0)
    dm_part(1)
    dm_sum(0)
    for j in range(2, NC):
        dm_part(j)
        dm_sum(j - 1)
        forward_u(j - 2)
    dm_sum(NC - 1)
    forward_u(NC - 2)
    forward_u(NC - 1)
    for cp in list(c_gd.values()) + list(c_gf.values()):
        cp.wait_recv()
    for j in range(NC):
        grads_mine(j)
        if j > 0:
            grads_theirs(j - 1)
    grads_theirs(NC - 1)
    dxp_ref[...] = acc[...].T.astype(BF)
    for cp in live:
        cp.wait_send()
    for cp in outs:
        cp.wait()


def comm_call(x, w1, b1, w2, b2, gam, dy):
    scratch = [pltpu.VMEM((4, H, NU * 256), BF), pltpu.VMEM((4 * NU * 128, H), BF),
               pltpu.VMEM((4, NU, T, 256), BF), pltpu.VMEM((2, NU, T, 256), BF),
               pltpu.VMEM((NU, T, 256), BF), pltpu.VMEM((NU, T, 256), BF),
               pltpu.VMEM((T, H), F32), pltpu.VMEM((2, T, 512), BF), pltpu.VMEM((2, T, 512), BF),
               pltpu.VMEM((4, 8, T), F32),
               pltpu.VMEM((4, NU, T, 128), BF), pltpu.VMEM((2, NU, T, 128), BF),
               pltpu.VMEM((2, NU, T, 128), BF), pltpu.VMEM((2, NU, T, 128), BF),
               pltpu.VMEM((4, NU, T, 128), BF), pltpu.VMEM((4, NU, T, 256), BF), pltpu.VMEM((4, NU, T, 128), BF),
               pltpu.VMEM((4, NU, T, 256), BF),
               pltpu.VMEM((T, H), BF), pltpu.VMEM((T, H), F32), pltpu.VMEM((T, H), F32), pltpu.VMEM((H, T), F32),
               pltpu.SemaphoreType.DMA((NC, 4)), pltpu.SemaphoreType.DMA((NC,)), pltpu.SemaphoreType.DMA((NC + 4,))]
    for n in SEM_NAMES:
        scratch += [pltpu.SemaphoreType.DMA((N_SEM[n],)), pltpu.SemaphoreType.DMA((N_SEM[n],))]
    outs = [sds((4, NU, T, 128), BF), sds((4, NU, T, 256), BF), sds((T, H), BF), sds((T, H), F32), sds((T, H), F32),
            sds((4 * NU, 1, 256), F32), sds((T, H), BF)]
    return pl.pallas_call(
        comm_kernel, out_shape=outs, name="comm",
        in_specs=[VMEM, ANY, VMEM, ANY, VMEM, VMEM, VMEM], out_specs=[ANY] * 5 + [VMEM] * 2, scratch_shapes=scratch,
        compiler_params=pltpu.CompilerParams(collective_id=0, has_side_effects=True, vmem_limit_bytes=VLIM),
        cost_estimate=pl.CostEstimate(flops=8 * 10 ** 9, bytes_accessed=32 << 20, transcendentals=0),
    )(x, w1, b1, w2, b2, gam, dy)


NB2 = 6
NB1 = 6


def grads_kernel(m_hbm, du_hbm, d_hbm, nrm_hbm, dr_hbm, db1_in, x_ref, gam_ref, beta_ref, dy_ref,
                 dw1_ref, dw2_ref, y_ref, db1_ref, db2_ref, dgam_ref, dbeta_ref,
                 m_ref, du_ref, d_ref, nrm_ref, dr_ref, ob2, ob1, xt, ls, so2, so1):
    loads = [pltpu.make_async_copy(a, b, ls.at[i]) for i, (a, b) in enumerate(
        ((d_hbm, d_ref), (m_hbm, m_ref), (du_hbm, du_ref), (nrm_hbm, nrm_ref), (dr_hbm, dr_ref)))]
    for cp in loads:
        cp.start()
    tiles = [(j, q) for j in range(NC) for q in range(4)]

    def put2(t):
        j, q = tiles[t]
        n = CH[j][1] - CH[j][0]
        r0 = unit(j, q) * 128
        return pltpu.make_async_copy(ob2.at[t % NB2, :n * 128], dw2_ref.at[r0:r0 + n * 128, :], so2.at[t % NB2])

    def put1(t):
        j, q = tiles[t]
        n = CH[j][1] - CH[j][0]
        c0 = unit(j, q) * 256
        return pltpu.make_async_copy(ob1.at[t % NB1, :, :n * 256], dw1_ref.at[:, c0:c0 + n * 256], so1.at[t % NB1])

    loads[0].wait()
    loads[1].wait()
    for t, (j, q) in enumerate(tiles):
        if t >= NB2:
            put2(t - NB2).wait()
        for i, a in enumerate(range(*CH[j])):
            ob2[t % NB2, i * 128:(i + 1) * 128] = dot(m_ref[q, a].T, d_ref[...])
        put2(t).start()
        if t == 0:
            xt[...] = x_ref[...].T
    loads[2].wait()
    for t, (j, q) in enumerate(tiles):
        if t >= NB1:
            put1(t - NB1).wait()
        for i, a in enumerate(range(*CH[j])):
            ob1[t % NB1, :, i * 256:(i + 1) * 256] = dot(xt[...], du_ref[q, a])
        put1(t).start()
    loads[3].wait()
    loads[4].wait()
    dy = dy_ref[...].astype(F32)
    y_ref[...] = (gam_ref[...] * nrm_ref[...] + beta_ref[...]).astype(BF)
    db2_ref[...] = jnp.sum(dr_ref[...], axis=0, keepdims=True)
    dgam_ref[...] = jnp.sum(dy * nrm_ref[...], axis=0, keepdims=True)
    dbeta_ref[...] = jnp.sum(dy, axis=0, keepdims=True)
    for i in range(4 * NU):
        db1_ref[:, i * 256:(i + 1) * 256] = db1_in[i]
    last = len(tiles)
    for t in range(last - NB2, last):
        put2(t).wait()
    for t in range(last - NB1, last):
        put1(t).wait()


def grads_call(m, du, d, nrm, dr, db1, x, gam, beta, dy):
    outs = [sds((H, 4 * NU * 256), F32), sds((4 * NU * 128, H), F32), sds((T, H), BF), sds((1, 4 * NU * 256), F32),
            sds((1, H), F32), sds((1, H), F32), sds((1, H), F32)]
    return pl.pallas_call(
        grads_kernel, out_shape=outs, name="grads",
        in_specs=[ANY] * 5 + [VMEM] * 5, out_specs=[ANY, ANY] + [VMEM] * 5,
        scratch_shapes=[pltpu.VMEM((4, NU, T, 128), BF), pltpu.VMEM((4, NU, T, 256), BF), pltpu.VMEM((T, H), BF),
                        pltpu.VMEM((T, H), F32), pltpu.VMEM((T, H), F32),
                        pltpu.VMEM((NB2, 256, H), F32), pltpu.VMEM((NB1, H, 512), F32), pltpu.VMEM((H, T), BF),
                        pltpu.SemaphoreType.DMA((5,)), pltpu.SemaphoreType.DMA((NB2,)), pltpu.SemaphoreType.DMA((NB1,))],
        compiler_params=pltpu.CompilerParams(vmem_limit_bytes=VLIM),
        cost_estimate=pl.CostEstimate(flops=4 * 10 ** 9, bytes_accessed=66 << 20, transcendentals=0),
    )(m, du, d, nrm, dr, db1, x, gam, beta, dy)


def solution(mesh):
    data_spec = P('dp', 'hd')
    hid_spec = P('hd')
    in_specs = (data_spec, P('hd', 'ff'), P('ff'), P('ff', 'hd'), hid_spec, hid_spec, hid_spec, data_spec)
    out_specs = (data_spec, data_spec, P(('dp', 'hd'), 'ff'), P(('dp', 'ff'), 'hd'), P(('dp', 'ff')), P(('dp', 'hd')), P(('dp', 'hd')), P(('dp', 'hd')))

    def device_step(x, w1, b1, w2, b2, gam, beta, dy):
        b2, gam, beta = (a.reshape(1, H) for a in (b2, gam, beta))
        m, du, d, dr, nrm, db1, dxp = comm_call(x, w1, b1.reshape(4 * NU, 1, 256), w2, b2, gam, dy)
        dxr = lax.ppermute(dxp, 'ff', [(0, 1), (1, 0)])
        dw1, dw2, y, db1, db2, dgam, dbeta = grads_call(m, du, d, nrm, dr, db1, x, gam, beta, dy)
        dx = (ALPHA * dr + (dxp.astype(F32) + dxr.astype(F32))).astype(BF)
        return y, dx, dw1, dw2, db1.reshape(-1), db2.reshape(-1), dgam.reshape(-1), dbeta.reshape(-1)

    return jax.shard_map(device_step, mesh=mesh, in_specs=in_specs, out_specs=out_specs, check_vma=False)
```

```python
import functools
import math
import jax
import jax.numpy as jnp
from jax import lax
from jax.experimental import pallas as pl
from jax.experimental.pallas import tpu as pltpu
from jax.sharding import PartitionSpec as P

PAIR = 128
ALPHA = math.sqrt(140.0)
LN_EPS = 1e-5
C0 = math.sqrt(2.0 / math.pi)
C1 = 0.044715
MESH = pl.DeviceIdType.MESH
F32 = jnp.float32
BF = jnp.bfloat16
T = 128
H = 1024
NU = 10
CH = ((0, 1), (1, 3), (3, 5), (5, 7), (7, 9), (9, 10))
NC = len(CH)
COMM_LIM = 48 * 1024 * 1024
GRADS_LIM = 28 * 1024 * 1024

VMEM = pl.BlockSpec(memory_space=pltpu.VMEM)
ANY = pl.BlockSpec(memory_space=pl.ANY)
HBM = pl.BlockSpec(memory_space=pltpu.HBM)


def sds(shape, dtype):
    return jax.ShapeDtypeStruct(shape, dtype)


def dot(a, b):
    return jnp.dot(a, b, preferred_element_type=F32)


def gelu(g):
    t = jnp.tanh(C0 * (g + C1 * (g * g * g)))
    return g * (0.5 * (1.0 + t))


def gelu_both(g):
    g2 = g * g
    t = jnp.tanh(C0 * (g + C1 * (g2 * g)))
    cdf = 0.5 * (1.0 + t)
    slope = cdf + (0.5 * g) * (1.0 - t * t) * (C0 * (1.0 + (3.0 * C1) * g2))
    return g * cdf, slope


def grad_u(u, dm):
    u = u.astype(F32)
    v, g = u[:, :PAIR], u[:, PAIR:]
    val, slope = gelu_both(g)
    return jnp.concatenate([dm * val, dm * v * slope], axis=1)


def places():
    h = lax.axis_index("hd")
    y = lax.axis_index("ff")
    c = lax.rem(h, 2)
    sib = h + 1 - 2 * c
    xn = lax.rem(h + 2, 4)
    xs = lax.rem(sib + 2, 4)
    return h, y, c, sib, xn, xs


def remote(src, dst, sems, k, dev):
    return pltpu.make_async_remote_copy(src_ref=src, dst_ref=dst, send_sem=sems[0].at[k], recv_sem=sems[1].at[k],
                                        device_id=dev, device_id_type=MESH)


def unit(j, q):
    u0, u1 = CH[j]
    return 4 * u0 + q * (u1 - u0)


def aligned(start, size, tile):
    return pl.ds(pl.multiple_of(start * tile, tile), size * tile)


N_SEM = {"ud": 2 * NC, "ux": NC, "mx": NC, "md": NC, "mf": NC, "gx": NC, "gd": NC, "gf": NC, "fy": 2, "st": 3,
         "dd": 2 * NC, "dx": NC, "df": 2 * NC}
SEM_NAMES = list(N_SEM)


def comm_kernel(x_hbm, w1_ref, b1_hbm, w2_ref, b2_hbm, gam_hbm, dy_hbm,
                m_ref, du_ref, d_ref, dr_ref, nrm_ref, db1_ref, dxp_ref,
                x_ref, b1_ref, b2_ref, gam_ref, dy_ref, w1b, w2b, ub, rb, xsb, xrb, facc, fs, fr, stb, dmb, dmr, dsum, dxr, u_ref, dmf, acc,
                ls0, ls1, ls2, *sem_list):
    sems = {n: (sem_list[2 * i], sem_list[2 * i + 1]) for i, n in enumerate(SEM_NAMES)}
    h, y, c, sib, xn, xs = places()
    dev_sib, dev_x, dev_xs, dev_y = (0, y, sib), (0, y, xn), (0, y, xs), (0, 1 - y, h)
    order = [xs, xn, sib, h]

    def w1_load(j, k):
        u0, u1 = CH[j]
        n = u1 - u0
        return pltpu.make_async_copy(w1_ref.at[:, aligned(unit(j, order[k]), n, 256)], w1b.at[k, :, u0 * 256:u1 * 256],
                                     ls1.at[j, k])

    def w2_load(j):
        rows = slice(4 * 128 * CH[j][0], 4 * 128 * CH[j][1])
        return pltpu.make_async_copy(w2_ref.at[rows, :], w2b.at[rows, :], ls2.at[j])

    ins = [pltpu.make_async_copy(a, b, ls0.at[i]) for i, (a, b) in enumerate(
        ((x_hbm, x_ref), (b1_hbm, b1_ref), (b2_hbm, b2_ref), (gam_hbm, gam_ref), (dy_hbm, dy_ref)))]
    bar = pltpu.get_barrier_semaphore()
    for dev in (dev_sib, dev_x, dev_xs, dev_y):
        pl.semaphore_signal(bar, inc=1, device_id=dev, device_id_type=MESH)
    ins[0].start()
    for j in range(NC + 1):
        for k in (0, 1):
            if j < NC:
                w1_load(j, k).start()
        for k in (2, 3):
            if j > 0:
                w1_load(j - 1, k).start()
    for cp in ins[1:]:
        cp.start()
    ins[0].wait()

    live = []

    def send(src, dst, name, k, dev):
        cp = remote(src, dst, sems[name], k, dev)
        cp.start()
        live.append(cp)
        return cp

    def u_part(j, ks):
        u0, u1 = CH[j]
        us = slice(u0, u1)
        for k in ks:
            w1_load(j, k).wait()
            r = dot(x_ref[...], w1b[k, :, u0 * 256:u1 * 256]).astype(BF)
            for i in range(u1 - u0):
                ub[k, u0 + i] = r[:, i * 256:(i + 1) * 256]
            if j == 0 and k == 1:
                pl.semaphore_wait(bar, 4)
                c_ud[j, 1] = send(ub.at[0, us], rb.at[1, us], "ud", 2 * j + 1, dev_sib)
            if j > 0 and k == 0:
                c_ud[j, 1] = send(ub.at[0, us], rb.at[1, us], "ud", 2 * j + 1, dev_sib)
            if k == 2:
                c_ud[j, 0] = send(ub.at[2, us], rb.at[0, us], "ud", 2 * j, dev_sib)

    def ux(j):
        u_part(j, (0, 1))

    def uo(j):
        u_part(j, (2, 3))

    def s1(j):
        us = slice(*CH[j])
        c_ud[j, 1].wait_recv()
        xsb[us] = (ub[1, us].astype(F32) + rb[1, us].astype(F32)).astype(BF)
        c_ux[j] = send(xsb.at[us], xrb.at[us], "ux", j, dev_x)

    def s2(j):
        u0, u1 = CH[j]
        us = slice(u0, u1)
        c_ud[j, 0].wait_recv()
        c_ux[j].wait_recv()
        for i in range(u1 - u0):
            a = u0 + i
            u = ub[3, a].astype(F32) + rb[0, a].astype(F32) + xrb[a].astype(F32) + b1_ref[unit(j, h) + i]
            u = u.astype(BF)
            u_ref[h, a] = u
            u = u.astype(F32)
            m_ref[h, a] = (u[:, :PAIR] * gelu(u[:, PAIR:])).astype(BF)
        c_mx[j] = send(m_ref.at[h, us], m_ref.at[h, us], "mx", j, dev_x)
        c_md[j] = send(m_ref.at[h, us], m_ref.at[h, us], "md", j, dev_sib)

    def s3(j):
        us = slice(*CH[j])
        c_mx[j].wait_recv()
        c_mf[j] = send(m_ref.at[xn, us], m_ref.at[xn, us], "mf", j, dev_sib)

    def s4(j):
        u0, u1 = CH[j]
        c_md[j].wait_recv()
        c_mf[j].wait_recv()
        w2_load(j).wait()
        m = jnp.concatenate([m_ref[q, a] for q in range(4) for a in range(u0, u1)], axis=1)
        for n in range(2):
            cols = slice(n * 512, (n + 1) * 512)
            part = dot(m, w2b[4 * 128 * u0:4 * 128 * u1, cols])
            if j > 0:
                part = facc[:, cols] + part
            if j < NC - 1:
                facc[:, cols] = part
            else:
                fs[n] = part.astype(BF)
                c_fy.append(send(fs.at[n], fr.at[n], "fy", n, dev_y))

    def gather_u(j):
        us = slice(*CH[j])
        c_gx[j] = send(u_ref.at[h, us], u_ref.at[h, us], "gx", j, dev_x)
        c_gd[j] = send(u_ref.at[h, us], u_ref.at[h, us], "gd", j, dev_sib)

    def forward_u(j):
        us = slice(*CH[j])
        c_gx[j].wait_recv()
        c_gf[j] = send(u_ref.at[xn, us], u_ref.at[xn, us], "gf", j, dev_sib)

    c_ud, c_ux, c_mx, c_md, c_mf, c_fy, c_gx, c_gd, c_gf = {}, {}, {}, {}, {}, [], {}, {}, {}
    ux(0)
    ux(1)
    s1(0)
    uo(0)
    ux(2)
    s1(1)
    uo(1)
    ux(3)
    s1(2)
    for j in range(NC):
        w2_load(j).start()
    uo(2)
    ux(4)
    s1(3)
    ins[1].wait()
    s2(0)
    ux(5)
    s1(4)
    uo(3)
    s1(5)
    uo(4)
    s2(1)
    uo(5)
    s2(2)
    s2(3)
    s2(4)
    s3(0)
    s4(0)
    s2(5)
    for j in range(NC):
        gather_u(j)
    for j in range(1, NC):
        s3(j)
        if j > 1:
            s4(j - 1)
    s4(NC - 1)
    for cp in ins[2:]:
        cp.wait()

    for n in range(2):
        cols = slice(n * 512, (n + 1) * 512)
        c_fy[n].wait_recv()
        f = fs[n].astype(F32) + fr[n].astype(F32)
        nrm_ref[:, cols] = ALPHA * x_ref[:, cols].astype(F32) + f + b2_ref[:, cols]
    r = nrm_ref[...]
    gdy = dy_ref[...].astype(F32) * gam_ref[...]
    m_loc = jnp.sum(r, axis=1, keepdims=True) * (1.0 / H)
    cen = r - m_loc
    m2 = jnp.sum(cen * cen, axis=1, keepdims=True)
    sg = jnp.sum(gdy, axis=1, keepdims=True)
    cg = jnp.sum(gdy * cen, axis=1, keepdims=True)
    lane = lax.broadcasted_iota(jnp.int32, (T, 128), 1)
    pack = jnp.where(lane == 0, m_loc, jnp.where(lane == 1, m2, jnp.where(lane == 2, sg, cg)))
    stb[h] = pack.T[0:8]
    c_st = [send(stb.at[h], stb.at[h], "st", i, dev) for i, dev in enumerate((dev_sib, dev_x, dev_xs))]
    for cp in c_st:
        cp.wait_recv()
    st = [stb[i] for i in range(4)]
    mu = ((st[0][0:1] + st[1][0:1]) + (st[2][0:1] + st[3][0:1])) * 0.25
    m2t = jnp.zeros_like(mu)
    sgt = jnp.zeros_like(mu)
    cgt = jnp.zeros_like(mu)
    for i in range(4):
        delta = st[i][0:1] - mu
        m2t += st[i][1:2] + (H * delta) * delta
        sgt += st[i][2:3]
        cgt += st[i][3:4] + delta * st[i][2:3]
    rho = lax.rsqrt(m2t * (1.0 / (4 * H)) + LN_EPS)
    rows = jnp.concatenate([mu, rho, sgt * (1.0 / (4 * H)), cgt * rho * (1.0 / (4 * H)), jnp.zeros((124, T), F32)], axis=0)
    colst = rows.T
    mu_c, rho_c, mg_c, mgr_c = (colst[:, i:i + 1] for i in range(4))
    nrm = (r - mu_c) * rho_c
    dr = rho_c * (gdy - mg_c - nrm * mgr_c)
    nrm_ref[...] = nrm
    dr_ref[...] = dr
    d_ref[...] = dr.astype(BF)
    d_t = dr.T.astype(BF)

    c_dd, c_dx, c_df = {}, {}, {}
    mine, mine_k, theirs, theirs_k = (h, xn), (3, 1), (sib, xs), (2, 0)

    def dm_part(j):
        u0, u1 = CH[j]
        n = u1 - u0
        for i, q in enumerate(theirs + mine):
            r = dot(w2b[aligned(unit(j, q), n, 128), :], d_t).T.astype(BF)
            for a in range(n):
                dmb[i, u0 + a] = r[:, a * 128:(a + 1) * 128]
            if i < 2:
                c_dd[j, i] = send(dmb.at[i, u0:u1], dmr.at[i, u0:u1], "dd", 2 * j + i, dev_sib)

    def dm_sum(j):
        us = slice(*CH[j])
        for i in range(2):
            c_dd[j, i].wait_recv()
            dsum[i, us] = (dmb[2 + i, us].astype(F32) + dmr[i, us].astype(F32)).astype(BF)
        c_dx[j] = send(dsum.at[:, us], dxr.at[:, us], "dx", j, dev_x)

    def dm_full(j):
        us = slice(*CH[j])
        c_dx[j].wait_recv()
        for i in range(2):
            q = mine[i]
            dmf[q, us] = (dsum[i, us].astype(F32) + dxr[1 - i, us].astype(F32)).astype(BF)
            c_df[j, i] = send(dmf.at[q, us], dmf.at[q, us], "df", 2 * j + i, dev_sib)

    def grads(j, qs, ks, first):
        u0, u1 = CH[j]
        for q, k in zip(qs, ks):
            parts = []
            for a in range(u0, u1):
                du_f = grad_u(u_ref[q, a], dmf[q, a].astype(F32))
                db1_ref[unit(j, q) + a - u0] = jnp.sum(du_f, axis=0, keepdims=True)
                du_ref[q, a] = du_f.astype(BF)
                parts.append(du_f)
            du_t = jnp.concatenate(parts, axis=1).T.astype(BF)
            part = dot(w1b[k, :, u0 * 256:u1 * 256], du_t)
            acc[...] = part if first else acc[...] + part
            first = False

    def grads_mine(j):
        dm_full(j)
        grads(j, mine, mine_k, j == 0)

    def grads_theirs(j):
        for i in range(2):
            c_df[j, i].wait_recv()
        grads(j, theirs, theirs_k, False)

    dm_part(0)
    dm_part(1)
    dm_sum(0)
    for j in range(2, NC):
        dm_part(j)
        dm_sum(j - 1)
        forward_u(j - 2)
    dm_sum(NC - 1)
    forward_u(NC - 2)
    forward_u(NC - 1)
    for cp in list(c_gd.values()) + list(c_gf.values()):
        cp.wait_recv()
    for j in range(NC):
        grads_mine(j)
        grads_theirs(j)
    dxp_ref[...] = acc[...].T.astype(BF)
    for cp in live:
        cp.wait_send()


def comm_call(x, w1, b1, w2, b2, gam, dy):
    scratch = [pltpu.VMEM((T, H), BF), pltpu.VMEM((4 * NU, 1, 256), F32), pltpu.VMEM((1, H), F32), pltpu.VMEM((1, H), F32),
               pltpu.VMEM((T, H), BF),
               pltpu.VMEM((4, H, NU * 256), BF), pltpu.VMEM((4 * NU * 128, H), BF),
               pltpu.VMEM((4, NU, T, 256), BF), pltpu.VMEM((2, NU, T, 256), BF),
               pltpu.VMEM((NU, T, 256), BF), pltpu.VMEM((NU, T, 256), BF),
               pltpu.VMEM((T, H), F32), pltpu.VMEM((2, T, 512), BF), pltpu.VMEM((2, T, 512), BF),
               pltpu.VMEM((4, 8, T), F32),
               pltpu.VMEM((4, NU, T, 128), BF), pltpu.VMEM((2, NU, T, 128), BF),
               pltpu.VMEM((2, NU, T, 128), BF), pltpu.VMEM((2, NU, T, 128), BF),
               pltpu.VMEM((4, NU, T, 256), BF), pltpu.VMEM((4, NU, T, 128), BF), pltpu.VMEM((H, T), F32),
               pltpu.SemaphoreType.DMA((5,)), pltpu.SemaphoreType.DMA((NC, 4)), pltpu.SemaphoreType.DMA((NC,))]
    for n in SEM_NAMES:
        scratch += [pltpu.SemaphoreType.DMA((N_SEM[n],)), pltpu.SemaphoreType.DMA((N_SEM[n],))]
    outs = [sds((4, NU, T, 128), BF), sds((4, NU, T, 256), BF), sds((T, H), BF), sds((T, H), F32), sds((T, H), F32),
            sds((4 * NU, 1, 256), F32), sds((T, H), BF)]
    return pl.pallas_call(
        comm_kernel, out_shape=outs, name="comm",
        in_specs=[HBM] * 7, out_specs=[VMEM] * 7, scratch_shapes=scratch,
        compiler_params=pltpu.CompilerParams(collective_id=0, has_side_effects=True, vmem_limit_bytes=COMM_LIM),
        cost_estimate=pl.CostEstimate(flops=8 * 10 ** 9, bytes_accessed=32 << 20, transcendentals=0),
    )(x, w1, b1, w2, b2, gam, dy)


NB2 = 6
NB1 = 6


def grads_kernel(m_ref, du_ref, d_ref, nrm_ref, dr_ref, db1_in, x_ref, gam_ref, beta_ref, dy_ref,
                 dw1_ref, dw2_ref, y_ref, db1_ref, db2_ref, dgam_ref, dbeta_ref,
                 ob2, ob1, xt, yb, db1b, so2, so1, so0):
    tiles = [(j, q) for j in range(NC) for q in range(4)]

    def put2(t):
        j, q = tiles[t]
        n = CH[j][1] - CH[j][0]
        r0 = unit(j, q) * 128
        return pltpu.make_async_copy(ob2.at[t % NB2, :n * 128], dw2_ref.at[r0:r0 + n * 128, :], so2.at[t % NB2])

    def put1(t):
        j, q = tiles[t]
        n = CH[j][1] - CH[j][0]
        c0 = unit(j, q) * 256
        return pltpu.make_async_copy(ob1.at[t % NB1, :, :n * 256], dw1_ref.at[:, c0:c0 + n * 256], so1.at[t % NB1])

    small = [pltpu.make_async_copy(yb, y_ref, so0.at[0]), pltpu.make_async_copy(db1b, db1_ref, so0.at[1])]
    for t, (j, q) in enumerate(tiles):
        if t >= NB2:
            put2(t - NB2).wait()
        for i, a in enumerate(range(*CH[j])):
            ob2[t % NB2, i * 128:(i + 1) * 128] = dot(m_ref[q, a].T, d_ref[...])
        put2(t).start()
        if t == 6:
            xt[...] = x_ref[...].T
        if t == 8:
            yb[...] = (gam_ref[...] * nrm_ref[...] + beta_ref[...]).astype(BF)
            for i in range(4 * NU):
                db1b[:, i * 256:(i + 1) * 256] = db1_in[i]
            for cp in small:
                cp.start()
        if t == 10:
            dy = dy_ref[...].astype(F32)
            db2_ref[...] = jnp.sum(dr_ref[...], axis=0, keepdims=True)
            dgam_ref[...] = jnp.sum(dy * nrm_ref[...], axis=0, keepdims=True)
            dbeta_ref[...] = jnp.sum(dy, axis=0, keepdims=True)
    for t, (j, q) in enumerate(tiles):
        if t >= NB1:
            put1(t - NB1).wait()
        for i, a in enumerate(range(*CH[j])):
            ob1[t % NB1, :, i * 256:(i + 1) * 256] = dot(xt[...], du_ref[q, a])
        put1(t).start()
    last = len(tiles)
    for t in range(last - NB2, last):
        put2(t).wait()
    for cp in small:
        cp.wait()
    for t in range(last - NB1, last):
        put1(t).wait()


def grads_call(m, du, d, nrm, dr, db1, x, gam, beta, dy):
    outs = [sds((H, 4 * NU * 256), F32), sds((4 * NU * 128, H), F32), sds((T, H), BF), sds((1, 4 * NU * 256), F32),
            sds((1, H), F32), sds((1, H), F32), sds((1, H), F32)]
    return pl.pallas_call(
        grads_kernel, out_shape=outs, name="grads",
        in_specs=[VMEM] * 10, out_specs=[HBM] * 4 + [VMEM] * 3,
        scratch_shapes=[pltpu.VMEM((NB2, 256, H), F32), pltpu.VMEM((NB1, H, 512), F32), pltpu.VMEM((H, T), BF),
                        pltpu.VMEM((T, H), BF), pltpu.VMEM((1, 4 * NU * 256), F32),
                        pltpu.SemaphoreType.DMA((NB2,)), pltpu.SemaphoreType.DMA((NB1,)), pltpu.SemaphoreType.DMA((2,))],
        compiler_params=pltpu.CompilerParams(vmem_limit_bytes=GRADS_LIM),
        cost_estimate=pl.CostEstimate(flops=4 * 10 ** 9, bytes_accessed=66 << 20, transcendentals=0),
    )(m, du, d, nrm, dr, db1, x, gam, beta, dy)


def solution(mesh):
    data_spec = P('dp', 'hd')
    hid_spec = P('hd')
    in_specs = (data_spec, P('hd', 'ff'), P('ff'), P('ff', 'hd'), hid_spec, hid_spec, hid_spec, data_spec)
    out_specs = (data_spec, data_spec, P(('dp', 'hd'), 'ff'), P(('dp', 'ff'), 'hd'), P(('dp', 'ff')), P(('dp', 'hd')), P(('dp', 'hd')), P(('dp', 'hd')))

    def device_step(x, w1, b1, w2, b2, gam, beta, dy):
        b2, gam, beta = (a.reshape(1, H) for a in (b2, gam, beta))
        hbm = [pltpu.with_memory_space_constraint(a, pltpu.HBM) for a in (x, w1, b1.reshape(4 * NU, 1, 256), w2, b2, gam, dy)]
        m, du, d, dr, nrm, db1, dxp = comm_call(*hbm)
        dxr = lax.ppermute(dxp, 'ff', [(0, 1), (1, 0)])
        dw1, dw2, y, db1, db2, dgam, dbeta = grads_call(m, du, d, nrm, dr, db1, x, gam, beta, dy)
        dx = (ALPHA * dr + (dxp.astype(F32) + dxr.astype(F32))).astype(BF)
        return y, dx, dw1, dw2, db1.reshape(-1), db2.reshape(-1), dgam.reshape(-1), dbeta.reshape(-1)

    return jax.shard_map(device_step, mesh=mesh, in_specs=in_specs, out_specs=out_specs, check_vma=False)
```

```python
import functools
import math
import jax
import jax.numpy as jnp
from jax import lax
from jax.experimental import pallas as pl
from jax.experimental.pallas import tpu as pltpu
from jax.sharding import PartitionSpec as P

PAIR = 128
ALPHA = math.sqrt(140.0)
LN_EPS = 1e-5
C0 = math.sqrt(2.0 / math.pi)
C1 = 0.044715
MESH = pl.DeviceIdType.MESH
F32 = jnp.float32
BF = jnp.bfloat16
T = 128
H = 1024
NU = 10
CH = ((0, 1), (1, 3), (3, 5), (5, 7), (7, 9), (9, 10))
NC = len(CH)
COMM_LIM = 48 * 1024 * 1024
GRADS_LIM = 28 * 1024 * 1024

VMEM = pl.BlockSpec(memory_space=pltpu.VMEM)
ANY = pl.BlockSpec(memory_space=pl.ANY)
HBM = pl.BlockSpec(memory_space=pltpu.HBM)


def sds(shape, dtype):
    return jax.ShapeDtypeStruct(shape, dtype)


def dot(a, b):
    return jnp.dot(a, b, preferred_element_type=F32)


def gelu_both(g):
    g2 = g * g
    t = jnp.tanh(C0 * (g + C1 * (g2 * g)))
    cdf = 0.5 * (1.0 + t)
    slope = cdf + (0.5 * g) * (1.0 - t * t) * (C0 * (1.0 + (3.0 * C1) * g2))
    return g * cdf, slope


def places():
    h = lax.axis_index("hd")
    y = lax.axis_index("ff")
    c = lax.rem(h, 2)
    sib = h + 1 - 2 * c
    xn = lax.rem(h + 2, 4)
    xs = lax.rem(sib + 2, 4)
    return h, y, c, sib, xn, xs


def remote(src, dst, sems, k, dev):
    return pltpu.make_async_remote_copy(src_ref=src, dst_ref=dst, send_sem=sems[0].at[k], recv_sem=sems[1].at[k],
                                        device_id=dev, device_id_type=MESH)


def unit(j, q):
    u0, u1 = CH[j]
    return 4 * u0 + q * (u1 - u0)


def aligned(start, size, tile):
    return pl.ds(pl.multiple_of(start * tile, tile), size * tile)


N_SEM = {"ud": 2 * NC, "ux": NC, "mx": NC, "md": NC, "mf": NC, "gx": NC, "gd": NC, "gf": NC, "fy": 2, "st": 3,
         "dd": 2 * NC, "dx": NC, "df": 2 * NC}
SEM_NAMES = list(N_SEM)


def comm_kernel(x_hbm, w1_ref, b1_hbm, w2_ref, b2_hbm, gam_hbm, dy_hbm,
                m_ref, du_ref, d_ref, dr_ref, nrm_ref, db1_ref, dxp_ref,
                x_ref, b1_ref, b2_ref, gam_ref, dy_ref, w1b, w2b, ub, rb, xsb, xrb, fs, fr, stb, dmb, dmr, u_ref, dmf, pr_ref, acc,
                ls0, ls1, ls2, *sem_list):
    sems = {n: (sem_list[2 * i], sem_list[2 * i + 1]) for i, n in enumerate(SEM_NAMES)}
    h, y, c, sib, xn, xs = places()
    dev_sib, dev_x, dev_xs, dev_y = (0, y, sib), (0, y, xn), (0, y, xs), (0, 1 - y, h)
    order = [xs, xn, sib, h]

    def w1_load(j, k):
        u0, u1 = CH[j]
        n = u1 - u0
        return pltpu.make_async_copy(w1_ref.at[:, aligned(unit(j, order[k]), n, 256)], w1b.at[k, :, u0 * 256:u1 * 256],
                                     ls1.at[j, k])

    def w2_load(j):
        rows = slice(4 * 128 * CH[j][0], 4 * 128 * CH[j][1])
        return pltpu.make_async_copy(w2_ref.at[rows, :], w2b.at[rows, :], ls2.at[j])

    ins = [pltpu.make_async_copy(a, b, ls0.at[i]) for i, (a, b) in enumerate(
        ((x_hbm, x_ref), (b1_hbm, b1_ref), (b2_hbm, b2_ref), (gam_hbm, gam_ref), (dy_hbm, dy_ref)))]
    bar = pltpu.get_barrier_semaphore()
    for dev in (dev_sib, dev_x, dev_xs, dev_y):
        pl.semaphore_signal(bar, inc=1, device_id=dev, device_id_type=MESH)
    ins[0].start()
    for j in range(NC + 1):
        for k in (0, 1):
            if j < NC:
                w1_load(j, k).start()
        for k in (2, 3):
            if j > 0:
                w1_load(j - 1, k).start()
    for cp in ins[1:]:
        cp.start()
    ins[0].wait()

    live = []

    def send(src, dst, name, k, dev):
        cp = remote(src, dst, sems[name], k, dev)
        cp.start()
        live.append(cp)
        return cp

    def u_parts(*slabs):
        for j, k in slabs:
            w1_load(j, k).wait()
        for j, k in slabs:
            u0, u1 = CH[j]
            r = dot(x_ref[...], w1b[k, :, u0 * 256:u1 * 256]).astype(BF)
            for i in range(u1 - u0):
                ub[k, u0 + i] = r[:, i * 256:(i + 1) * 256]
        if slabs[0] == (0, 0):
            pl.semaphore_wait(bar, 4)
        for j, k in slabs:
            us = slice(*CH[j])
            if k == 0:
                c_ud[j, 1] = send(ub.at[0, us], rb.at[1, us], "ud", 2 * j + 1, dev_sib)
            if k == 2:
                c_ud[j, 0] = send(ub.at[2, us], rb.at[0, us], "ud", 2 * j, dev_sib)

    def s1(j):
        us = slice(*CH[j])
        c_ud[j, 1].wait_recv()
        xsb[us] = (ub[1, us].astype(F32) + rb[1, us].astype(F32)).astype(BF)
        c_ux[j] = send(xsb.at[us], xrb.at[us], "ux", j, dev_x)

    def s2(j):
        u0, u1 = CH[j]
        us = slice(u0, u1)
        c_ud[j, 0].wait_recv()
        c_ux[j].wait_recv()
        for i in range(u1 - u0):
            a = u0 + i
            u = ub[3, a].astype(F32) + rb[0, a].astype(F32) + xrb[a].astype(F32) + b1_ref[unit(j, h) + i]
            u = u.astype(BF)
            u_ref[h, a] = u
            u = u.astype(F32)
            val, slope = gelu_both(u[:, PAIR:])
            m_ref[h, a] = (u[:, :PAIR] * val).astype(BF)
            pr_ref[h, a, :, :PAIR] = val
            pr_ref[h, a, :, PAIR:] = u[:, :PAIR] * slope
        c_mx[j] = send(m_ref.at[h, us], m_ref.at[h, us], "mx", j, dev_x)
        c_md[j] = send(m_ref.at[h, us], m_ref.at[h, us], "md", j, dev_sib)

    def s3(j):
        us = slice(*CH[j])
        c_mx[j].wait_recv()
        c_mf[j] = send(m_ref.at[xn, us], m_ref.at[xn, us], "mf", j, dev_sib)

    def s4(j):
        u0, u1 = CH[j]
        c_md[j].wait_recv()
        c_mf[j].wait_recv()
        w2_load(j).wait()
        m = jnp.concatenate([m_ref[q, a] for q in range(4) for a in range(u0, u1)], axis=1)
        for n in range(2):
            cols = slice(n * 512, (n + 1) * 512)
            part = dot(m, w2b[4 * 128 * u0:4 * 128 * u1, cols])
            if j > 0:
                part = nrm_ref[:, cols] + part
            if j < NC - 1:
                nrm_ref[:, cols] = part
            else:
                fs[n] = part.astype(BF)
                c_fy.append(send(fs.at[n], fr.at[n], "fy", n, dev_y))

    def gather_u(j):
        us = slice(*CH[j])
        c_gx[j] = send(u_ref.at[h, us], u_ref.at[h, us], "gx", j, dev_x)
        c_gd[j] = send(u_ref.at[h, us], u_ref.at[h, us], "gd", j, dev_sib)

    def forward_u(j):
        us = slice(*CH[j])
        c_gx[j].wait_recv()
        c_gf[j] = send(u_ref.at[xn, us], u_ref.at[xn, us], "gf", j, dev_sib)
        products(j, xn)

    def products(j, q):
        for a in range(*CH[j]):
            u = u_ref[q, a].astype(F32)
            val, slope = gelu_both(u[:, PAIR:])
            pr_ref[q, a, :, :PAIR] = val
            pr_ref[q, a, :, PAIR:] = u[:, :PAIR] * slope

    def products_sib(j):
        c_gd[j].wait_recv()
        c_gf[j].wait_recv()
        products(j, sib)
        products(j, xs)

    c_ud, c_ux, c_mx, c_md, c_mf, c_fy, c_gx, c_gd, c_gf = {}, {}, {}, {}, {}, [], {}, {}, {}
    u_parts((0, 0), (0, 1))
    u_parts((1, 0), (1, 1), (0, 2), (0, 3))
    s1(0)
    u_parts((2, 0), (2, 1), (1, 2), (1, 3))
    s1(1)
    u_parts((3, 0), (3, 1), (2, 2), (2, 3))
    s1(2)
    for j in range(NC):
        w2_load(j).start()
    u_parts((4, 0), (4, 1), (3, 2), (3, 3))
    s1(3)
    ins[1].wait()
    s2(0)
    u_parts((5, 0), (5, 1), (4, 2), (4, 3))
    s1(4)
    u_parts((5, 2), (5, 3))
    s1(5)
    s2(1)
    s2(2)
    s2(3)
    s2(4)
    s3(0)
    s4(0)
    s2(5)
    for j in range(NC):
        gather_u(j)
    for j in range(1, NC):
        s3(j)
        if j > 1:
            s4(j - 1)
    s4(NC - 1)
    for cp in ins[2:]:
        cp.wait()

    for j in range(3):
        forward_u(j)
    for n in range(2):
        cols = slice(n * 512, (n + 1) * 512)
        c_fy[n].wait_recv()
        f = fs[n].astype(F32) + fr[n].astype(F32)
        nrm_ref[:, cols] = ALPHA * x_ref[:, cols].astype(F32) + f + b2_ref[:, cols]
    r = nrm_ref[...]
    gdy = dy_ref[...].astype(F32) * gam_ref[...]
    m_loc = jnp.sum(r, axis=1, keepdims=True) * (1.0 / H)
    cen = r - m_loc
    m2 = jnp.sum(cen * cen, axis=1, keepdims=True)
    sg = jnp.sum(gdy, axis=1, keepdims=True)
    cg = jnp.sum(gdy * cen, axis=1, keepdims=True)
    lane = lax.broadcasted_iota(jnp.int32, (T, 128), 1)
    pack = jnp.where(lane == 0, m_loc, jnp.where(lane == 1, m2, jnp.where(lane == 2, sg, cg)))
    stb[h] = pack.T[0:8]
    c_st = [send(stb.at[h], stb.at[h], "st", i, dev) for i, dev in enumerate((dev_sib, dev_x, dev_xs))]
    forward_u(3)
    for j in range(3):
        products_sib(j)
    for cp in c_st:
        cp.wait_recv()
    st = [stb[i] for i in range(4)]
    mu = ((st[0][0:1] + st[1][0:1]) + (st[2][0:1] + st[3][0:1])) * 0.25
    m2t = jnp.zeros_like(mu)
    sgt = jnp.zeros_like(mu)
    cgt = jnp.zeros_like(mu)
    for i in range(4):
        delta = st[i][0:1] - mu
        m2t += st[i][1:2] + (H * delta) * delta
        sgt += st[i][2:3]
        cgt += st[i][3:4] + delta * st[i][2:3]
    rho = lax.rsqrt(m2t * (1.0 / (4 * H)) + LN_EPS)
    rows = jnp.concatenate([mu, rho, sgt * (1.0 / (4 * H)), cgt * rho * (1.0 / (4 * H)), jnp.zeros((124, T), F32)], axis=0)
    colst = rows.T
    mu_c, rho_c, mg_c, mgr_c = (colst[:, i:i + 1] for i in range(4))
    nrm = (r - mu_c) * rho_c
    dr = rho_c * (gdy - mg_c - nrm * mgr_c)
    nrm_ref[...] = nrm
    dr_ref[...] = dr
    d_ref[...] = dr.astype(BF)
    d_t = dr.T.astype(BF)

    c_dd, c_dx, c_df = {}, {}, {}
    mine, mine_k, theirs, theirs_k = (h, xn), (3, 1), (sib, xs), (2, 0)

    def dm_part(j):
        u0, u1 = CH[j]
        n = u1 - u0
        for i, q in enumerate(theirs + mine):
            r = dot(w2b[aligned(unit(j, q), n, 128), :], d_t).T.astype(BF)
            for a in range(n):
                dmb[i, u0 + a] = r[:, a * 128:(a + 1) * 128]
            if i == 1:
                for k in range(2):
                    c_dd[j, k] = send(dmb.at[k, u0:u1], dmr.at[k, u0:u1], "dd", 2 * j + k, dev_sib)

    def dm_sum(j):
        us = slice(*CH[j])
        c_ux[j].wait_send()
        live[:] = [cp for cp in live if cp is not c_ux[j]]
        for i in range(2):
            c_dd[j, i].wait_recv()
            xsb[us, :, i * 128:(i + 1) * 128] = (dmb[2 + i, us].astype(F32) + dmr[i, us].astype(F32)).astype(BF)
        c_dx[j] = send(xsb.at[us], xrb.at[us], "dx", j, dev_x)

    def dm_full(j):
        us = slice(*CH[j])
        c_dx[j].wait_recv()
        for i in range(2):
            q = mine[i]
            dmf[q, us] = (xsb[us, :, i * 128:(i + 1) * 128].astype(F32)
                          + xrb[us, :, (1 - i) * 128:(2 - i) * 128].astype(F32)).astype(BF)
        for i in range(2):
            q = mine[i]
            c_df[j, i] = send(dmf.at[q, us], dmf.at[q, us], "df", 2 * j + i, dev_sib)

    def grads(j, qs, ks, first):
        u0, u1 = CH[j]
        for q, k in zip(qs, ks):
            parts = []
            for a in range(u0, u1):
                dm = dmf[q, a].astype(F32)
                du_f = pr_ref[q, a] * jnp.concatenate([dm, dm], axis=1)
                db1_ref[unit(j, q) + a - u0] = jnp.sum(du_f, axis=0, keepdims=True)
                du_ref[q, a] = du_f.astype(BF)
                parts.append(du_f)
            du_t = jnp.concatenate(parts, axis=1).T.astype(BF)
            part = dot(w1b[k, :, u0 * 256:u1 * 256], du_t)
            acc[...] = part if first else acc[...] + part
            first = False

    def grads_mine(j):
        dm_full(j)
        grads(j, mine, mine_k, j == 0)

    def grads_theirs(j):
        for i in range(2):
            c_df[j, i].wait_recv()
        grads(j, theirs, theirs_k, False)

    dm_part(0)
    dm_part(1)
    dm_sum(0)
    dm_part(2)
    dm_sum(1)
    dm_part(3)
    dm_sum(2)
    forward_u(4)
    dm_part(4)
    dm_sum(3)
    forward_u(5)
    dm_part(5)
    dm_sum(4)
    dm_sum(5)
    for j in range(3, NC):
        products_sib(j)
    grads_mine(0)
    for j in range(1, NC):
        grads_theirs(j - 1)
        grads_mine(j)
    grads_theirs(NC - 1)
    dxp_ref[...] = acc[...].T.astype(BF)
    for cp in live:
        cp.wait_send()


def comm_call(x, w1, b1, w2, b2, gam, dy):
    scratch = [pltpu.VMEM((T, H), BF), pltpu.VMEM((4 * NU, 1, 256), F32), pltpu.VMEM((1, H), F32), pltpu.VMEM((1, H), F32),
               pltpu.VMEM((T, H), BF),
               pltpu.VMEM((4, H, NU * 256), BF), pltpu.VMEM((4 * NU * 128, H), BF),
               pltpu.VMEM((4, NU, T, 256), BF), pltpu.VMEM((2, NU, T, 256), BF),
               pltpu.VMEM((NU, T, 256), BF), pltpu.VMEM((NU, T, 256), BF),
               pltpu.VMEM((2, T, 512), BF), pltpu.VMEM((2, T, 512), BF),
               pltpu.VMEM((4, 8, T), F32),
               pltpu.VMEM((4, NU, T, 128), BF), pltpu.VMEM((2, NU, T, 128), BF),
               pltpu.VMEM((4, NU, T, 256), BF), pltpu.VMEM((4, NU, T, 128), BF), pltpu.VMEM((4, NU, T, 256), F32),
               pltpu.VMEM((H, T), F32),
               pltpu.SemaphoreType.DMA((5,)), pltpu.SemaphoreType.DMA((NC, 4)), pltpu.SemaphoreType.DMA((NC,))]
    for n in SEM_NAMES:
        scratch += [pltpu.SemaphoreType.DMA((N_SEM[n],)), pltpu.SemaphoreType.DMA((N_SEM[n],))]
    outs = [sds((4, NU, T, 128), BF), sds((4, NU, T, 256), BF), sds((T, H), BF), sds((T, H), F32), sds((T, H), F32),
            sds((4 * NU, 1, 256), F32), sds((T, H), BF)]
    return pl.pallas_call(
        comm_kernel, out_shape=outs, name="comm",
        in_specs=[HBM] * 7, out_specs=[VMEM] * 7, scratch_shapes=scratch,
        compiler_params=pltpu.CompilerParams(collective_id=0, has_side_effects=True, vmem_limit_bytes=COMM_LIM),
        cost_estimate=pl.CostEstimate(flops=8 * 10 ** 9, bytes_accessed=32 << 20, transcendentals=0),
    )(x, w1, b1, w2, b2, gam, dy)


NB2 = 6
NB1 = 6


def grads_kernel(m_ref, du_ref, d_ref, nrm_ref, dr_ref, db1_in, x_ref, gam_ref, beta_ref, dy_ref,
                 dw1_ref, dw2_ref, y_ref, db1_ref, db2_ref, dgam_ref, dbeta_ref,
                 ob2, ob1, xt, yb, db1b, so2, so1, so0):
    tiles = [(j, q) for j in range(NC) for q in range(4)]

    def put2(t):
        j, q = tiles[t]
        n = CH[j][1] - CH[j][0]
        r0 = unit(j, q) * 128
        return pltpu.make_async_copy(ob2.at[t % NB2, :n * 128], dw2_ref.at[r0:r0 + n * 128, :], so2.at[t % NB2])

    def put1(t):
        j, q = tiles[t]
        n = CH[j][1] - CH[j][0]
        c0 = unit(j, q) * 256
        return pltpu.make_async_copy(ob1.at[t % NB1, :, :n * 256], dw1_ref.at[:, c0:c0 + n * 256], so1.at[t % NB1])

    small = [pltpu.make_async_copy(yb, y_ref, so0.at[0]), pltpu.make_async_copy(db1b, db1_ref, so0.at[1])]
    for t, (j, q) in enumerate(tiles):
        if t >= NB2:
            put2(t - NB2).wait()
        for i, a in enumerate(range(*CH[j])):
            ob2[t % NB2, i * 128:(i + 1) * 128] = dot(m_ref[q, a].T, d_ref[...])
        put2(t).start()
        if t == 6:
            xt[...] = x_ref[...].T
        if t == 8:
            yb[...] = (gam_ref[...] * nrm_ref[...] + beta_ref[...]).astype(BF)
            for i in range(4 * NU):
                db1b[:, i * 256:(i + 1) * 256] = db1_in[i]
            for cp in small:
                cp.start()
        if t == 10:
            dy = dy_ref[...].astype(F32)
            db2_ref[...] = jnp.sum(dr_ref[...], axis=0, keepdims=True)
            dgam_ref[...] = jnp.sum(dy * nrm_ref[...], axis=0, keepdims=True)
            dbeta_ref[...] = jnp.sum(dy, axis=0, keepdims=True)
    for t, (j, q) in enumerate(tiles):
        if t >= NB1:
            put1(t - NB1).wait()
        for i, a in enumerate(range(*CH[j])):
            ob1[t % NB1, :, i * 256:(i + 1) * 256] = dot(xt[...], du_ref[q, a])
        put1(t).start()
    last = len(tiles)
    for t in range(last - NB2, last):
        put2(t).wait()
    for cp in small:
        cp.wait()
    for t in range(last - NB1, last):
        put1(t).wait()


def grads_call(m, du, d, nrm, dr, db1, x, gam, beta, dy):
    outs = [sds((H, 4 * NU * 256), F32), sds((4 * NU * 128, H), F32), sds((T, H), BF), sds((1, 4 * NU * 256), F32),
            sds((1, H), F32), sds((1, H), F32), sds((1, H), F32)]
    return pl.pallas_call(
        grads_kernel, out_shape=outs, name="grads",
        in_specs=[VMEM] * 10, out_specs=[HBM] * 4 + [VMEM] * 3,
        scratch_shapes=[pltpu.VMEM((NB2, 256, H), F32), pltpu.VMEM((NB1, H, 512), F32), pltpu.VMEM((H, T), BF),
                        pltpu.VMEM((T, H), BF), pltpu.VMEM((1, 4 * NU * 256), F32),
                        pltpu.SemaphoreType.DMA((NB2,)), pltpu.SemaphoreType.DMA((NB1,)), pltpu.SemaphoreType.DMA((2,))],
        compiler_params=pltpu.CompilerParams(vmem_limit_bytes=GRADS_LIM),
        cost_estimate=pl.CostEstimate(flops=4 * 10 ** 9, bytes_accessed=66 << 20, transcendentals=0),
    )(m, du, d, nrm, dr, db1, x, gam, beta, dy)


def solution(mesh):
    data_spec = P('dp', 'hd')
    hid_spec = P('hd')
    in_specs = (data_spec, P('hd', 'ff'), P('ff'), P('ff', 'hd'), hid_spec, hid_spec, hid_spec, data_spec)
    out_specs = (data_spec, data_spec, P(('dp', 'hd'), 'ff'), P(('dp', 'ff'), 'hd'), P(('dp', 'ff')), P(('dp', 'hd')), P(('dp', 'hd')), P(('dp', 'hd')))

    def device_step(x, w1, b1, w2, b2, gam, beta, dy):
        b2, gam, beta = (a.reshape(1, H) for a in (b2, gam, beta))
        hbm = [pltpu.with_memory_space_constraint(a, pltpu.HBM) for a in (x, w1, b1.reshape(4 * NU, 1, 256), w2, b2, gam, dy)]
        m, du, d, dr, nrm, db1, dxp = comm_call(*hbm)
        dxr = lax.ppermute(dxp, 'ff', [(0, 1), (1, 0)])
        dw1, dw2, y, db1, db2, dgam, dbeta = grads_call(m, du, d, nrm, dr, db1, x, gam, beta, dy)
        dx = (ALPHA * dr + (dxp.astype(F32) + dxr.astype(F32))).astype(BF)
        return y, dx, dw1, dw2, db1.reshape(-1), db2.reshape(-1), dgam.reshape(-1), dbeta.reshape(-1)

    return jax.shard_map(device_step, mesh=mesh, in_specs=in_specs, out_specs=out_specs, check_vma=False)
```

```python
import functools
import math
import jax
import jax.numpy as jnp
from jax import lax
from jax.experimental import pallas as pl
from jax.experimental.pallas import tpu as pltpu
from jax.sharding import PartitionSpec as P

PAIR = 128
ALPHA = math.sqrt(140.0)
LN_EPS = 1e-5
C0 = math.sqrt(2.0 / math.pi)
C1 = 0.044715
MESH = pl.DeviceIdType.MESH
F32 = jnp.float32
BF = jnp.bfloat16
T = 128
H = 1024
NU = 10
CH = ((0, 1), (1, 3), (3, 5), (5, 7), (7, 9), (9, 10))
NC = len(CH)
COMM_LIM = 48 * 1024 * 1024
GRADS_LIM = 28 * 1024 * 1024

VMEM = pl.BlockSpec(memory_space=pltpu.VMEM)
ANY = pl.BlockSpec(memory_space=pl.ANY)
HBM = pl.BlockSpec(memory_space=pltpu.HBM)


def sds(shape, dtype):
    return jax.ShapeDtypeStruct(shape, dtype)


def dot(a, b):
    return jnp.dot(a, b, preferred_element_type=F32)


def gelu_both(g):
    g2 = g * g
    t = jnp.tanh(C0 * (g + C1 * (g2 * g)))
    cdf = 0.5 * (1.0 + t)
    slope = cdf + (0.5 * g) * (1.0 - t * t) * (C0 * (1.0 + (3.0 * C1) * g2))
    return g * cdf, slope


def places():
    h = lax.axis_index("hd")
    y = lax.axis_index("ff")
    c = lax.rem(h, 2)
    sib = h + 1 - 2 * c
    xn = lax.rem(h + 2, 4)
    xs = lax.rem(sib + 2, 4)
    return h, y, c, sib, xn, xs


def remote(src, dst, sems, k, dev):
    return pltpu.make_async_remote_copy(src_ref=src, dst_ref=dst, send_sem=sems[0].at[k], recv_sem=sems[1].at[k],
                                        device_id=dev, device_id_type=MESH)


def unit(j, q):
    u0, u1 = CH[j]
    return 4 * u0 + q * (u1 - u0)


def aligned(start, size, tile):
    return pl.ds(pl.multiple_of(start * tile, tile), size * tile)


N_SEM = {"ud": 2 * NC, "ux": NC, "mx": NC, "md": NC, "mf": NC, "gx": NC, "gd": NC, "gf": NC, "fy": 2, "st": 3,
         "dd": 2 * NC, "dx": NC, "df": 2 * NC}
SEM_NAMES = list(N_SEM)


def comm_kernel(x_hbm, w1_ref, b1_hbm, w2_ref, b2_hbm, gam_hbm, dy_hbm,
                m_ref, du_ref, d_ref, dr_ref, nrm_ref, db1_ref, dxp_ref,
                x_ref, b1_ref, b2_ref, gam_ref, dy_ref, w1b, w2b, ub, rb, xsb, xrb, fs, fr, stb, dmb, dmr, u_ref, dmf, pr_ref, acc,
                ls0, ls1, ls2, *sem_list):
    sems = {n: (sem_list[2 * i], sem_list[2 * i + 1]) for i, n in enumerate(SEM_NAMES)}
    h, y, c, sib, xn, xs = places()
    dev_sib, dev_x, dev_xs, dev_y = (0, y, sib), (0, y, xn), (0, y, xs), (0, 1 - y, h)
    order = [xs, xn, sib, h]

    def w1_load(j, k):
        u0, u1 = CH[j]
        n = u1 - u0
        return pltpu.make_async_copy(w1_ref.at[:, aligned(unit(j, order[k]), n, 256)], w1b.at[k, :, u0 * 256:u1 * 256],
                                     ls1.at[j, k])

    def w2_load(j):
        rows = slice(4 * 128 * CH[j][0], 4 * 128 * CH[j][1])
        return pltpu.make_async_copy(w2_ref.at[rows, :], w2b.at[rows, :], ls2.at[j])

    ins = [pltpu.make_async_copy(a, b, ls0.at[i]) for i, (a, b) in enumerate(
        ((x_hbm, x_ref), (b1_hbm, b1_ref), (b2_hbm, b2_ref), (gam_hbm, gam_ref), (dy_hbm, dy_ref)))]
    bar = pltpu.get_barrier_semaphore()
    for dev in (dev_sib, dev_x, dev_xs, dev_y):
        pl.semaphore_signal(bar, inc=1, device_id=dev, device_id_type=MESH)
    ins[0].start()
    load_order = []
    for j in range(NC + 1):
        load_order += [(j, k) for k in (0, 1) if j < NC] + [(j - 1, k) for k in (2, 3) if j > 0]
    for j, k in load_order[:6]:
        w1_load(j, k).start()
    loaded = [6]

    def load_more(n):
        for j, k in load_order[loaded[0]:loaded[0] + n]:
            w1_load(j, k).start()
        loaded[0] += n

    ins[0].wait()

    live = []

    def send(src, dst, name, k, dev):
        cp = remote(src, dst, sems[name], k, dev)
        cp.start()
        live.append(cp)
        return cp

    def u_parts(*slabs):
        for j, k in slabs:
            w1_load(j, k).wait()
        load_more(4)
        for j, k in slabs:
            u0, u1 = CH[j]
            r = dot(x_ref[...], w1b[k, :, u0 * 256:u1 * 256]).astype(BF)
            for i in range(u1 - u0):
                ub[k, u0 + i] = r[:, i * 256:(i + 1) * 256]
        if slabs[0] == (0, 0):
            pl.semaphore_wait(bar, 4)
            for cp in ins[1:]:
                cp.start()
        for j, k in slabs:
            us = slice(*CH[j])
            if k == 0:
                c_ud[j, 1] = send(ub.at[0, us], rb.at[1, us], "ud", 2 * j + 1, dev_sib)
            if k == 2:
                c_ud[j, 0] = send(ub.at[2, us], rb.at[0, us], "ud", 2 * j, dev_sib)

    def s1(j):
        us = slice(*CH[j])
        c_ud[j, 1].wait_recv()
        xsb[us] = (ub[1, us].astype(F32) + rb[1, us].astype(F32)).astype(BF)
        c_ux[j] = send(xsb.at[us], xrb.at[us], "ux", j, dev_x)

    def s2(j):
        u0, u1 = CH[j]
        us = slice(u0, u1)
        c_ud[j, 0].wait_recv()
        c_ux[j].wait_recv()
        for i in range(u1 - u0):
            a = u0 + i
            u = ub[3, a].astype(F32) + rb[0, a].astype(F32) + xrb[a].astype(F32) + b1_ref[unit(j, h) + i]
            u = u.astype(BF)
            u_ref[h, a] = u
            u = u.astype(F32)
            val, slope = gelu_both(u[:, PAIR:])
            m_ref[h, a] = (u[:, :PAIR] * val).astype(BF)
            pr_ref[h, a, :, :PAIR] = val
            pr_ref[h, a, :, PAIR:] = u[:, :PAIR] * slope
        c_mx[j] = send(m_ref.at[h, us], m_ref.at[h, us], "mx", j, dev_x)
        c_md[j] = send(m_ref.at[h, us], m_ref.at[h, us], "md", j, dev_sib)

    def s3(j):
        us = slice(*CH[j])
        c_mx[j].wait_recv()
        c_mf[j] = send(m_ref.at[xn, us], m_ref.at[xn, us], "mf", j, dev_sib)

    def s4(j):
        u0, u1 = CH[j]
        c_md[j].wait_recv()
        c_mf[j].wait_recv()
        w2_load(j).wait()
        m = jnp.concatenate([m_ref[q, a] for q in range(4) for a in range(u0, u1)], axis=1)
        for n in range(2):
            cols = slice(n * 512, (n + 1) * 512)
            part = dot(m, w2b[4 * 128 * u0:4 * 128 * u1, cols])
            if j > 0:
                part = nrm_ref[:, cols] + part
            if j < NC - 1:
                nrm_ref[:, cols] = part
            else:
                fs[n] = part.astype(BF)
                c_fy.append(send(fs.at[n], fr.at[n], "fy", n, dev_y))

    def gather_u(j):
        us = slice(*CH[j])
        c_gx[j] = send(u_ref.at[h, us], u_ref.at[h, us], "gx", j, dev_x)
        c_gd[j] = send(u_ref.at[h, us], u_ref.at[h, us], "gd", j, dev_sib)

    def forward_u(j):
        us = slice(*CH[j])
        c_gx[j].wait_recv()
        c_gf[j] = send(u_ref.at[xn, us], u_ref.at[xn, us], "gf", j, dev_sib)
        products(j, xn)

    def products(j, q):
        for a in range(*CH[j]):
            u = u_ref[q, a].astype(F32)
            val, slope = gelu_both(u[:, PAIR:])
            pr_ref[q, a, :, :PAIR] = val
            pr_ref[q, a, :, PAIR:] = u[:, :PAIR] * slope

    def products_sib(j):
        c_gd[j].wait_recv()
        c_gf[j].wait_recv()
        products(j, sib)
        products(j, xs)

    c_ud, c_ux, c_mx, c_md, c_mf, c_fy, c_gx, c_gd, c_gf = {}, {}, {}, {}, {}, [], {}, {}, {}
    u_parts((0, 0), (0, 1))
    u_parts((1, 0), (1, 1), (0, 2), (0, 3))
    s1(0)
    u_parts((2, 0), (2, 1), (1, 2), (1, 3))
    s1(1)
    u_parts((3, 0), (3, 1), (2, 2), (2, 3))
    s1(2)
    for j in range(NC):
        w2_load(j).start()
    u_parts((4, 0), (4, 1), (3, 2), (3, 3))
    s1(3)
    ins[1].wait()
    s2(0)
    u_parts((5, 0), (5, 1), (4, 2), (4, 3))
    s1(4)
    u_parts((5, 2), (5, 3))
    s1(5)
    s2(1)
    s2(2)
    s2(3)
    s2(4)
    s3(0)
    s4(0)
    s2(5)
    for j in range(NC):
        gather_u(j)
    for j in range(1, NC):
        s3(j)
        if j > 1:
            s4(j - 1)
    s4(NC - 1)
    for cp in ins[2:]:
        cp.wait()

    for j in range(3):
        forward_u(j)
    for n in range(2):
        cols = slice(n * 512, (n + 1) * 512)
        c_fy[n].wait_recv()
        f = fs[n].astype(F32) + fr[n].astype(F32)
        nrm_ref[:, cols] = ALPHA * x_ref[:, cols].astype(F32) + f + b2_ref[:, cols]
    r = nrm_ref[...]
    gdy = dy_ref[...].astype(F32) * gam_ref[...]
    m_loc = jnp.sum(r, axis=1, keepdims=True) * (1.0 / H)
    cen = r - m_loc
    m2 = jnp.sum(cen * cen, axis=1, keepdims=True)
    sg = jnp.sum(gdy, axis=1, keepdims=True)
    cg = jnp.sum(gdy * cen, axis=1, keepdims=True)
    lane = lax.broadcasted_iota(jnp.int32, (T, 128), 1)
    pack = jnp.where(lane == 0, m_loc, jnp.where(lane == 1, m2, jnp.where(lane == 2, sg, cg)))
    stb[h] = pack.T[0:8]
    c_st = [send(stb.at[h], stb.at[h], "st", i, dev) for i, dev in enumerate((dev_sib, dev_x, dev_xs))]
    forward_u(3)
    for j in range(3):
        products_sib(j)
    for cp in c_st:
        cp.wait_recv()
    st = [stb[i] for i in range(4)]
    mu = ((st[0][0:1] + st[1][0:1]) + (st[2][0:1] + st[3][0:1])) * 0.25
    m2t = jnp.zeros_like(mu)
    sgt = jnp.zeros_like(mu)
    cgt = jnp.zeros_like(mu)
    for i in range(4):
        delta = st[i][0:1] - mu
        m2t += st[i][1:2] + (H * delta) * delta
        sgt += st[i][2:3]
        cgt += st[i][3:4] + delta * st[i][2:3]
    rho = lax.rsqrt(m2t * (1.0 / (4 * H)) + LN_EPS)
    rows = jnp.concatenate([mu, rho, sgt * (1.0 / (4 * H)), cgt * rho * (1.0 / (4 * H)), jnp.zeros((124, T), F32)], axis=0)
    colst = rows.T
    mu_c, rho_c, mg_c, mgr_c = (colst[:, i:i + 1] for i in range(4))
    nrm = (r - mu_c) * rho_c
    dr = rho_c * (gdy - mg_c - nrm * mgr_c)
    nrm_ref[...] = nrm
    dr_ref[...] = dr
    d_ref[...] = dr.astype(BF)
    d_t = dr.T.astype(BF)

    c_dd, c_dx, c_df = {}, {}, {}
    mine, mine_k, theirs, theirs_k = (h, xn), (3, 1), (sib, xs), (2, 0)

    def dm_part(j):
        u0, u1 = CH[j]
        n = u1 - u0
        for i, q in enumerate(theirs + mine):
            r = dot(w2b[aligned(unit(j, q), n, 128), :], d_t).T.astype(BF)
            for a in range(n):
                dmb[i, u0 + a] = r[:, a * 128:(a + 1) * 128]
            if i == 1:
                for k in range(2):
                    c_dd[j, k] = send(dmb.at[k, u0:u1], dmr.at[k, u0:u1], "dd", 2 * j + k, dev_sib)

    def dm_sum(j):
        us = slice(*CH[j])
        c_ux[j].wait_send()
        live[:] = [cp for cp in live if cp is not c_ux[j]]
        for i in range(2):
            c_dd[j, i].wait_recv()
            xsb[us, :, i * 128:(i + 1) * 128] = (dmb[2 + i, us].astype(F32) + dmr[i, us].astype(F32)).astype(BF)
        c_dx[j] = send(xsb.at[us], xrb.at[us], "dx", j, dev_x)

    def dm_full(j):
        us = slice(*CH[j])
        c_dx[j].wait_recv()
        for i in range(2):
            q = mine[i]
            dmf[q, us] = (xsb[us, :, i * 128:(i + 1) * 128].astype(F32)
                          + xrb[us, :, (1 - i) * 128:(2 - i) * 128].astype(F32)).astype(BF)
        for i in range(2):
            q = mine[i]
            c_df[j, i] = send(dmf.at[q, us], dmf.at[q, us], "df", 2 * j + i, dev_sib)

    def grads(j, qs, ks, first):
        u0, u1 = CH[j]
        for q, k in zip(qs, ks):
            parts = []
            for a in range(u0, u1):
                dm = dmf[q, a].astype(F32)
                du_f = pr_ref[q, a] * jnp.concatenate([dm, dm], axis=1)
                db1_ref[unit(j, q) + a - u0] = jnp.sum(du_f, axis=0, keepdims=True)
                du_ref[q, a] = du_f.astype(BF)
                parts.append(du_f)
            du_t = jnp.concatenate(parts, axis=1).T.astype(BF)
            part = dot(w1b[k, :, u0 * 256:u1 * 256], du_t)
            acc[...] = part if first else acc[...] + part
            first = False

    def grads_mine(j):
        dm_full(j)
        grads(j, mine, mine_k, j == 0)

    def grads_theirs(j):
        for i in range(2):
            c_df[j, i].wait_recv()
        grads(j, theirs, theirs_k, False)

    dm_part(0)
    dm_part(1)
    dm_sum(0)
    dm_part(2)
    dm_sum(1)
    dm_part(3)
    dm_sum(2)
    forward_u(4)
    dm_part(4)
    dm_sum(3)
    forward_u(5)
    dm_part(5)
    dm_sum(4)
    dm_sum(5)
    for j in range(3, NC):
        products_sib(j)
    grads_mine(0)
    for j in range(1, NC):
        grads_theirs(j - 1)
        grads_mine(j)
    grads_theirs(NC - 1)
    dxp_ref[...] = acc[...].T.astype(BF)
    for cp in live:
        cp.wait_send()


def comm_call(x, w1, b1, w2, b2, gam, dy):
    scratch = [pltpu.VMEM((T, H), BF), pltpu.VMEM((4 * NU, 1, 256), F32), pltpu.VMEM((1, H), F32), pltpu.VMEM((1, H), F32),
               pltpu.VMEM((T, H), BF),
               pltpu.VMEM((4, H, NU * 256), BF), pltpu.VMEM((4 * NU * 128, H), BF),
               pltpu.VMEM((4, NU, T, 256), BF), pltpu.VMEM((2, NU, T, 256), BF),
               pltpu.VMEM((NU, T, 256), BF), pltpu.VMEM((NU, T, 256), BF),
               pltpu.VMEM((2, T, 512), BF), pltpu.VMEM((2, T, 512), BF),
               pltpu.VMEM((4, 8, T), F32),
               pltpu.VMEM((4, NU, T, 128), BF), pltpu.VMEM((2, NU, T, 128), BF),
               pltpu.VMEM((4, NU, T, 256), BF), pltpu.VMEM((4, NU, T, 128), BF), pltpu.VMEM((4, NU, T, 256), F32),
               pltpu.VMEM((H, T), F32),
               pltpu.SemaphoreType.DMA((5,)), pltpu.SemaphoreType.DMA((NC, 4)), pltpu.SemaphoreType.DMA((NC,))]
    for n in SEM_NAMES:
        scratch += [pltpu.SemaphoreType.DMA((N_SEM[n],)), pltpu.SemaphoreType.DMA((N_SEM[n],))]
    outs = [sds((4, NU, T, 128), BF), sds((4, NU, T, 256), BF), sds((T, H), BF), sds((T, H), F32), sds((T, H), F32),
            sds((4 * NU, 1, 256), F32), sds((T, H), BF)]
    return pl.pallas_call(
        comm_kernel, out_shape=outs, name="comm",
        in_specs=[HBM] * 7, out_specs=[VMEM] * 7, scratch_shapes=scratch,
        compiler_params=pltpu.CompilerParams(collective_id=0, has_side_effects=True, vmem_limit_bytes=COMM_LIM),
        cost_estimate=pl.CostEstimate(flops=8 * 10 ** 9, bytes_accessed=32 << 20, transcendentals=0),
    )(x, w1, b1, w2, b2, gam, dy)


NB2 = 6
NB1 = 6


def grads_kernel(m_ref, du_ref, d_ref, nrm_ref, dr_ref, db1_in, x_ref, gam_ref, beta_ref, dy_ref,
                 dw1_ref, dw2_ref, y_ref, db1_ref, db2_ref, dgam_ref, dbeta_ref,
                 ob2, ob1, xt, yb, db1b, so2, so1, so0):
    tiles = [(j, q) for j in range(NC) for q in range(4)]

    def put2(t):
        j, q = tiles[t]
        n = CH[j][1] - CH[j][0]
        r0 = unit(j, q) * 128
        return pltpu.make_async_copy(ob2.at[t % NB2, :n * 128], dw2_ref.at[r0:r0 + n * 128, :], so2.at[t % NB2])

    def put1(t):
        j, q = tiles[t]
        n = CH[j][1] - CH[j][0]
        c0 = unit(j, q) * 256
        return pltpu.make_async_copy(ob1.at[t % NB1, :, :n * 256], dw1_ref.at[:, c0:c0 + n * 256], so1.at[t % NB1])

    small = [pltpu.make_async_copy(yb, y_ref, so0.at[0]), pltpu.make_async_copy(db1b, db1_ref, so0.at[1])]
    for t, (j, q) in enumerate(tiles):
        if t >= NB2:
            put2(t - NB2).wait()
        for i, a in enumerate(range(*CH[j])):
            ob2[t % NB2, i * 128:(i + 1) * 128] = dot(m_ref[q, a].T, d_ref[...])
        put2(t).start()
        if t == 6:
            xt[...] = x_ref[...].T
        if t == 8:
            yb[...] = (gam_ref[...] * nrm_ref[...] + beta_ref[...]).astype(BF)
            for i in range(4 * NU):
                db1b[:, i * 256:(i + 1) * 256] = db1_in[i]
            for cp in small:
                cp.start()
        if t == 10:
            dy = dy_ref[...].astype(F32)
            db2_ref[...] = jnp.sum(dr_ref[...], axis=0, keepdims=True)
            dgam_ref[...] = jnp.sum(dy * nrm_ref[...], axis=0, keepdims=True)
            dbeta_ref[...] = jnp.sum(dy, axis=0, keepdims=True)
    for t, (j, q) in enumerate(tiles):
        if t >= NB1:
            put1(t - NB1).wait()
        for i, a in enumerate(range(*CH[j])):
            ob1[t % NB1, :, i * 256:(i + 1) * 256] = dot(xt[...], du_ref[q, a])
        put1(t).start()
    last = len(tiles)
    for t in range(last - NB2, last):
        put2(t).wait()
    for cp in small:
        cp.wait()
    for t in range(last - NB1, last):
        put1(t).wait()


def grads_call(m, du, d, nrm, dr, db1, x, gam, beta, dy):
    outs = [sds((H, 4 * NU * 256), F32), sds((4 * NU * 128, H), F32), sds((T, H), BF), sds((1, 4 * NU * 256), F32),
            sds((1, H), F32), sds((1, H), F32), sds((1, H), F32)]
    return pl.pallas_call(
        grads_kernel, out_shape=outs, name="grads",
        in_specs=[VMEM] * 10, out_specs=[HBM] * 4 + [VMEM] * 3,
        scratch_shapes=[pltpu.VMEM((NB2, 256, H), F32), pltpu.VMEM((NB1, H, 512), F32), pltpu.VMEM((H, T), BF),
                        pltpu.VMEM((T, H), BF), pltpu.VMEM((1, 4 * NU * 256), F32),
                        pltpu.SemaphoreType.DMA((NB2,)), pltpu.SemaphoreType.DMA((NB1,)), pltpu.SemaphoreType.DMA((2,))],
        compiler_params=pltpu.CompilerParams(vmem_limit_bytes=GRADS_LIM),
        cost_estimate=pl.CostEstimate(flops=4 * 10 ** 9, bytes_accessed=66 << 20, transcendentals=0),
    )(m, du, d, nrm, dr, db1, x, gam, beta, dy)


def solution(mesh):
    data_spec = P('dp', 'hd')
    hid_spec = P('hd')
    in_specs = (data_spec, P('hd', 'ff'), P('ff'), P('ff', 'hd'), hid_spec, hid_spec, hid_spec, data_spec)
    out_specs = (data_spec, data_spec, P(('dp', 'hd'), 'ff'), P(('dp', 'ff'), 'hd'), P(('dp', 'ff')), P(('dp', 'hd')), P(('dp', 'hd')), P(('dp', 'hd')))

    def device_step(x, w1, b1, w2, b2, gam, beta, dy):
        b2, gam, beta = (a.reshape(1, H) for a in (b2, gam, beta))
        hbm = [pltpu.with_memory_space_constraint(a, pltpu.HBM) for a in (x, w1, b1.reshape(4 * NU, 1, 256), w2, b2, gam, dy)]
        m, du, d, dr, nrm, db1, dxp = comm_call(*hbm)
        dxr = lax.ppermute(dxp, 'ff', [(0, 1), (1, 0)])
        dw1, dw2, y, db1, db2, dgam, dbeta = grads_call(m, du, d, nrm, dr, db1, x, gam, beta, dy)
        dx = (ALPHA * dr + (dxp.astype(F32) + dxr.astype(F32))).astype(BF)
        return y, dx, dw1, dw2, db1.reshape(-1), db2.reshape(-1), dgam.reshape(-1), dbeta.reshape(-1)

    return jax.shard_map(device_step, mesh=mesh, in_specs=in_specs, out_specs=out_specs, check_vma=False)
```

```python
import functools
import math
import jax
import jax.numpy as jnp
from jax import lax
from jax.experimental import pallas as pl
from jax.experimental.pallas import tpu as pltpu
from jax.sharding import PartitionSpec as P

PAIR = 128
ALPHA = math.sqrt(140.0)
LN_EPS = 1e-5
C0 = math.sqrt(2.0 / math.pi)
C1 = 0.044715
MESH = pl.DeviceIdType.MESH
F32 = jnp.float32
BF = jnp.bfloat16
T = 128
H = 1024
NU = 10
CH = ((0, 1), (1, 3), (3, 5), (5, 7), (7, 9), (9, 10))
NC = len(CH)
COMM_LIM = 48 * 1024 * 1024
GRADS_LIM = 28 * 1024 * 1024

VMEM = pl.BlockSpec(memory_space=pltpu.VMEM)
ANY = pl.BlockSpec(memory_space=pl.ANY)
HBM = pl.BlockSpec(memory_space=pltpu.HBM)


def sds(shape, dtype):
    return jax.ShapeDtypeStruct(shape, dtype)


def dot(a, b):
    return jnp.dot(a, b, preferred_element_type=F32)


def gelu_both(g):
    g2 = g * g
    t = jnp.tanh(C0 * (g + C1 * (g2 * g)))
    cdf = 0.5 * (1.0 + t)
    slope = cdf + (0.5 * g) * (1.0 - t * t) * (C0 * (1.0 + (3.0 * C1) * g2))
    return g * cdf, slope


def places():
    h = lax.axis_index("hd")
    y = lax.axis_index("ff")
    c = lax.rem(h, 2)
    sib = h + 1 - 2 * c
    xn = lax.rem(h + 2, 4)
    xs = lax.rem(sib + 2, 4)
    return h, y, c, sib, xn, xs


def remote(src, dst, sems, k, dev):
    return pltpu.make_async_remote_copy(src_ref=src, dst_ref=dst, send_sem=sems[0].at[k], recv_sem=sems[1].at[k],
                                        device_id=dev, device_id_type=MESH)


def unit(j, q):
    u0, u1 = CH[j]
    return 4 * u0 + q * (u1 - u0)


def aligned(start, size, tile):
    return pl.ds(pl.multiple_of(start * tile, tile), size * tile)


GCH = ((0, 3), (3, 7), (7, 10))
NG = len(GCH)
NLS = 16
N_SEM = {"ud": 2 * NC, "ux": NC, "mx": NC, "md": 2 * NC, "gx": NG, "gd": NG, "gf": NG, "fy": 2, "st": 3}
SEM_NAMES = list(N_SEM)


def comm_kernel(x_hbm, w1_ref, b1_hbm, w2_ref, b2_hbm, gam_hbm, dy_hbm,
                m_ref, du_ref, d_ref, dr_ref, nrm_ref, db1_ref, dxp_ref,
                x_ref, b1_ref, b2_ref, gam_ref, dy_ref, w1b, w2b, ub, rb, xsb, xrb, fs, fr, stb, dmb, dmr, u_ref, dmf, pr_ref, acc,
                ls0, ls1, *sem_list):
    sems = {n: (sem_list[2 * i], sem_list[2 * i + 1]) for i, n in enumerate(SEM_NAMES)}
    h, y, c, sib, xn, xs = places()
    dev_sib, dev_x, dev_xs, dev_y = (0, y, sib), (0, y, xn), (0, y, xs), (0, 1 - y, h)
    order = [xs, xn, sib, h]

    load_order = []
    for j in range(NC + 1):
        load_order += [(j, k) for k in (0, 1) if j < NC] + [(j - 1, k) for k in (2, 3) if j > 0]

    def w1_load(j, k):
        u0, u1 = CH[j]
        n = u1 - u0
        return pltpu.make_async_copy(w1_ref.at[:, aligned(unit(j, order[k]), n, 256)], w1b.at[k, :, u0 * 256:u1 * 256],
                                     ls1.at[load_order.index((j, k)) % NLS])

    def w2_load(j):
        rows = slice(4 * 128 * CH[j][0], 4 * 128 * CH[j][1])
        return pltpu.make_async_copy(w2_ref.at[rows, :], w2b.at[rows, :], ls1.at[(4 * NC + j) % NLS])

    ins = [pltpu.make_async_copy(a, b, ls0.at[i]) for i, (a, b) in enumerate(
        ((x_hbm, x_ref), (b1_hbm, b1_ref), (b2_hbm, b2_ref), (gam_hbm, gam_ref), (dy_hbm, dy_ref)))]
    bar = pltpu.get_barrier_semaphore()
    for dev in (dev_sib, dev_x, dev_xs, dev_y):
        pl.semaphore_signal(bar, inc=1, device_id=dev, device_id_type=MESH)
    ins[0].start()
    for j, k in load_order[:6]:
        w1_load(j, k).start()
    loaded = [6]

    def load_more(n):
        for j, k in load_order[loaded[0]:loaded[0] + n]:
            w1_load(j, k).start()
        loaded[0] += n

    ins[0].wait()

    live = []

    def send(src, dst, name, k, dev):
        cp = remote(src, dst, sems[name], k, dev)
        cp.start()
        live.append(cp)
        return cp

    def sent(*cps):
        for cp in cps:
            cp.wait_send()
        live[:] = [cp for cp in live if not any(cp is old for old in cps)]

    def u_parts(*slabs):
        for j, k in slabs:
            w1_load(j, k).wait()
        load_more(4)
        for j, k in slabs:
            u0, u1 = CH[j]
            r = dot(x_ref[...], w1b[k, :, u0 * 256:u1 * 256]).astype(BF)
            for i in range(u1 - u0):
                ub[k, u0 + i] = r[:, i * 256:(i + 1) * 256]
        if slabs[0] == (0, 0):
            pl.semaphore_wait(bar, 4)
            for cp in ins[1:]:
                cp.start()
        for j, k in slabs:
            us = slice(*CH[j])
            if k == 0:
                c_ud[j, 1] = send(ub.at[0, us], rb.at[1, us], "ud", 2 * j + 1, dev_sib)
            if k == 2:
                c_ud[j, 0] = send(ub.at[2, us], rb.at[0, us], "ud", 2 * j, dev_sib)

    def s1(j):
        us = slice(*CH[j])
        c_ud[j, 1].wait_recv()
        xsb[us] = (ub[1, us].astype(F32) + rb[1, us].astype(F32)).astype(BF)
        c_ux[j] = send(xsb.at[us], xrb.at[us], "ux", j, dev_x)

    def s2(j):
        u0, u1 = CH[j]
        us = slice(u0, u1)
        c_ud[j, 0].wait_recv()
        c_ux[j].wait_recv()
        for i in range(u1 - u0):
            a = u0 + i
            u = ub[3, a].astype(F32) + rb[0, a].astype(F32) + xrb[a].astype(F32) + b1_ref[unit(j, h) + i]
            u = u.astype(BF)
            u_ref[h, a] = u
            u = u.astype(F32)
            val, slope = gelu_both(u[:, PAIR:])
            m_ref[h, a] = (u[:, :PAIR] * val).astype(BF)
            pr_ref[h, a, :, :PAIR] = val
            pr_ref[h, a, :, PAIR:] = u[:, :PAIR] * slope
        c_mx[j] = send(m_ref.at[h, us], m_ref.at[h, us], "mx", j, dev_x)
        c_md[j] = send(m_ref.at[h, us], m_ref.at[h, us], "md", 2 * j, dev_sib)

    def s3(j):
        us = slice(*CH[j])
        c_mx[j].wait_recv()
        c_mf[j] = send(m_ref.at[xn, us], m_ref.at[xn, us], "md", 2 * j + 1, dev_sib)

    def s4(j):
        u0, u1 = CH[j]
        c_md[j].wait_recv()
        c_mf[j].wait_recv()
        w2_load(j).wait()
        m = jnp.concatenate([m_ref[q, a] for q in range(4) for a in range(u0, u1)], axis=1)
        for n in range(2):
            cols = slice(n * 512, (n + 1) * 512)
            part = dot(m, w2b[4 * 128 * u0:4 * 128 * u1, cols])
            if j > 0:
                part = nrm_ref[:, cols] + part
            if j < NC - 1:
                nrm_ref[:, cols] = part
            else:
                fs[n] = part.astype(BF)
                c_fy.append(send(fs.at[n], fr.at[n], "fy", n, dev_y))

    def gather_u(j):
        us = slice(*GCH[j])
        c_gx[j] = send(u_ref.at[h, us], u_ref.at[h, us], "gx", j, dev_x)
        c_gd[j] = send(u_ref.at[h, us], u_ref.at[h, us], "gd", j, dev_sib)

    def forward_u(j):
        us = slice(*GCH[j])
        c_gx[j].wait_recv()
        c_gf[j] = send(u_ref.at[xn, us], u_ref.at[xn, us], "gf", j, dev_sib)
        products(j, xn)

    def products(j, q):
        for a in range(*GCH[j]):
            u = u_ref[q, a].astype(F32)
            val, slope = gelu_both(u[:, PAIR:])
            pr_ref[q, a, :, :PAIR] = val
            pr_ref[q, a, :, PAIR:] = u[:, :PAIR] * slope

    def products_sib(j):
        c_gd[j].wait_recv()
        c_gf[j].wait_recv()
        products(j, sib)
        products(j, xs)

    c_ud, c_ux, c_mx, c_md, c_mf, c_fy, c_gx, c_gd, c_gf = {}, {}, {}, {}, {}, [], {}, {}, {}
    u_parts((0, 0), (0, 1))
    u_parts((1, 0), (1, 1), (0, 2), (0, 3))
    s1(0)
    u_parts((2, 0), (2, 1), (1, 2), (1, 3))
    s1(1)
    u_parts((3, 0), (3, 1), (2, 2), (2, 3))
    s1(2)
    for j in range(NC):
        w2_load(j).start()
    u_parts((4, 0), (4, 1), (3, 2), (3, 3))
    s1(3)
    ins[1].wait()
    s2(0)
    u_parts((5, 0), (5, 1), (4, 2), (4, 3))
    s1(4)
    u_parts((5, 2), (5, 3))
    s1(5)
    s2(1)
    s2(2)
    s2(3)
    s2(4)
    s3(0)
    s4(0)
    s2(5)
    for j in range(NG):
        gather_u(j)
    for j in range(1, NC):
        s3(j)
        if j > 1:
            s4(j - 1)
    s4(NC - 1)
    for cp in ins[2:]:
        cp.wait()

    forward_u(0)
    for n in range(2):
        cols = slice(n * 512, (n + 1) * 512)
        c_fy[n].wait_recv()
        f = fs[n].astype(F32) + fr[n].astype(F32)
        nrm_ref[:, cols] = ALPHA * x_ref[:, cols].astype(F32) + f + b2_ref[:, cols]
    r = nrm_ref[...]
    gdy = dy_ref[...].astype(F32) * gam_ref[...]
    m_loc = jnp.sum(r, axis=1, keepdims=True) * (1.0 / H)
    cen = r - m_loc
    m2 = jnp.sum(cen * cen, axis=1, keepdims=True)
    sg = jnp.sum(gdy, axis=1, keepdims=True)
    cg = jnp.sum(gdy * cen, axis=1, keepdims=True)
    lane = lax.broadcasted_iota(jnp.int32, (T, 128), 1)
    pack = jnp.where(lane == 0, m_loc, jnp.where(lane == 1, m2, jnp.where(lane == 2, sg, cg)))
    stb[h] = pack.T[0:8]
    c_st = [send(stb.at[h], stb.at[h], "st", i, dev) for i, dev in enumerate((dev_sib, dev_x, dev_xs))]
    forward_u(1)
    products_sib(0)
    for cp in c_st:
        cp.wait_recv()
    st = [stb[i] for i in range(4)]
    mu = ((st[0][0:1] + st[1][0:1]) + (st[2][0:1] + st[3][0:1])) * 0.25
    m2t = jnp.zeros_like(mu)
    sgt = jnp.zeros_like(mu)
    cgt = jnp.zeros_like(mu)
    for i in range(4):
        delta = st[i][0:1] - mu
        m2t += st[i][1:2] + (H * delta) * delta
        sgt += st[i][2:3]
        cgt += st[i][3:4] + delta * st[i][2:3]
    rho = lax.rsqrt(m2t * (1.0 / (4 * H)) + LN_EPS)
    rows = jnp.concatenate([mu, rho, sgt * (1.0 / (4 * H)), cgt * rho * (1.0 / (4 * H)), jnp.zeros((124, T), F32)], axis=0)
    colst = rows.T
    mu_c, rho_c, mg_c, mgr_c = (colst[:, i:i + 1] for i in range(4))
    nrm = (r - mu_c) * rho_c
    dr = rho_c * (gdy - mg_c - nrm * mgr_c)
    nrm_ref[...] = nrm
    dr_ref[...] = dr
    d_ref[...] = dr.astype(BF)
    d_t = dr.T.astype(BF)

    c_dd, c_dx, c_df = {}, {}, {}
    mine, mine_k, theirs, theirs_k = (h, xn), (3, 1), (sib, xs), (2, 0)

    def dm_part(j):
        u0, u1 = CH[j]
        n = u1 - u0
        for i, q in enumerate(theirs + mine):
            r = dot(w2b[aligned(unit(j, q), n, 128), :], d_t).astype(BF).T
            for a in range(n):
                dmb[i, u0 + a] = r[:, a * 128:(a + 1) * 128]
            if i == 1:
                sent(c_ud[j, 0], c_ud[j, 1])
                for k in range(2):
                    c_dd[j, k] = send(dmb.at[k, u0:u1], dmr.at[k, u0:u1], "ud", 2 * j + k, dev_sib)

    def dm_sum(j):
        us = slice(*CH[j])
        sent(c_ux[j])
        for i in range(2):
            c_dd[j, i].wait_recv()
            xsb[us, :, i * 128:(i + 1) * 128] = (dmb[2 + i, us].astype(F32) + dmr[i, us].astype(F32)).astype(BF)
        c_dx[j] = send(xsb.at[us], xrb.at[us], "ux", j, dev_x)

    def dm_full(j):
        us = slice(*CH[j])
        c_dx[j].wait_recv()
        sent(c_md[j], c_mf[j])
        for i in range(2):
            q = mine[i]
            dmf[q, us] = (xsb[us, :, i * 128:(i + 1) * 128].astype(F32)
                          + xrb[us, :, (1 - i) * 128:(2 - i) * 128].astype(F32)).astype(BF)
        for i in range(2):
            q = mine[i]
            c_df[j, i] = send(dmf.at[q, us], dmf.at[q, us], "md", 2 * j + i, dev_sib)

    def grads(j, qs, ks, first):
        u0, u1 = CH[j]
        for q, k in zip(qs, ks):
            parts = []
            for a in range(u0, u1):
                dm = dmf[q, a].astype(F32)
                du_f = pr_ref[q, a] * jnp.concatenate([dm, dm], axis=1)
                db1_ref[unit(j, q) + a - u0] = jnp.sum(du_f, axis=0, keepdims=True)
                du = du_f.astype(BF)
                du_ref[q, a] = du
                parts.append(du)
            du_t = jnp.concatenate(parts, axis=1).T
            part = dot(w1b[k, :, u0 * 256:u1 * 256], du_t)
            acc[...] = part if first else acc[...] + part
            first = False

    def grads_mine(j):
        dm_full(j)
        grads(j, mine, mine_k, j == 0)

    def grads_theirs(j):
        for i in range(2):
            c_df[j, i].wait_recv()
        grads(j, theirs, theirs_k, False)

    dm_part(0)
    dm_part(1)
    dm_sum(0)
    dm_part(2)
    dm_sum(1)
    dm_part(3)
    dm_sum(2)
    products_sib(1)
    dm_part(4)
    dm_sum(3)
    forward_u(2)
    dm_part(5)
    dm_sum(4)
    dm_sum(5)
    products_sib(2)
    grads_mine(0)
    for j in range(1, NC):
        grads_theirs(j - 1)
        grads_mine(j)
    grads_theirs(NC - 1)
    dxp_ref[...] = acc[...].T.astype(BF)
    for cp in live:
        cp.wait_send()


def comm_call(x, w1, b1, w2, b2, gam, dy):
    scratch = [pltpu.VMEM((T, H), BF), pltpu.VMEM((4 * NU, 1, 256), F32), pltpu.VMEM((1, H), F32), pltpu.VMEM((1, H), F32),
               pltpu.VMEM((T, H), BF),
               pltpu.VMEM((4, H, NU * 256), BF), pltpu.VMEM((4 * NU * 128, H), BF),
               pltpu.VMEM((4, NU, T, 256), BF), pltpu.VMEM((2, NU, T, 256), BF),
               pltpu.VMEM((NU, T, 256), BF), pltpu.VMEM((NU, T, 256), BF),
               pltpu.VMEM((2, T, 512), BF), pltpu.VMEM((2, T, 512), BF),
               pltpu.VMEM((4, 8, T), F32),
               pltpu.VMEM((4, NU, T, 128), BF), pltpu.VMEM((2, NU, T, 128), BF),
               pltpu.VMEM((4, NU, T, 256), BF), pltpu.VMEM((4, NU, T, 128), BF), pltpu.VMEM((4, NU, T, 256), F32),
               pltpu.VMEM((H, T), F32),
               pltpu.SemaphoreType.DMA((5,)), pltpu.SemaphoreType.DMA((NLS,))]
    for n in SEM_NAMES:
        scratch += [pltpu.SemaphoreType.DMA((N_SEM[n],)), pltpu.SemaphoreType.DMA((N_SEM[n],))]
    outs = [sds((4, NU, T, 128), BF), sds((4, NU, T, 256), BF), sds((T, H), BF), sds((T, H), F32), sds((T, H), F32),
            sds((4 * NU, 1, 256), F32), sds((T, H), BF)]
    return pl.pallas_call(
        comm_kernel, out_shape=outs, name="comm",
        in_specs=[HBM] * 7, out_specs=[VMEM] * 7, scratch_shapes=scratch,
        compiler_params=pltpu.CompilerParams(collective_id=0, has_side_effects=True, vmem_limit_bytes=COMM_LIM),
        cost_estimate=pl.CostEstimate(flops=8 * 10 ** 9, bytes_accessed=32 << 20, transcendentals=0),
    )(x, w1, b1, w2, b2, gam, dy)


NB2 = 6
NB1 = 6


def grads_kernel(m_ref, du_ref, d_ref, nrm_ref, dr_ref, db1_in, x_ref, gam_ref, beta_ref, dy_ref,
                 dw1_ref, dw2_ref, y_ref, db1_ref, db2_ref, dgam_ref, dbeta_ref,
                 ob2, ob1, xt, yb, db1b, sb, so2, so1, so0):
    tiles = [(j, q) for j in range(NC) for q in range(4)]

    def put2(t):
        j, q = tiles[t]
        n = CH[j][1] - CH[j][0]
        r0 = unit(j, q) * 128
        return pltpu.make_async_copy(ob2.at[t % NB2, :n * 128], dw2_ref.at[r0:r0 + n * 128, :], so2.at[t % NB2])

    def put1(t):
        j, q = tiles[t]
        n = CH[j][1] - CH[j][0]
        c0 = unit(j, q) * 256
        return pltpu.make_async_copy(ob1.at[t % NB1, :, :n * 256], dw1_ref.at[:, c0:c0 + n * 256], so1.at[t % NB1])

    small = [pltpu.make_async_copy(a, b, so0.at[i]) for i, (a, b) in enumerate(
        ((yb, y_ref), (db1b, db1_ref), (sb.at[0], db2_ref), (sb.at[1], dgam_ref), (sb.at[2], dbeta_ref)))]
    for t, (j, q) in enumerate(tiles):
        if t >= NB2:
            put2(t - NB2).wait()
        for i, a in enumerate(range(*CH[j])):
            ob2[t % NB2, i * 128:(i + 1) * 128] = dot(m_ref[q, a].T, d_ref[...])
        put2(t).start()
        if t == 6:
            xt[...] = x_ref[...].T
        if t == 8:
            yb[...] = (gam_ref[...] * nrm_ref[...] + beta_ref[...]).astype(BF)
            for i in range(4 * NU):
                db1b[:, i * 256:(i + 1) * 256] = db1_in[i]
            for cp in small[:2]:
                cp.start()
        if t == 10:
            dy = dy_ref[...].astype(F32)
            sb[0] = jnp.sum(dr_ref[...], axis=0, keepdims=True)
            sb[1] = jnp.sum(dy * nrm_ref[...], axis=0, keepdims=True)
            sb[2] = jnp.sum(dy, axis=0, keepdims=True)
            for cp in small[2:]:
                cp.start()
    for t, (j, q) in enumerate(tiles):
        if t >= NB1:
            put1(t - NB1).wait()
        for i, a in enumerate(range(*CH[j])):
            ob1[t % NB1, :, i * 256:(i + 1) * 256] = dot(xt[...], du_ref[q, a])
        put1(t).start()
    last = len(tiles)
    for t in range(last - NB2, last):
        put2(t).wait()
    for cp in small:
        cp.wait()
    for t in range(last - NB1, last):
        put1(t).wait()


def grads_call(m, du, d, nrm, dr, db1, x, gam, beta, dy):
    outs = [sds((H, 4 * NU * 256), F32), sds((4 * NU * 128, H), F32), sds((T, H), BF), sds((1, 4 * NU * 256), F32),
            sds((1, H), F32), sds((1, H), F32), sds((1, H), F32)]
    return pl.pallas_call(
        grads_kernel, out_shape=outs, name="grads",
        in_specs=[VMEM] * 10, out_specs=[HBM] * 7,
        scratch_shapes=[pltpu.VMEM((NB2, 256, H), F32), pltpu.VMEM((NB1, H, 512), F32), pltpu.VMEM((H, T), BF),
                        pltpu.VMEM((T, H), BF), pltpu.VMEM((1, 4 * NU * 256), F32), pltpu.VMEM((3, 1, H), F32),
                        pltpu.SemaphoreType.DMA((NB2,)), pltpu.SemaphoreType.DMA((NB1,)), pltpu.SemaphoreType.DMA((5,))],
        compiler_params=pltpu.CompilerParams(vmem_limit_bytes=GRADS_LIM),
        cost_estimate=pl.CostEstimate(flops=4 * 10 ** 9, bytes_accessed=66 << 20, transcendentals=0),
    )(m, du, d, nrm, dr, db1, x, gam, beta, dy)


def solution(mesh):
    data_spec = P('dp', 'hd')
    hid_spec = P('hd')
    in_specs = (data_spec, P('hd', 'ff'), P('ff'), P('ff', 'hd'), hid_spec, hid_spec, hid_spec, data_spec)
    out_specs = (data_spec, data_spec, P(('dp', 'hd'), 'ff'), P(('dp', 'ff'), 'hd'), P(('dp', 'ff')), P(('dp', 'hd')), P(('dp', 'hd')), P(('dp', 'hd')))

    def device_step(x, w1, b1, w2, b2, gam, beta, dy):
        b2, gam, beta = (a.reshape(1, H) for a in (b2, gam, beta))
        hbm = [pltpu.with_memory_space_constraint(a, pltpu.HBM) for a in (x, w1, b1.reshape(4 * NU, 1, 256), w2, b2, gam, dy)]
        m, du, d, dr, nrm, db1, dxp = comm_call(*hbm)
        dxr = lax.ppermute(dxp, 'ff', [(0, 1), (1, 0)])
        dw1, dw2, y, db1, db2, dgam, dbeta = grads_call(m, du, d, nrm, dr, db1, x, gam, beta, dy)
        dx = (ALPHA * dr + (dxp.astype(F32) + dxr.astype(F32))).astype(BF)
        return y, dx, dw1, dw2, db1.reshape(-1), db2.reshape(-1), dgam.reshape(-1), dbeta.reshape(-1)

    return jax.shard_map(device_step, mesh=mesh, in_specs=in_specs, out_specs=out_specs, check_vma=False)
```

```python
import functools
import math
import jax
import jax.numpy as jnp
from jax import lax
from jax.experimental import pallas as pl
from jax.experimental.pallas import tpu as pltpu
from jax.sharding import PartitionSpec as P

PAIR = 128
ALPHA = math.sqrt(140.0)
LN_EPS = 1e-5
C0 = math.sqrt(2.0 / math.pi)
C1 = 0.044715
MESH = pl.DeviceIdType.MESH
F32 = jnp.float32
BF = jnp.bfloat16
T = 128
H = 1024
NU = 10
CH = ((0, 1), (1, 3), (3, 5), (5, 7), (7, 9), (9, 10))
NC = len(CH)
COMM_LIM = 48 * 1024 * 1024
GRADS_LIM = 28 * 1024 * 1024

VMEM = pl.BlockSpec(memory_space=pltpu.VMEM)
ANY = pl.BlockSpec(memory_space=pl.ANY)
HBM = pl.BlockSpec(memory_space=pltpu.HBM)


def sds(shape, dtype):
    return jax.ShapeDtypeStruct(shape, dtype)


def dot(a, b):
    return jnp.dot(a, b, preferred_element_type=F32)


def gelu_both(g):
    g2 = g * g
    t = jnp.tanh(C0 * (g + C1 * (g2 * g)))
    cdf = 0.5 * (1.0 + t)
    slope = cdf + (0.5 * g) * (1.0 - t * t) * (C0 * (1.0 + (3.0 * C1) * g2))
    return g * cdf, slope


def places():
    h = lax.axis_index("hd")
    y = lax.axis_index("ff")
    c = lax.rem(h, 2)
    sib = h + 1 - 2 * c
    xn = lax.rem(h + 2, 4)
    xs = lax.rem(sib + 2, 4)
    return h, y, c, sib, xn, xs


def remote(src, dst, sems, k, dev):
    return pltpu.make_async_remote_copy(src_ref=src, dst_ref=dst, send_sem=sems[0].at[k], recv_sem=sems[1].at[k],
                                        device_id=dev, device_id_type=MESH)


def unit(j, q):
    u0, u1 = CH[j]
    return 4 * u0 + q * (u1 - u0)


def aligned(start, size, tile):
    return pl.ds(pl.multiple_of(start * tile, tile), size * tile)


GCH = ((0, 3), (3, 7), (7, 10))
NG = len(GCH)
NLS = 16
N_SEM = {"ud": 2 * NC, "ux": NC, "mx": NC, "md": 2 * NC, "gx": NG, "gd": NG, "gf": NG, "fy": 2, "st": 3}
SEM_NAMES = list(N_SEM)


def comm_kernel(x_hbm, w1_ref, b1_hbm, w2_ref, b2_hbm, gam_hbm, dy_hbm,
                m_ref, du_ref, d_ref, dr_ref, nrm_ref, db1_ref, dxp_ref,
                x_ref, b1_ref, b2_ref, gam_ref, dy_ref, w1b, w2b, ub, rb, xsb, xrb, fs, fr, stb, dmb, dmr, u_ref, dmf, pr_ref, acc,
                ls0, ls1, *sem_list):
    sems = {n: (sem_list[2 * i], sem_list[2 * i + 1]) for i, n in enumerate(SEM_NAMES)}
    h, y, c, sib, xn, xs = places()
    dev_sib, dev_x, dev_xs, dev_y = (0, y, sib), (0, y, xn), (0, y, xs), (0, 1 - y, h)
    order = [xs, xn, sib, h]

    load_order = []
    for j in range(NC + 1):
        load_order += [(j, k) for k in (0, 1) if j < NC] + [(j - 1, k) for k in (2, 3) if j > 0]

    def w1_load(j, k):
        u0, u1 = CH[j]
        n = u1 - u0
        return pltpu.make_async_copy(w1_ref.at[:, aligned(unit(j, order[k]), n, 256)], w1b.at[k, :, u0 * 256:u1 * 256],
                                     ls1.at[load_order.index((j, k)) % NLS])

    def w2_load(j):
        rows = slice(4 * 128 * CH[j][0], 4 * 128 * CH[j][1])
        return pltpu.make_async_copy(w2_ref.at[rows, :], w2b.at[rows, :], ls1.at[(4 * NC + j) % NLS])

    ins = [pltpu.make_async_copy(a, b, ls0.at[i]) for i, (a, b) in enumerate(
        ((x_hbm, x_ref), (b1_hbm, b1_ref), (b2_hbm, b2_ref), (gam_hbm, gam_ref), (dy_hbm, dy_ref)))]
    bar = pltpu.get_barrier_semaphore()
    for dev in (dev_sib, dev_x, dev_xs, dev_y):
        pl.semaphore_signal(bar, inc=1, device_id=dev, device_id_type=MESH)
    ins[0].start()
    for j, k in load_order[:6]:
        w1_load(j, k).start()
    loaded = [6]

    def load_more(n):
        for j, k in load_order[loaded[0]:loaded[0] + n]:
            w1_load(j, k).start()
        loaded[0] += n

    ins[0].wait()

    live = []

    def send(src, dst, name, k, dev):
        cp = remote(src, dst, sems[name], k, dev)
        cp.start()
        live.append(cp)
        return cp

    def sent(*cps):
        for cp in cps:
            cp.wait_send()
        live[:] = [cp for cp in live if not any(cp is old for old in cps)]

    def u_parts(*slabs):
        for j, k in slabs:
            w1_load(j, k).wait()
        load_more(4)
        for j, k in slabs:
            u0, u1 = CH[j]
            r = dot(x_ref[...], w1b[k, :, u0 * 256:u1 * 256]).astype(BF)
            for i in range(u1 - u0):
                ub[k, u0 + i] = r[:, i * 256:(i + 1) * 256]
        if slabs[0] == (0, 0):
            pl.semaphore_wait(bar, 4)
            for cp in ins[1:]:
                cp.start()
        for j, k in slabs:
            us = slice(*CH[j])
            if k == 0:
                c_ud[j, 1] = send(ub.at[0, us], rb.at[1, us], "ud", 2 * j + 1, dev_sib)
            if k == 2:
                c_ud[j, 0] = send(ub.at[2, us], rb.at[0, us], "ud", 2 * j, dev_sib)

    def s1(j):
        us = slice(*CH[j])
        c_ud[j, 1].wait_recv()
        xsb[us] = (ub[1, us].astype(F32) + rb[1, us].astype(F32)).astype(BF)
        c_ux[j] = send(xsb.at[us], xrb.at[us], "ux", j, dev_x)

    def s2(j):
        u0, u1 = CH[j]
        us = slice(u0, u1)
        c_ud[j, 0].wait_recv()
        c_ux[j].wait_recv()
        for i in range(u1 - u0):
            a = u0 + i
            u = ub[3, a].astype(F32) + rb[0, a].astype(F32) + xrb[a].astype(F32) + b1_ref[unit(j, h) + i]
            u = u.astype(BF)
            u_ref[h, a] = u
            u = u.astype(F32)
            val, slope = gelu_both(u[:, PAIR:])
            m_ref[h, a] = (u[:, :PAIR] * val).astype(BF)
            pr_ref[h, a, :, :PAIR] = val
            pr_ref[h, a, :, PAIR:] = u[:, :PAIR] * slope
        c_mx[j] = send(m_ref.at[h, us], m_ref.at[h, us], "mx", j, dev_x)
        c_md[j] = send(m_ref.at[h, us], m_ref.at[h, us], "md", 2 * j, dev_sib)

    def s3(j):
        us = slice(*CH[j])
        c_mx[j].wait_recv()
        c_mf[j] = send(m_ref.at[xn, us], m_ref.at[xn, us], "md", 2 * j + 1, dev_sib)

    def s4(j):
        u0, u1 = CH[j]
        c_md[j].wait_recv()
        c_mf[j].wait_recv()
        w2_load(j).wait()
        m = jnp.concatenate([m_ref[q, a] for q in range(4) for a in range(u0, u1)], axis=1)
        for n in range(2):
            cols = slice(n * 512, (n + 1) * 512)
            part = dot(m, w2b[4 * 128 * u0:4 * 128 * u1, cols])
            if j > 0:
                part = nrm_ref[:, cols] + part
            if j < NC - 1:
                nrm_ref[:, cols] = part
            else:
                fs[n] = part.astype(BF)
                c_fy.append(send(fs.at[n], fr.at[n], "fy", n, dev_y))

    def gather_u(j):
        us = slice(*GCH[j])
        c_gx[j] = send(u_ref.at[h, us], u_ref.at[h, us], "gx", j, dev_x)
        c_gd[j] = send(u_ref.at[h, us], u_ref.at[h, us], "gd", j, dev_sib)

    def forward_u(j):
        us = slice(*GCH[j])
        c_gx[j].wait_recv()
        c_gf[j] = send(u_ref.at[xn, us], u_ref.at[xn, us], "gf", j, dev_sib)
        products(j, xn)

    def products(j, q):
        for a in range(*GCH[j]):
            u = u_ref[q, a].astype(F32)
            val, slope = gelu_both(u[:, PAIR:])
            pr_ref[q, a, :, :PAIR] = val
            pr_ref[q, a, :, PAIR:] = u[:, :PAIR] * slope

    def products_sib(j):
        c_gd[j].wait_recv()
        c_gf[j].wait_recv()
        products(j, sib)
        products(j, xs)

    c_ud, c_ux, c_mx, c_md, c_mf, c_fy, c_gx, c_gd, c_gf = {}, {}, {}, {}, {}, [], {}, {}, {}
    u_parts((0, 0), (0, 1))
    u_parts((1, 0), (1, 1), (0, 2), (0, 3))
    s1(0)
    u_parts((2, 0), (2, 1), (1, 2), (1, 3))
    s1(1)
    u_parts((3, 0), (3, 1), (2, 2), (2, 3))
    s1(2)
    for j in range(NC):
        w2_load(j).start()
    u_parts((4, 0), (4, 1), (3, 2), (3, 3))
    s1(3)
    ins[1].wait()
    s2(0)
    u_parts((5, 0), (5, 1), (4, 2), (4, 3))
    s1(4)
    u_parts((5, 2), (5, 3))
    s1(5)
    s2(1)
    s2(2)
    s2(3)
    s2(4)
    s3(0)
    s4(0)
    s2(5)
    for j in range(NG):
        gather_u(j)
    for j in range(1, NC):
        s3(j)
        if j > 1:
            s4(j - 1)
    s4(NC - 1)
    for cp in ins[2:]:
        cp.wait()

    forward_u(0)
    for n in range(2):
        cols = slice(n * 512, (n + 1) * 512)
        c_fy[n].wait_recv()
        f = fs[n].astype(F32) + fr[n].astype(F32)
        nrm_ref[:, cols] = ALPHA * x_ref[:, cols].astype(F32) + f + b2_ref[:, cols]
    r = nrm_ref[...]
    gdy = dy_ref[...].astype(F32) * gam_ref[...]
    m_loc = jnp.sum(r, axis=1, keepdims=True) * (1.0 / H)
    cen = r - m_loc
    m2 = jnp.sum(cen * cen, axis=1, keepdims=True)
    sg = jnp.sum(gdy, axis=1, keepdims=True)
    cg = jnp.sum(gdy * cen, axis=1, keepdims=True)
    lane = lax.broadcasted_iota(jnp.int32, (T, 128), 1)
    pack = jnp.where(lane == 0, m_loc, jnp.where(lane == 1, m2, jnp.where(lane == 2, sg, cg)))
    stb[h] = pack.T[0:8]
    c_st = [send(stb.at[h], stb.at[h], "st", i, dev) for i, dev in enumerate((dev_sib, dev_x, dev_xs))]
    forward_u(1)
    products_sib(0)
    for cp in c_st:
        cp.wait_recv()
    st = [stb[i] for i in range(4)]
    mu = ((st[0][0:1] + st[1][0:1]) + (st[2][0:1] + st[3][0:1])) * 0.25
    m2t = jnp.zeros_like(mu)
    sgt = jnp.zeros_like(mu)
    cgt = jnp.zeros_like(mu)
    for i in range(4):
        delta = st[i][0:1] - mu
        m2t += st[i][1:2] + (H * delta) * delta
        sgt += st[i][2:3]
        cgt += st[i][3:4] + delta * st[i][2:3]
    rho = lax.rsqrt(m2t * (1.0 / (4 * H)) + LN_EPS)
    rows = jnp.concatenate([mu, rho, sgt * (1.0 / (4 * H)), cgt * rho * (1.0 / (4 * H)), jnp.zeros((124, T), F32)], axis=0)
    colst = rows.T
    mu_c, rho_c, mg_c, mgr_c = (colst[:, i:i + 1] for i in range(4))
    nrm = (r - mu_c) * rho_c
    dr = rho_c * (gdy - mg_c - nrm * mgr_c)
    nrm_ref[...] = nrm
    dr_ref[...] = dr
    d_ref[...] = dr.astype(BF)
    d_t = dr.T.astype(BF)

    c_dd, c_dx, c_df = {}, {}, {}
    mine, mine_k, theirs, theirs_k = (h, xn), (3, 1), (sib, xs), (2, 0)

    def dm_part(j):
        u0, u1 = CH[j]
        n = u1 - u0
        for i, q in enumerate(theirs + mine):
            r = dot(w2b[aligned(unit(j, q), n, 128), :], d_t).astype(BF).T
            for a in range(n):
                dmb[i, u0 + a] = r[:, a * 128:(a + 1) * 128]
            if i == 1:
                sent(c_ud[j, 0], c_ud[j, 1])
                for k in range(2):
                    c_dd[j, k] = send(dmb.at[k, u0:u1], dmr.at[k, u0:u1], "ud", 2 * j + k, dev_sib)

    def dm_sum(j):
        us = slice(*CH[j])
        sent(c_ux[j])
        for i in range(2):
            c_dd[j, i].wait_recv()
            xsb[us, :, i * 128:(i + 1) * 128] = (dmb[2 + i, us].astype(F32) + dmr[i, us].astype(F32)).astype(BF)
        c_dx[j] = send(xsb.at[us], xrb.at[us], "ux", j, dev_x)

    def dm_full(j):
        us = slice(*CH[j])
        c_dx[j].wait_recv()
        sent(c_md[j], c_mf[j])
        for i in range(2):
            q = mine[i]
            dmf[q, us] = (xsb[us, :, i * 128:(i + 1) * 128].astype(F32)
                          + xrb[us, :, (1 - i) * 128:(2 - i) * 128].astype(F32)).astype(BF)
        for i in range(2):
            q = mine[i]
            c_df[j, i] = send(dmf.at[q, us], dmf.at[q, us], "md", 2 * j + i, dev_sib)

    def grads(j, qs, ks, first):
        u0, u1 = CH[j]
        total = None
        dus = []
        for q in qs:
            parts = []
            for a in range(u0, u1):
                dm = dmf[q, a].astype(F32)
                du_f = pr_ref[q, a] * jnp.concatenate([dm, dm], axis=1)
                db1_ref[unit(j, q) + a - u0] = jnp.sum(du_f, axis=0, keepdims=True)
                du = du_f.astype(BF)
                du_ref[q, a] = du
                parts.append(du)
            dus.append(jnp.concatenate(parts, axis=1).T)
        for du_t, k in zip(dus, ks):
            part = dot(w1b[k, :, u0 * 256:u1 * 256], du_t)
            total = part if total is None else total + part
        acc[...] = total if first else acc[...] + total

    def grads_mine(j):
        dm_full(j)
        grads(j, mine, mine_k, j == 0)

    def grads_theirs(j):
        for i in range(2):
            c_df[j, i].wait_recv()
        grads(j, theirs, theirs_k, False)

    dm_part(0)
    dm_part(1)
    dm_sum(0)
    dm_part(2)
    dm_sum(1)
    dm_part(3)
    dm_sum(2)
    products_sib(1)
    dm_part(4)
    dm_sum(3)
    forward_u(2)
    dm_part(5)
    dm_sum(4)
    dm_sum(5)
    products_sib(2)
    grads_mine(0)
    for j in range(1, NC):
        grads_theirs(j - 1)
        grads_mine(j)
    grads_theirs(NC - 1)
    dxp_ref[...] = acc[...].T.astype(BF)
    for cp in live:
        cp.wait_send()


def comm_call(x, w1, b1, w2, b2, gam, dy):
    scratch = [pltpu.VMEM((T, H), BF), pltpu.VMEM((4 * NU, 1, 256), F32), pltpu.VMEM((1, H), F32), pltpu.VMEM((1, H), F32),
               pltpu.VMEM((T, H), BF),
               pltpu.VMEM((4, H, NU * 256), BF), pltpu.VMEM((4 * NU * 128, H), BF),
               pltpu.VMEM((4, NU, T, 256), BF), pltpu.VMEM((2, NU, T, 256), BF),
               pltpu.VMEM((NU, T, 256), BF), pltpu.VMEM((NU, T, 256), BF),
               pltpu.VMEM((2, T, 512), BF), pltpu.VMEM((2, T, 512), BF),
               pltpu.VMEM((4, 8, T), F32),
               pltpu.VMEM((4, NU, T, 128), BF), pltpu.VMEM((2, NU, T, 128), BF),
               pltpu.VMEM((4, NU, T, 256), BF), pltpu.VMEM((4, NU, T, 128), BF), pltpu.VMEM((4, NU, T, 256), F32),
               pltpu.VMEM((H, T), F32),
               pltpu.SemaphoreType.DMA((5,)), pltpu.SemaphoreType.DMA((NLS,))]
    for n in SEM_NAMES:
        scratch += [pltpu.SemaphoreType.DMA((N_SEM[n],)), pltpu.SemaphoreType.DMA((N_SEM[n],))]
    outs = [sds((4, NU, T, 128), BF), sds((4, NU, T, 256), BF), sds((T, H), BF), sds((T, H), F32), sds((T, H), F32),
            sds((4 * NU, 1, 256), F32), sds((T, H), BF)]
    return pl.pallas_call(
        comm_kernel, out_shape=outs, name="comm",
        in_specs=[HBM] * 7, out_specs=[VMEM] * 7, scratch_shapes=scratch,
        compiler_params=pltpu.CompilerParams(collective_id=0, has_side_effects=True, vmem_limit_bytes=COMM_LIM),
        cost_estimate=pl.CostEstimate(flops=8 * 10 ** 9, bytes_accessed=32 << 20, transcendentals=0),
    )(x, w1, b1, w2, b2, gam, dy)


NB2 = 6
NB1 = 6


def grads_kernel(m_ref, du_ref, d_ref, nrm_ref, dr_ref, db1_in, x_ref, gam_ref, beta_ref, dy_ref,
                 dw1_ref, dw2_ref, y_ref, db1_ref, db2_ref, dgam_ref, dbeta_ref,
                 ob2, ob1, xt, yb, db1b, sb, so2, so1, so0):
    tiles = [(j, q) for j in range(NC) for q in range(4)]

    def put2(t):
        j, q = tiles[t]
        n = CH[j][1] - CH[j][0]
        r0 = unit(j, q) * 128
        return pltpu.make_async_copy(ob2.at[t % NB2, :n * 128], dw2_ref.at[r0:r0 + n * 128, :], so2.at[t % NB2])

    def put1(t):
        j, q = tiles[t]
        n = CH[j][1] - CH[j][0]
        c0 = unit(j, q) * 256
        return pltpu.make_async_copy(ob1.at[t % NB1, :, :n * 256], dw1_ref.at[:, c0:c0 + n * 256], so1.at[t % NB1])

    small = [pltpu.make_async_copy(a, b, so0.at[i]) for i, (a, b) in enumerate(
        ((yb, y_ref), (db1b, db1_ref), (sb.at[0], db2_ref), (sb.at[1], dgam_ref), (sb.at[2], dbeta_ref)))]
    for t, (j, q) in enumerate(tiles):
        if t >= NB2:
            put2(t - NB2).wait()
        for i, a in enumerate(range(*CH[j])):
            ob2[t % NB2, i * 128:(i + 1) * 128] = dot(m_ref[q, a].T, d_ref[...])
        put2(t).start()
        if t == 6:
            xt[...] = x_ref[...].T
        if t == 8:
            yb[...] = (gam_ref[...] * nrm_ref[...] + beta_ref[...]).astype(BF)
            for i in range(4 * NU):
                db1b[:, i * 256:(i + 1) * 256] = db1_in[i]
            for cp in small[:2]:
                cp.start()
        if t == 10:
            dy = dy_ref[...].astype(F32)
            sb[0] = jnp.sum(dr_ref[...], axis=0, keepdims=True)
            sb[1] = jnp.sum(dy * nrm_ref[...], axis=0, keepdims=True)
            sb[2] = jnp.sum(dy, axis=0, keepdims=True)
            for cp in small[2:]:
                cp.start()
    for t, (j, q) in enumerate(tiles):
        if t >= NB1:
            put1(t - NB1).wait()
        for i, a in enumerate(range(*CH[j])):
            ob1[t % NB1, :, i * 256:(i + 1) * 256] = dot(xt[...], du_ref[q, a])
        put1(t).start()
    last = len(tiles)
    for t in range(last - NB2, last):
        put2(t).wait()
    for cp in small:
        cp.wait()
    for t in range(last - NB1, last):
        put1(t).wait()


def grads_call(m, du, d, nrm, dr, db1, x, gam, beta, dy):
    outs = [sds((H, 4 * NU * 256), F32), sds((4 * NU * 128, H), F32), sds((T, H), BF), sds((1, 4 * NU * 256), F32),
            sds((1, H), F32), sds((1, H), F32), sds((1, H), F32)]
    return pl.pallas_call(
        grads_kernel, out_shape=outs, name="grads",
        in_specs=[VMEM] * 10, out_specs=[HBM] * 7,
        scratch_shapes=[pltpu.VMEM((NB2, 256, H), F32), pltpu.VMEM((NB1, H, 512), F32), pltpu.VMEM((H, T), BF),
                        pltpu.VMEM((T, H), BF), pltpu.VMEM((1, 4 * NU * 256), F32), pltpu.VMEM((3, 1, H), F32),
                        pltpu.SemaphoreType.DMA((NB2,)), pltpu.SemaphoreType.DMA((NB1,)), pltpu.SemaphoreType.DMA((5,))],
        compiler_params=pltpu.CompilerParams(vmem_limit_bytes=GRADS_LIM),
        cost_estimate=pl.CostEstimate(flops=4 * 10 ** 9, bytes_accessed=66 << 20, transcendentals=0),
    )(m, du, d, nrm, dr, db1, x, gam, beta, dy)


def solution(mesh):
    data_spec = P('dp', 'hd')
    hid_spec = P('hd')
    in_specs = (data_spec, P('hd', 'ff'), P('ff'), P('ff', 'hd'), hid_spec, hid_spec, hid_spec, data_spec)
    out_specs = (data_spec, data_spec, P(('dp', 'hd'), 'ff'), P(('dp', 'ff'), 'hd'), P(('dp', 'ff')), P(('dp', 'hd')), P(('dp', 'hd')), P(('dp', 'hd')))

    def device_step(x, w1, b1, w2, b2, gam, beta, dy):
        b2, gam, beta = (a.reshape(1, H) for a in (b2, gam, beta))
        hbm = [pltpu.with_memory_space_constraint(a, pltpu.HBM) for a in (x, w1, b1.reshape(4 * NU, 1, 256), w2, b2, gam, dy)]
        m, du, d, dr, nrm, db1, dxp = comm_call(*hbm)
        dxr = lax.ppermute(dxp, 'ff', [(0, 1), (1, 0)])
        dw1, dw2, y, db1, db2, dgam, dbeta = grads_call(m, du, d, nrm, dr, db1, x, gam, beta, dy)
        dx = (ALPHA * dr + (dxp.astype(F32) + dxr.astype(F32))).astype(BF)
        return y, dx, dw1, dw2, db1.reshape(-1), db2.reshape(-1), dgam.reshape(-1), dbeta.reshape(-1)

    return jax.shard_map(device_step, mesh=mesh, in_specs=in_specs, out_specs=out_specs, check_vma=False)
```

```python
import functools
import math
import jax
import jax.numpy as jnp
from jax import lax
from jax.experimental import pallas as pl
from jax.experimental.pallas import tpu as pltpu
from jax.sharding import PartitionSpec as P

PAIR = 128
ALPHA = math.sqrt(140.0)
LN_EPS = 1e-5
C0 = math.sqrt(2.0 / math.pi)
C1 = 0.044715
MESH = pl.DeviceIdType.MESH
F32 = jnp.float32
BF = jnp.bfloat16
T = 128
H = 1024
NU = 10
CH = ((0, 1), (1, 3), (3, 5), (5, 7), (7, 9), (9, 10))
NC = len(CH)
COMM_LIM = 48 * 1024 * 1024
GRADS_LIM = 28 * 1024 * 1024

VMEM = pl.BlockSpec(memory_space=pltpu.VMEM)
ANY = pl.BlockSpec(memory_space=pl.ANY)
HBM = pl.BlockSpec(memory_space=pltpu.HBM)


def sds(shape, dtype):
    return jax.ShapeDtypeStruct(shape, dtype)


def dot(a, b):
    return jnp.dot(a, b, preferred_element_type=F32)


def gelu_both(g):
    g2 = g * g
    t = jnp.tanh(C0 * (g + C1 * (g2 * g)))
    cdf = 0.5 * (1.0 + t)
    slope = cdf + (0.5 * g) * (1.0 - t * t) * (C0 * (1.0 + (3.0 * C1) * g2))
    return g * cdf, slope


def places():
    h = lax.axis_index("hd")
    y = lax.axis_index("ff")
    c = lax.rem(h, 2)
    sib = h + 1 - 2 * c
    xn = lax.rem(h + 2, 4)
    xs = lax.rem(sib + 2, 4)
    return h, y, c, sib, xn, xs


def remote(src, dst, sems, k, dev):
    return pltpu.make_async_remote_copy(src_ref=src, dst_ref=dst, send_sem=sems[0].at[k], recv_sem=sems[1].at[k],
                                        device_id=dev, device_id_type=MESH)


def unit(j, q):
    u0, u1 = CH[j]
    return 4 * u0 + q * (u1 - u0)


def aligned(start, size, tile):
    return pl.ds(pl.multiple_of(start * tile, tile), size * tile)


GCH = ((0, 3), (3, 7), (7, 10))
HT = T // 2
NG = len(GCH)
NLS = 16
N_SEM = {"ud": 2 * NC, "ux": 2 * NC, "mx": 2 * NG, "md": 4 * NG, "gx": NG, "gd": NG, "gf": NG, "fy": 4, "st": 3}
SEM_NAMES = list(N_SEM)


def comm_kernel(x_hbm, w1_ref, b1_hbm, w2_ref, b2_hbm, gam_hbm, dy_hbm,
                m_ref, du_ref, d_ref, dr_ref, nrm_ref, db1_ref, dxp_ref,
                x_ref, b1_ref, b2_ref, gam_ref, dy_ref, w1b, w2b, ub, rb, xsb, xrb, fs, fr, stb, dmb, dmr, u_ref, dmf, pr_ref, acc,
                ls0, ls1, *sem_list):
    sems = {n: (sem_list[2 * i], sem_list[2 * i + 1]) for i, n in enumerate(SEM_NAMES)}
    h, y, c, sib, xn, xs = places()
    dev_sib, dev_x, dev_xs, dev_y = (0, y, sib), (0, y, xn), (0, y, xs), (0, 1 - y, h)
    order = [xs, xn, sib, h]

    load_order = []
    for j in range(NC + 1):
        load_order += [(j, k) for k in (0, 1) if j < NC] + [(j - 1, k) for k in (2, 3) if j > 0]

    def w1_load(j, k):
        u0, u1 = CH[j]
        n = u1 - u0
        return pltpu.make_async_copy(w1_ref.at[:, aligned(unit(j, order[k]), n, 256)], w1b.at[k, :, u0 * 256:u1 * 256],
                                     ls1.at[load_order.index((j, k)) % NLS])

    def w2_load(j):
        rows = slice(4 * 128 * CH[j][0], 4 * 128 * CH[j][1])
        return pltpu.make_async_copy(w2_ref.at[rows, :], w2b.at[rows, :], ls1.at[(4 * NC + j) % NLS])

    ins = [pltpu.make_async_copy(a, b, ls0.at[i]) for i, (a, b) in enumerate(
        ((x_hbm, x_ref), (b1_hbm, b1_ref), (b2_hbm, b2_ref), (gam_hbm, gam_ref), (dy_hbm, dy_ref)))]
    bar = pltpu.get_barrier_semaphore()
    for dev in (dev_sib, dev_x, dev_xs, dev_y):
        pl.semaphore_signal(bar, inc=1, device_id=dev, device_id_type=MESH)
    ins[0].start()
    for j, k in load_order[:6]:
        w1_load(j, k).start()
    loaded = [6]

    def load_more(n):
        for j, k in load_order[loaded[0]:loaded[0] + n]:
            w1_load(j, k).start()
        loaded[0] += n

    ins[0].wait()

    live = []

    def send(src, dst, name, k, dev):
        cp = remote(src, dst, sems[name], k, dev)
        cp.start()
        live.append(cp)
        return cp

    def sent(*cps):
        for cp in cps:
            cp.wait_send()
        live[:] = [cp for cp in live if not any(cp is old for old in cps)]

    def u_parts(*slabs):
        for j, k in slabs:
            w1_load(j, k).wait()
        load_more(4)
        for j, k in slabs:
            u0, u1 = CH[j]
            r = dot(x_ref[...], w1b[k, :, u0 * 256:u1 * 256]).astype(BF)
            for i in range(u1 - u0):
                ub[k, u0 + i] = r[:, i * 256:(i + 1) * 256]
        if slabs[0] == (0, 0):
            pl.semaphore_wait(bar, 4)
            for cp in ins[1:]:
                cp.start()
        for j, k in slabs:
            us = slice(*CH[j])
            if k == 0:
                c_ud[j, 1] = send(ub.at[0, us], rb.at[1, us], "ud", 2 * j + 1, dev_sib)
            if k == 2:
                c_ud[j, 0] = send(ub.at[2, us], rb.at[0, us], "ud", 2 * j, dev_sib)

    def s1(j):
        us = slice(*CH[j])
        c_ud[j, 1].wait_recv()
        xsb[us] = (ub[1, us].astype(F32) + rb[1, us].astype(F32)).astype(BF)
        send_x(0, j)

    def half(a):
        return slice(a * HT, (a + 1) * HT)

    def send_x(a, j):
        us = slice(*CH[j])
        c_ux[a, j] = send(xsb.at[us, half(a)], xrb.at[us, half(a)], "ux", a * NC + j, dev_x)

    def s2(a, j):
        rows = half(a)
        u0, u1 = CH[j]
        if a == 0:
            c_ud[j, 0].wait_recv()
        c_ux[a, j].wait_recv()
        for i in range(u1 - u0):
            n = u0 + i
            u = (ub[3, n, rows].astype(F32) + rb[0, n, rows].astype(F32) + xrb[n, rows].astype(F32)
                 + b1_ref[unit(j, h) + i])
            u = u.astype(BF)
            u_ref[h, n, rows] = u
            u = u.astype(F32)
            val, slope = gelu_both(u[:, PAIR:])
            m_ref[h, n, rows] = (u[:, :PAIR] * val).astype(BF)
            pr_ref[h, n, rows, :PAIR] = val
            pr_ref[h, n, rows, PAIR:] = u[:, :PAIR] * slope
        if j % 2 == 1:
            g = j // 2
            part = m_ref.at[h, slice(*GCH[g]), rows]
            c_mx[a, g] = send(part, part, "mx", a * NG + g, dev_x)
            c_md[a, g] = send(part, part, "md", a * NG + g, dev_sib)

    def s3(a, g):
        c_mx[a, g].wait_recv()
        part = m_ref.at[xn, slice(*GCH[g]), half(a)]
        c_mf[a, g] = send(part, part, "md", (2 + a) * NG + g, dev_sib)

    def s4(a, g):
        rows = half(a)
        c_md[a, g].wait_recv()
        c_mf[a, g].wait_recv()
        if a == 0:
            for j in (2 * g, 2 * g + 1):
                w2_load(j).wait()
        m = jnp.concatenate([m_ref[q, n, rows] for j in (2 * g, 2 * g + 1) for q in range(4) for n in range(*CH[j])], axis=1)
        u0, u1 = GCH[g]
        for n in range(2):
            cols = slice(n * 512, (n + 1) * 512)
            part = dot(m, w2b[4 * 128 * u0:4 * 128 * u1, cols])
            if g > 0:
                part = nrm_ref[rows, cols] + part
            if g < NG - 1:
                nrm_ref[rows, cols] = part
            else:
                fs[a, n] = part.astype(BF)
                c_fy[a, n] = send(fs.at[a, n], fr.at[a, n], "fy", 2 * a + n, dev_y)

    def gather_u(j):
        us = slice(*GCH[j])
        c_gx[j] = send(u_ref.at[h, us], u_ref.at[h, us], "gx", j, dev_x)
        c_gd[j] = send(u_ref.at[h, us], u_ref.at[h, us], "gd", j, dev_sib)

    def forward_u(j):
        us = slice(*GCH[j])
        c_gx[j].wait_recv()
        c_gf[j] = send(u_ref.at[xn, us], u_ref.at[xn, us], "gf", j, dev_sib)
        products(j, xn)

    def products(j, q):
        for a in range(*GCH[j]):
            u = u_ref[q, a].astype(F32)
            val, slope = gelu_both(u[:, PAIR:])
            pr_ref[q, a, :, :PAIR] = val
            pr_ref[q, a, :, PAIR:] = u[:, :PAIR] * slope

    def products_sib(j):
        c_gd[j].wait_recv()
        c_gf[j].wait_recv()
        products(j, sib)
        products(j, xs)

    c_ud, c_ux, c_mx, c_md, c_mf, c_fy, c_gx, c_gd, c_gf = {}, {}, {}, {}, {}, {}, {}, {}, {}
    u_parts((0, 0), (0, 1))
    u_parts((1, 0), (1, 1), (0, 2), (0, 3))
    s1(0)
    u_parts((2, 0), (2, 1), (1, 2), (1, 3))
    s1(1)
    u_parts((3, 0), (3, 1), (2, 2), (2, 3))
    s1(2)
    for j in range(NC):
        w2_load(j).start()
    u_parts((4, 0), (4, 1), (3, 2), (3, 3))
    s1(3)
    u_parts((5, 0), (5, 1), (4, 2), (4, 3))
    s1(4)
    send_x(1, 0)
    u_parts((5, 2), (5, 3))
    s1(5)
    for j in range(1, NC):
        send_x(1, j)
    ins[1].wait()
    for a in range(2):
        for j in range(NC):
            s2(a, j)
    for g in range(NG):
        gather_u(g)
    for a in range(2):
        s3(a, 0)
        s3(a, 1)
        s4(a, 0)
        s3(a, 2)
        s4(a, 1)
        s4(a, 2)
    for cp in ins[2:]:
        cp.wait()

    forward_u(0)
    for a in range(2):
        for n in range(2):
            rows, cols = half(a), slice(n * 512, (n + 1) * 512)
            c_fy[a, n].wait_recv()
            f = fs[a, n].astype(F32) + fr[a, n].astype(F32)
            nrm_ref[rows, cols] = ALPHA * x_ref[rows, cols].astype(F32) + f + b2_ref[:, cols]
    r = nrm_ref[...]
    gdy = dy_ref[...].astype(F32) * gam_ref[...]
    m_loc = jnp.sum(r, axis=1, keepdims=True) * (1.0 / H)
    cen = r - m_loc
    m2 = jnp.sum(cen * cen, axis=1, keepdims=True)
    sg = jnp.sum(gdy, axis=1, keepdims=True)
    cg = jnp.sum(gdy * cen, axis=1, keepdims=True)
    lane = lax.broadcasted_iota(jnp.int32, (T, 128), 1)
    pack = jnp.where(lane == 0, m_loc, jnp.where(lane == 1, m2, jnp.where(lane == 2, sg, cg)))
    stb[h] = pack.T[0:8]
    c_st = [send(stb.at[h], stb.at[h], "st", i, dev) for i, dev in enumerate((dev_sib, dev_x, dev_xs))]
    forward_u(1)
    products_sib(0)
    for cp in c_st:
        cp.wait_recv()
    st = [stb[i] for i in range(4)]
    mu = ((st[0][0:1] + st[1][0:1]) + (st[2][0:1] + st[3][0:1])) * 0.25
    m2t = jnp.zeros_like(mu)
    sgt = jnp.zeros_like(mu)
    cgt = jnp.zeros_like(mu)
    for i in range(4):
        delta = st[i][0:1] - mu
        m2t += st[i][1:2] + (H * delta) * delta
        sgt += st[i][2:3]
        cgt += st[i][3:4] + delta * st[i][2:3]
    rho = lax.rsqrt(m2t * (1.0 / (4 * H)) + LN_EPS)
    rows = jnp.concatenate([mu, rho, sgt * (1.0 / (4 * H)), cgt * rho * (1.0 / (4 * H)), jnp.zeros((124, T), F32)], axis=0)
    colst = rows.T
    mu_c, rho_c, mg_c, mgr_c = (colst[:, i:i + 1] for i in range(4))
    nrm = (r - mu_c) * rho_c
    dr = rho_c * (gdy - mg_c - nrm * mgr_c)
    nrm_ref[...] = nrm
    dr_ref[...] = dr
    d_ref[...] = dr.astype(BF)
    d_t = dr.T.astype(BF)

    c_dd, c_dx, c_df = {}, {}, {}
    mine, mine_k, theirs, theirs_k = (h, xn), (3, 1), (sib, xs), (2, 0)

    def dm_part(j):
        u0, u1 = CH[j]
        n = u1 - u0
        for i, q in enumerate(theirs + mine):
            r = dot(w2b[aligned(unit(j, q), n, 128), :], d_t).astype(BF).T
            for a in range(n):
                dmb[i, u0 + a] = r[:, a * 128:(a + 1) * 128]
            if i == 1:
                sent(c_ud[j, 0], c_ud[j, 1])
                for k in range(2):
                    c_dd[j, k] = send(dmb.at[k, u0:u1], dmr.at[k, u0:u1], "ud", 2 * j + k, dev_sib)

    def dm_sum(j):
        us = slice(*CH[j])
        sent(c_ux[0, j], c_ux[1, j])
        for i in range(2):
            c_dd[j, i].wait_recv()
            xsb[us, :, i * 128:(i + 1) * 128] = (dmb[2 + i, us].astype(F32) + dmr[i, us].astype(F32)).astype(BF)
        c_dx[j] = send(xsb.at[us], xrb.at[us], "ux", j, dev_x)

    def dm_full(j):
        us = slice(*CH[j])
        c_dx[j].wait_recv()
        if j == 0:
            sent(*c_md.values(), *c_mf.values())
        for i in range(2):
            q = mine[i]
            dmf[q, us] = (xsb[us, :, i * 128:(i + 1) * 128].astype(F32)
                          + xrb[us, :, (1 - i) * 128:(2 - i) * 128].astype(F32)).astype(BF)
        for i in range(2):
            q = mine[i]
            c_df[j, i] = send(dmf.at[q, us], dmf.at[q, us], "md", 2 * j + i, dev_sib)

    def grads(j, qs, ks, first):
        u0, u1 = CH[j]
        total = None
        dus = []
        for q in qs:
            parts = []
            for a in range(u0, u1):
                dm = dmf[q, a].astype(F32)
                du_f = pr_ref[q, a] * jnp.concatenate([dm, dm], axis=1)
                db1_ref[unit(j, q) + a - u0] = jnp.sum(du_f, axis=0, keepdims=True)
                du = du_f.astype(BF)
                du_ref[q, a] = du
                parts.append(du)
            dus.append(jnp.concatenate(parts, axis=1).T)
        for du_t, k in zip(dus, ks):
            part = dot(w1b[k, :, u0 * 256:u1 * 256], du_t)
            total = part if total is None else total + part
        acc[...] = total if first else acc[...] + total

    def grads_mine(j):
        grads(j, mine, mine_k, j == 0)

    def grads_theirs(j):
        for i in range(2):
            c_df[j, i].wait_recv()
        grads(j, theirs, theirs_k, False)

    dm_part(0)
    dm_part(1)
    dm_sum(0)
    dm_part(2)
    dm_sum(1)
    dm_part(3)
    dm_sum(2)
    products_sib(1)
    dm_part(4)
    dm_sum(3)
    forward_u(2)
    dm_part(5)
    dm_sum(4)
    dm_sum(5)
    products_sib(2)
    dm_full(0)
    grads_mine(0)
    for j in range(1, NC):
        if j == NC - 1:
            dm_full(j)
        grads_theirs(j - 1)
        if j < NC - 1:
            dm_full(j)
        grads_mine(j)
    grads_theirs(NC - 1)
    dxp_ref[...] = acc[...].T.astype(BF)
    for cp in live:
        cp.wait_send()


def comm_call(x, w1, b1, w2, b2, gam, dy):
    scratch = [pltpu.VMEM((T, H), BF), pltpu.VMEM((4 * NU, 1, 256), F32), pltpu.VMEM((1, H), F32), pltpu.VMEM((1, H), F32),
               pltpu.VMEM((T, H), BF),
               pltpu.VMEM((4, H, NU * 256), BF), pltpu.VMEM((4 * NU * 128, H), BF),
               pltpu.VMEM((4, NU, T, 256), BF), pltpu.VMEM((2, NU, T, 256), BF),
               pltpu.VMEM((NU, T, 256), BF), pltpu.VMEM((NU, T, 256), BF),
               pltpu.VMEM((2, 2, HT, 512), BF), pltpu.VMEM((2, 2, HT, 512), BF),
               pltpu.VMEM((4, 8, T), F32),
               pltpu.VMEM((4, NU, T, 128), BF), pltpu.VMEM((2, NU, T, 128), BF),
               pltpu.VMEM((4, NU, T, 256), BF), pltpu.VMEM((4, NU, T, 128), BF), pltpu.VMEM((4, NU, T, 256), F32),
               pltpu.VMEM((H, T), F32),
               pltpu.SemaphoreType.DMA((5,)), pltpu.SemaphoreType.DMA((NLS,))]
    for n in SEM_NAMES:
        scratch += [pltpu.SemaphoreType.DMA((N_SEM[n],)), pltpu.SemaphoreType.DMA((N_SEM[n],))]
    outs = [sds((4, NU, T, 128), BF), sds((4, NU, T, 256), BF), sds((T, H), BF), sds((T, H), F32), sds((T, H), F32),
            sds((4 * NU, 1, 256), F32), sds((T, H), BF)]
    return pl.pallas_call(
        comm_kernel, out_shape=outs, name="comm",
        in_specs=[HBM] * 7, out_specs=[VMEM] * 7, scratch_shapes=scratch,
        compiler_params=pltpu.CompilerParams(collective_id=0, has_side_effects=True, vmem_limit_bytes=COMM_LIM),
        cost_estimate=pl.CostEstimate(flops=8 * 10 ** 9, bytes_accessed=32 << 20, transcendentals=0),
    )(x, w1, b1, w2, b2, gam, dy)


NB2 = 6
NB1 = 6


def grads_kernel(m_ref, du_ref, d_ref, nrm_ref, dr_ref, db1_in, x_ref, gam_ref, beta_ref, dy_ref,
                 dw1_ref, dw2_ref, y_ref, db1_ref, db2_ref, dgam_ref, dbeta_ref,
                 ob2, ob1, xt, yb, db1b, sb, so2, so1, so0):
    tiles = [(j, q) for j in range(NC) for q in range(4)]

    def put2(t):
        j, q = tiles[t]
        n = CH[j][1] - CH[j][0]
        r0 = unit(j, q) * 128
        return pltpu.make_async_copy(ob2.at[t % NB2, :n * 128], dw2_ref.at[r0:r0 + n * 128, :], so2.at[t % NB2])

    def put1(t):
        j, q = tiles[t]
        n = CH[j][1] - CH[j][0]
        c0 = unit(j, q) * 256
        return pltpu.make_async_copy(ob1.at[t % NB1, :, :n * 256], dw1_ref.at[:, c0:c0 + n * 256], so1.at[t % NB1])

    small = [pltpu.make_async_copy(a, b, so0.at[i]) for i, (a, b) in enumerate(
        ((yb, y_ref), (db1b, db1_ref), (sb.at[0], db2_ref), (sb.at[1], dgam_ref), (sb.at[2], dbeta_ref)))]
    for t, (j, q) in enumerate(tiles):
        if t >= NB2:
            put2(t - NB2).wait()
        for i, a in enumerate(range(*CH[j])):
            ob2[t % NB2, i * 128:(i + 1) * 128] = dot(m_ref[q, a].T, d_ref[...])
        put2(t).start()
        if t == 6:
            xt[...] = x_ref[...].T
        if t == 8:
            yb[...] = (gam_ref[...] * nrm_ref[...] + beta_ref[...]).astype(BF)
            for i in range(4 * NU):
                db1b[:, i * 256:(i + 1) * 256] = db1_in[i]
            for cp in small[:2]:
                cp.start()
        if t == 10:
            dy = dy_ref[...].astype(F32)
            sb[0] = jnp.sum(dr_ref[...], axis=0, keepdims=True)
            sb[1] = jnp.sum(dy * nrm_ref[...], axis=0, keepdims=True)
            sb[2] = jnp.sum(dy, axis=0, keepdims=True)
            for cp in small[2:]:
                cp.start()
    for t, (j, q) in enumerate(tiles):
        if t >= NB1:
            put1(t - NB1).wait()
        for i, a in enumerate(range(*CH[j])):
            ob1[t % NB1, :, i * 256:(i + 1) * 256] = dot(xt[...], du_ref[q, a])
        put1(t).start()
    last = len(tiles)
    for t in range(last - NB2, last):
        put2(t).wait()
    for cp in small:
        cp.wait()
    for t in range(last - NB1, last):
        put1(t).wait()


def grads_call(m, du, d, nrm, dr, db1, x, gam, beta, dy):
    outs = [sds((H, 4 * NU * 256), F32), sds((4 * NU * 128, H), F32), sds((T, H), BF), sds((1, 4 * NU * 256), F32),
            sds((1, H), F32), sds((1, H), F32), sds((1, H), F32)]
    return pl.pallas_call(
        grads_kernel, out_shape=outs, name="grads",
        in_specs=[VMEM] * 10, out_specs=[HBM] * 7,
        scratch_shapes=[pltpu.VMEM((NB2, 256, H), F32), pltpu.VMEM((NB1, H, 512), F32), pltpu.VMEM((H, T), BF),
                        pltpu.VMEM((T, H), BF), pltpu.VMEM((1, 4 * NU * 256), F32), pltpu.VMEM((3, 1, H), F32),
                        pltpu.SemaphoreType.DMA((NB2,)), pltpu.SemaphoreType.DMA((NB1,)), pltpu.SemaphoreType.DMA((5,))],
        compiler_params=pltpu.CompilerParams(vmem_limit_bytes=GRADS_LIM),
        cost_estimate=pl.CostEstimate(flops=4 * 10 ** 9, bytes_accessed=66 << 20, transcendentals=0),
    )(m, du, d, nrm, dr, db1, x, gam, beta, dy)


def solution(mesh):
    data_spec = P('dp', 'hd')
    hid_spec = P('hd')
    in_specs = (data_spec, P('hd', 'ff'), P('ff'), P('ff', 'hd'), hid_spec, hid_spec, hid_spec, data_spec)
    out_specs = (data_spec, data_spec, P(('dp', 'hd'), 'ff'), P(('dp', 'ff'), 'hd'), P(('dp', 'ff')), P(('dp', 'hd')), P(('dp', 'hd')), P(('dp', 'hd')))

    def device_step(x, w1, b1, w2, b2, gam, beta, dy):
        b2, gam, beta = (a.reshape(1, H) for a in (b2, gam, beta))
        hbm = [pltpu.with_memory_space_constraint(a, pltpu.HBM) for a in (x, w1, b1.reshape(4 * NU, 1, 256), w2, b2, gam, dy)]
        m, du, d, dr, nrm, db1, dxp = comm_call(*hbm)
        dxr = lax.ppermute(dxp, 'ff', [(0, 1), (1, 0)])
        dw1, dw2, y, db1, db2, dgam, dbeta = grads_call(m, du, d, nrm, dr, db1, x, gam, beta, dy)
        dx = (ALPHA * dr + (dxp.astype(F32) + dxr.astype(F32))).astype(BF)
        return y, dx, dw1, dw2, db1.reshape(-1), db2.reshape(-1), dgam.reshape(-1), dbeta.reshape(-1)

    return jax.shard_map(device_step, mesh=mesh, in_specs=in_specs, out_specs=out_specs, check_vma=False)
```

```python
import functools
import math
import jax
import jax.numpy as jnp
from jax import lax
from jax.experimental import pallas as pl
from jax.experimental.pallas import tpu as pltpu
from jax.sharding import PartitionSpec as P

PAIR = 128
ALPHA = math.sqrt(140.0)
LN_EPS = 1e-5
C0 = math.sqrt(2.0 / math.pi)
C1 = 0.044715
MESH = pl.DeviceIdType.MESH
F32 = jnp.float32
BF = jnp.bfloat16
T = 128
H = 1024
NU = 10
CH = ((0, 1), (1, 3), (3, 5), (5, 7), (7, 9), (9, 10))
NC = len(CH)
COMM_LIM = 48 * 1024 * 1024
GRADS_LIM = 28 * 1024 * 1024

VMEM = pl.BlockSpec(memory_space=pltpu.VMEM)
ANY = pl.BlockSpec(memory_space=pl.ANY)
HBM = pl.BlockSpec(memory_space=pltpu.HBM)


def sds(shape, dtype):
    return jax.ShapeDtypeStruct(shape, dtype)


def dot(a, b):
    return jnp.dot(a, b, preferred_element_type=F32)


def gelu_both(g):
    g2 = g * g
    t = jnp.tanh(C0 * (g + C1 * (g2 * g)))
    cdf = 0.5 * (1.0 + t)
    slope = cdf + (0.5 * g) * (1.0 - t * t) * (C0 * (1.0 + (3.0 * C1) * g2))
    return g * cdf, slope


def places():
    h = lax.axis_index("hd")
    y = lax.axis_index("ff")
    c = lax.rem(h, 2)
    sib = h + 1 - 2 * c
    xn = lax.rem(h + 2, 4)
    xs = lax.rem(sib + 2, 4)
    return h, y, c, sib, xn, xs


def remote(src, dst, sems, k, dev):
    return pltpu.make_async_remote_copy(src_ref=src, dst_ref=dst, send_sem=sems[0].at[k], recv_sem=sems[1].at[k],
                                        device_id=dev, device_id_type=MESH)


def unit(j, q):
    u0, u1 = CH[j]
    return 4 * u0 + q * (u1 - u0)


def aligned(start, size, tile):
    return pl.ds(pl.multiple_of(start * tile, tile), size * tile)


GCH = ((0, 3), (3, 7), (7, 10))
HT = T // 2
NG = len(GCH)
NLS = 16
N_SEM = {"ud": 2 * NC, "ux": 2 * NC, "mx": 2 * NG, "md": 4 * NG, "gx": NG, "gd": NG, "gf": NG, "fy": 4, "st": 3}
SEM_NAMES = list(N_SEM)


def comm_kernel(x_hbm, w1_ref, b1_hbm, w2_ref, b2_hbm, gam_hbm, dy_hbm,
                m_ref, du_ref, d_ref, dr_ref, nrm_ref, db1_ref, dxp_ref,
                x_ref, b1_ref, b2_ref, gam_ref, dy_ref, w1b, w2b, ub, rb, xsb, xrb, fs, fr, stb, dmb, dmr, u_ref, dmf, pr_ref, acc,
                ls0, ls1, *sem_list):
    sems = {n: (sem_list[2 * i], sem_list[2 * i + 1]) for i, n in enumerate(SEM_NAMES)}
    h, y, c, sib, xn, xs = places()
    dev_sib, dev_x, dev_xs, dev_y = (0, y, sib), (0, y, xn), (0, y, xs), (0, 1 - y, h)
    order = [xs, xn, sib, h]

    load_order = []
    for j in range(NC + 1):
        load_order += [(j, k) for k in (0, 1) if j < NC] + [(j - 1, k) for k in (2, 3) if j > 0]

    def w1_load(j, k):
        u0, u1 = CH[j]
        n = u1 - u0
        return pltpu.make_async_copy(w1_ref.at[:, aligned(unit(j, order[k]), n, 256)], w1b.at[k, :, u0 * 256:u1 * 256],
                                     ls1.at[load_order.index((j, k)) % NLS])

    def w2_load(j):
        rows = slice(4 * 128 * CH[j][0], 4 * 128 * CH[j][1])
        return pltpu.make_async_copy(w2_ref.at[rows, :], w2b.at[rows, :], ls1.at[(4 * NC + j) % NLS])

    ins = [pltpu.make_async_copy(a, b, ls0.at[i]) for i, (a, b) in enumerate(
        ((x_hbm, x_ref), (b1_hbm, b1_ref), (b2_hbm, b2_ref), (gam_hbm, gam_ref), (dy_hbm, dy_ref)))]
    bar = pltpu.get_barrier_semaphore()
    for dev in (dev_sib, dev_x, dev_xs, dev_y):
        pl.semaphore_signal(bar, inc=1, device_id=dev, device_id_type=MESH)
    ins[0].start()
    for j, k in load_order[:6]:
        w1_load(j, k).start()
    loaded = [6]

    def load_more(n):
        for j, k in load_order[loaded[0]:loaded[0] + n]:
            w1_load(j, k).start()
        loaded[0] += n

    ins[0].wait()

    live = []

    def send(src, dst, name, k, dev):
        cp = remote(src, dst, sems[name], k, dev)
        cp.start()
        live.append(cp)
        return cp

    def sent(*cps):
        for cp in cps:
            cp.wait_send()
        live[:] = [cp for cp in live if not any(cp is old for old in cps)]

    def u_parts(*slabs):
        for j, k in slabs:
            w1_load(j, k).wait()
        load_more(4)
        for j, k in slabs:
            u0, u1 = CH[j]
            r = dot(x_ref[...], w1b[k, :, u0 * 256:u1 * 256]).astype(BF)
            for i in range(u1 - u0):
                ub[k, u0 + i] = r[:, i * 256:(i + 1) * 256]
        if slabs[0] == (0, 0):
            pl.semaphore_wait(bar, 4)
            for cp in ins[1:]:
                cp.start()
        for j, k in slabs:
            us = slice(*CH[j])
            if k == 0:
                c_ud[j, 1] = send(ub.at[0, us], rb.at[1, us], "ud", 2 * j + 1, dev_sib)
            if k == 2:
                c_ud[j, 0] = send(ub.at[2, us], rb.at[0, us], "ud", 2 * j, dev_sib)

    def s1(j):
        us = slice(*CH[j])
        c_ud[j, 1].wait_recv()
        xsb[us] = (ub[1, us].astype(F32) + rb[1, us].astype(F32)).astype(BF)
        send_x(0, j)

    def half(a):
        return slice(a * HT, (a + 1) * HT)

    def send_x(a, j):
        us = slice(*CH[j])
        c_ux[a, j] = send(xsb.at[us, half(a)], xrb.at[us, half(a)], "ux", a * NC + j, dev_x)

    def s2(a, j):
        rows = half(a)
        u0, u1 = CH[j]
        if a == 0:
            c_ud[j, 0].wait_recv()
        c_ux[a, j].wait_recv()
        for i in range(u1 - u0):
            n = u0 + i
            u = (ub[3, n, rows].astype(F32) + rb[0, n, rows].astype(F32) + xrb[n, rows].astype(F32)
                 + b1_ref[unit(j, h) + i])
            u = u.astype(BF)
            u_ref[h, n, rows] = u
            u = u.astype(F32)
            val, slope = gelu_both(u[:, PAIR:])
            m_ref[h, n, rows] = (u[:, :PAIR] * val).astype(BF)
            pr_ref[h, n, rows, :PAIR] = val
            pr_ref[h, n, rows, PAIR:] = u[:, :PAIR] * slope
        if j % 2 == 1:
            g = j // 2
            part = m_ref.at[h, slice(*GCH[g]), rows]
            c_mx[a, g] = send(part, part, "mx", a * NG + g, dev_x)
            c_md[a, g] = send(part, part, "md", a * NG + g, dev_sib)

    def s3(a, g):
        c_mx[a, g].wait_recv()
        part = m_ref.at[xn, slice(*GCH[g]), half(a)]
        c_mf[a, g] = send(part, part, "md", (2 + a) * NG + g, dev_sib)

    def s4(a, g):
        rows = half(a)
        c_md[a, g].wait_recv()
        c_mf[a, g].wait_recv()
        if a == 0:
            for j in (2 * g, 2 * g + 1):
                w2_load(j).wait()
        m = jnp.concatenate([m_ref[q, n, rows] for j in (2 * g, 2 * g + 1) for q in range(4) for n in range(*CH[j])], axis=1)
        u0, u1 = GCH[g]
        for n in range(2):
            cols = slice(n * 512, (n + 1) * 512)
            part = dot(m, w2b[4 * 128 * u0:4 * 128 * u1, cols])
            if g > 0:
                part = nrm_ref[rows, cols] + part
            if g < NG - 1:
                nrm_ref[rows, cols] = part
            else:
                fs[a, n] = part.astype(BF)
                c_fy[a, n] = send(fs.at[a, n], fr.at[a, n], "fy", 2 * a + n, dev_y)

    def gather_u(j):
        us = slice(*GCH[j])
        c_gx[j] = send(u_ref.at[h, us], u_ref.at[h, us], "gx", j, dev_x)
        c_gd[j] = send(u_ref.at[h, us], u_ref.at[h, us], "gd", j, dev_sib)

    def forward_u(j):
        us = slice(*GCH[j])
        c_gx[j].wait_recv()
        c_gf[j] = send(u_ref.at[xn, us], u_ref.at[xn, us], "gf", j, dev_sib)
        products(j, xn)

    def products(j, q):
        for a in range(*GCH[j]):
            u = u_ref[q, a].astype(F32)
            val, slope = gelu_both(u[:, PAIR:])
            pr_ref[q, a, :, :PAIR] = val
            pr_ref[q, a, :, PAIR:] = u[:, :PAIR] * slope

    def products_sib(j):
        c_gd[j].wait_recv()
        c_gf[j].wait_recv()
        products(j, sib)
        products(j, xs)

    c_ud, c_ux, c_mx, c_md, c_mf, c_fy, c_gx, c_gd, c_gf = {}, {}, {}, {}, {}, {}, {}, {}, {}
    u_parts((0, 0), (0, 1))
    u_parts((1, 0), (1, 1), (0, 2), (0, 3))
    s1(0)
    u_parts((2, 0), (2, 1), (1, 2), (1, 3))
    s1(1)
    send_x(1, 0)
    u_parts((3, 0), (3, 1), (2, 2), (2, 3))
    s1(2)
    for j in range(NC):
        w2_load(j).start()
    u_parts((4, 0), (4, 1), (3, 2), (3, 3))
    s1(3)
    send_x(1, 1)
    u_parts((5, 0), (5, 1), (4, 2), (4, 3))
    s1(4)
    u_parts((5, 2), (5, 3))
    s1(5)
    for j in range(2, NC):
        send_x(1, j)
    ins[1].wait()
    for a in range(2):
        for j in range(NC):
            s2(a, j)
    for g in range(NG):
        gather_u(g)
    for a in range(2):
        s3(a, 0)
        s3(a, 1)
        s4(a, 0)
        s3(a, 2)
        s4(a, 1)
        s4(a, 2)
    for cp in ins[2:]:
        cp.wait()

    forward_u(0)
    for a in range(2):
        for n in range(2):
            rows, cols = half(a), slice(n * 512, (n + 1) * 512)
            c_fy[a, n].wait_recv()
            f = fs[a, n].astype(F32) + fr[a, n].astype(F32)
            nrm_ref[rows, cols] = ALPHA * x_ref[rows, cols].astype(F32) + f + b2_ref[:, cols]
    r = nrm_ref[...]
    gdy = dy_ref[...].astype(F32) * gam_ref[...]
    m_loc = jnp.sum(r, axis=1, keepdims=True) * (1.0 / H)
    cen = r - m_loc
    m2 = jnp.sum(cen * cen, axis=1, keepdims=True)
    sg = jnp.sum(gdy, axis=1, keepdims=True)
    cg = jnp.sum(gdy * cen, axis=1, keepdims=True)
    lane = lax.broadcasted_iota(jnp.int32, (T, 128), 1)
    pack = jnp.where(lane == 0, m_loc, jnp.where(lane == 1, m2, jnp.where(lane == 2, sg, cg)))
    stb[h] = pack.T[0:8]
    c_st = [send(stb.at[h], stb.at[h], "st", i, dev) for i, dev in enumerate((dev_sib, dev_x, dev_xs))]
    products_sib(0)
    for cp in c_st:
        cp.wait_recv()
    st = [stb[i] for i in range(4)]
    mu = ((st[0][0:1] + st[1][0:1]) + (st[2][0:1] + st[3][0:1])) * 0.25
    m2t = jnp.zeros_like(mu)
    sgt = jnp.zeros_like(mu)
    cgt = jnp.zeros_like(mu)
    for i in range(4):
        delta = st[i][0:1] - mu
        m2t += st[i][1:2] + (H * delta) * delta
        sgt += st[i][2:3]
        cgt += st[i][3:4] + delta * st[i][2:3]
    rho = lax.rsqrt(m2t * (1.0 / (4 * H)) + LN_EPS)
    rows = jnp.concatenate([mu, rho, sgt * (1.0 / (4 * H)), cgt * rho * (1.0 / (4 * H)), jnp.zeros((124, T), F32)], axis=0)
    colst = rows.T
    mu_c, rho_c, mg_c, mgr_c = (colst[:, i:i + 1] for i in range(4))
    nrm = (r - mu_c) * rho_c
    dr = rho_c * (gdy - mg_c - nrm * mgr_c)
    nrm_ref[...] = nrm
    dr_ref[...] = dr
    d_ref[...] = dr.astype(BF)
    d_t = dr.T.astype(BF)

    c_dd, c_dx, c_df = {}, {}, {}
    mine, mine_k, theirs, theirs_k = (h, xn), (3, 1), (sib, xs), (2, 0)

    def dm_part(j):
        u0, u1 = CH[j]
        n = u1 - u0
        for i, q in enumerate(theirs + mine):
            r = dot(w2b[aligned(unit(j, q), n, 128), :], d_t).astype(BF).T
            for a in range(n):
                dmb[i, u0 + a] = r[:, a * 128:(a + 1) * 128]
            if i == 1:
                sent(c_ud[j, 0], c_ud[j, 1])
                for k in range(2):
                    c_dd[j, k] = send(dmb.at[k, u0:u1], dmr.at[k, u0:u1], "ud", 2 * j + k, dev_sib)

    def dm_sum(j):
        us = slice(*CH[j])
        sent(c_ux[0, j], c_ux[1, j])
        for i in range(2):
            c_dd[j, i].wait_recv()
            xsb[us, :, i * 128:(i + 1) * 128] = (dmb[2 + i, us].astype(F32) + dmr[i, us].astype(F32)).astype(BF)
        c_dx[j] = send(xsb.at[us], xrb.at[us], "ux", j, dev_x)

    def dm_full(j):
        us = slice(*CH[j])
        c_dx[j].wait_recv()
        if j == 0:
            sent(*c_md.values(), *c_mf.values())
        for i in range(2):
            q = mine[i]
            dmf[q, us] = (xsb[us, :, i * 128:(i + 1) * 128].astype(F32)
                          + xrb[us, :, (1 - i) * 128:(2 - i) * 128].astype(F32)).astype(BF)
        for i in range(2):
            q = mine[i]
            c_df[j, i] = send(dmf.at[q, us], dmf.at[q, us], "md", 2 * j + i, dev_sib)

    def grads(j, qs, ks, first):
        u0, u1 = CH[j]
        total = None
        dus = []
        for q in qs:
            parts = []
            for a in range(u0, u1):
                dm = dmf[q, a].astype(F32)
                du_f = pr_ref[q, a] * jnp.concatenate([dm, dm], axis=1)
                db1_ref[unit(j, q) + a - u0] = jnp.sum(du_f, axis=0, keepdims=True)
                du = du_f.astype(BF)
                du_ref[q, a] = du
                parts.append(du)
            dus.append(jnp.concatenate(parts, axis=1).T)
        for du_t, k in zip(dus, ks):
            part = dot(w1b[k, :, u0 * 256:u1 * 256], du_t)
            total = part if total is None else total + part
        acc[...] = total if first else acc[...] + total

    def grads_mine(j):
        grads(j, mine, mine_k, j == 0)

    def grads_theirs(j):
        for i in range(2):
            c_df[j, i].wait_recv()
        grads(j, theirs, theirs_k, False)

    dm_part(0)
    dm_part(1)
    dm_sum(0)
    forward_u(1)
    dm_part(2)
    dm_sum(1)
    products_sib(1)
    dm_part(3)
    dm_sum(2)
    dm_part(4)
    dm_sum(3)
    forward_u(2)
    dm_part(5)
    dm_sum(4)
    dm_sum(5)
    dm_full(0)
    grads_mine(0)
    for j in range(1, NC):
        if j == NC - 1:
            dm_full(j)
        grads_theirs(j - 1)
        if j < NC - 1:
            dm_full(j)
        grads_mine(j)
        if j == 3:
            products_sib(2)
    grads_theirs(NC - 1)
    dxp_ref[...] = acc[...].T.astype(BF)
    for cp in live:
        cp.wait_send()


def comm_call(x, w1, b1, w2, b2, gam, dy):
    scratch = [pltpu.VMEM((T, H), BF), pltpu.VMEM((4 * NU, 1, 256), F32), pltpu.VMEM((1, H), F32), pltpu.VMEM((1, H), F32),
               pltpu.VMEM((T, H), BF),
               pltpu.VMEM((4, H, NU * 256), BF), pltpu.VMEM((4 * NU * 128, H), BF),
               pltpu.VMEM((4, NU, T, 256), BF), pltpu.VMEM((2, NU, T, 256), BF),
               pltpu.VMEM((NU, T, 256), BF), pltpu.VMEM((NU, T, 256), BF),
               pltpu.VMEM((2, 2, HT, 512), BF), pltpu.VMEM((2, 2, HT, 512), BF),
               pltpu.VMEM((4, 8, T), F32),
               pltpu.VMEM((4, NU, T, 128), BF), pltpu.VMEM((2, NU, T, 128), BF),
               pltpu.VMEM((4, NU, T, 256), BF), pltpu.VMEM((4, NU, T, 128), BF), pltpu.VMEM((4, NU, T, 256), F32),
               pltpu.VMEM((H, T), F32),
               pltpu.SemaphoreType.DMA((5,)), pltpu.SemaphoreType.DMA((NLS,))]
    for n in SEM_NAMES:
        scratch += [pltpu.SemaphoreType.DMA((N_SEM[n],)), pltpu.SemaphoreType.DMA((N_SEM[n],))]
    outs = [sds((4, NU, T, 128), BF), sds((4, NU, T, 256), BF), sds((T, H), BF), sds((T, H), F32), sds((T, H), F32),
            sds((4 * NU, 1, 256), F32), sds((T, H), BF)]
    return pl.pallas_call(
        comm_kernel, out_shape=outs, name="comm",
        in_specs=[HBM] * 7, out_specs=[VMEM] * 7, scratch_shapes=scratch,
        compiler_params=pltpu.CompilerParams(collective_id=0, has_side_effects=True, vmem_limit_bytes=COMM_LIM),
        cost_estimate=pl.CostEstimate(flops=8 * 10 ** 9, bytes_accessed=32 << 20, transcendentals=0),
    )(x, w1, b1, w2, b2, gam, dy)


NB2 = 6
NB1 = 6


def grads_kernel(m_ref, du_ref, d_ref, nrm_ref, dr_ref, db1_in, x_ref, gam_ref, beta_ref, dy_ref,
                 dw1_ref, dw2_ref, y_ref, db1_ref, db2_ref, dgam_ref, dbeta_ref,
                 ob2, ob1, xt, yb, db1b, sb, so2, so1, so0):
    tiles = [(j, q) for j in range(NC) for q in range(4)]

    def put2(t):
        j, q = tiles[t]
        n = CH[j][1] - CH[j][0]
        r0 = unit(j, q) * 128
        return pltpu.make_async_copy(ob2.at[t % NB2, :n * 128], dw2_ref.at[r0:r0 + n * 128, :], so2.at[t % NB2])

    def put1(t):
        j, q = tiles[t]
        n = CH[j][1] - CH[j][0]
        c0 = unit(j, q) * 256
        return pltpu.make_async_copy(ob1.at[t % NB1, :, :n * 256], dw1_ref.at[:, c0:c0 + n * 256], so1.at[t % NB1])

    small = [pltpu.make_async_copy(a, b, so0.at[i]) for i, (a, b) in enumerate(
        ((yb, y_ref), (db1b, db1_ref), (sb.at[0], db2_ref), (sb.at[1], dgam_ref), (sb.at[2], dbeta_ref)))]
    for t, (j, q) in enumerate(tiles):
        if t >= NB2:
            put2(t - NB2).wait()
        for i, a in enumerate(range(*CH[j])):
            ob2[t % NB2, i * 128:(i + 1) * 128] = dot(m_ref[q, a].T, d_ref[...])
        put2(t).start()
        if t == 6:
            xt[...] = x_ref[...].T
        if t == 8:
            yb[...] = (gam_ref[...] * nrm_ref[...] + beta_ref[...]).astype(BF)
            for i in range(4 * NU):
                db1b[:, i * 256:(i + 1) * 256] = db1_in[i]
            for cp in small[:2]:
                cp.start()
        if t == 10:
            dy = dy_ref[...].astype(F32)
            sb[0] = jnp.sum(dr_ref[...], axis=0, keepdims=True)
            sb[1] = jnp.sum(dy * nrm_ref[...], axis=0, keepdims=True)
            sb[2] = jnp.sum(dy, axis=0, keepdims=True)
            for cp in small[2:]:
                cp.start()
    for t, (j, q) in enumerate(tiles):
        if t >= NB1:
            put1(t - NB1).wait()
        for i, a in enumerate(range(*CH[j])):
            ob1[t % NB1, :, i * 256:(i + 1) * 256] = dot(xt[...], du_ref[q, a])
        put1(t).start()
    last = len(tiles)
    for t in range(last - NB2, last):
        put2(t).wait()
    for cp in small:
        cp.wait()
    for t in range(last - NB1, last):
        put1(t).wait()


def grads_call(m, du, d, nrm, dr, db1, x, gam, beta, dy):
    outs = [sds((H, 4 * NU * 256), F32), sds((4 * NU * 128, H), F32), sds((T, H), BF), sds((1, 4 * NU * 256), F32),
            sds((1, H), F32), sds((1, H), F32), sds((1, H), F32)]
    return pl.pallas_call(
        grads_kernel, out_shape=outs, name="grads",
        in_specs=[VMEM] * 10, out_specs=[HBM] * 7,
        scratch_shapes=[pltpu.VMEM((NB2, 256, H), F32), pltpu.VMEM((NB1, H, 512), F32), pltpu.VMEM((H, T), BF),
                        pltpu.VMEM((T, H), BF), pltpu.VMEM((1, 4 * NU * 256), F32), pltpu.VMEM((3, 1, H), F32),
                        pltpu.SemaphoreType.DMA((NB2,)), pltpu.SemaphoreType.DMA((NB1,)), pltpu.SemaphoreType.DMA((5,))],
        compiler_params=pltpu.CompilerParams(vmem_limit_bytes=GRADS_LIM),
        cost_estimate=pl.CostEstimate(flops=4 * 10 ** 9, bytes_accessed=66 << 20, transcendentals=0),
    )(m, du, d, nrm, dr, db1, x, gam, beta, dy)


def solution(mesh):
    data_spec = P('dp', 'hd')
    hid_spec = P('hd')
    in_specs = (data_spec, P('hd', 'ff'), P('ff'), P('ff', 'hd'), hid_spec, hid_spec, hid_spec, data_spec)
    out_specs = (data_spec, data_spec, P(('dp', 'hd'), 'ff'), P(('dp', 'ff'), 'hd'), P(('dp', 'ff')), P(('dp', 'hd')), P(('dp', 'hd')), P(('dp', 'hd')))

    def device_step(x, w1, b1, w2, b2, gam, beta, dy):
        b2, gam, beta = (a.reshape(1, H) for a in (b2, gam, beta))
        hbm = [pltpu.with_memory_space_constraint(a, pltpu.HBM) for a in (x, w1, b1.reshape(4 * NU, 1, 256), w2, b2, gam, dy)]
        m, du, d, dr, nrm, db1, dxp = comm_call(*hbm)
        dxr = lax.ppermute(dxp, 'ff', [(0, 1), (1, 0)])
        dw1, dw2, y, db1, db2, dgam, dbeta = grads_call(m, du, d, nrm, dr, db1, x, gam, beta, dy)
        dx = (ALPHA * dr + (dxp.astype(F32) + dxr.astype(F32))).astype(BF)
        return y, dx, dw1, dw2, db1.reshape(-1), db2.reshape(-1), dgam.reshape(-1), dbeta.reshape(-1)

    return jax.shard_map(device_step, mesh=mesh, in_specs=in_specs, out_specs=out_specs, check_vma=False)
```

```python
import functools
import math
import jax
import jax.numpy as jnp
from jax import lax
from jax.experimental import pallas as pl
from jax.experimental.pallas import tpu as pltpu
from jax.sharding import PartitionSpec as P

PAIR = 128
ALPHA = math.sqrt(140.0)
LN_EPS = 1e-5
C0 = math.sqrt(2.0 / math.pi)
C1 = 0.044715
MESH = pl.DeviceIdType.MESH
F32 = jnp.float32
BF = jnp.bfloat16
T = 128
H = 1024
NU = 10
CH = ((0, 1), (1, 3), (3, 5), (5, 7), (7, 9), (9, 10))
NC = len(CH)
COMM_LIM = 48 * 1024 * 1024
GRADS_LIM = 28 * 1024 * 1024

VMEM = pl.BlockSpec(memory_space=pltpu.VMEM)
ANY = pl.BlockSpec(memory_space=pl.ANY)
HBM = pl.BlockSpec(memory_space=pltpu.HBM)


def sds(shape, dtype):
    return jax.ShapeDtypeStruct(shape, dtype)


def dot(a, b):
    return jnp.dot(a, b, preferred_element_type=F32)


def gelu_both(g):
    g2 = g * g
    t = jnp.tanh(C0 * (g + C1 * (g2 * g)))
    cdf = 0.5 * (1.0 + t)
    slope = cdf + (0.5 * g) * (1.0 - t * t) * (C0 * (1.0 + (3.0 * C1) * g2))
    return g * cdf, slope


def places():
    h = lax.axis_index("hd")
    y = lax.axis_index("ff")
    c = lax.rem(h, 2)
    sib = h + 1 - 2 * c
    xn = lax.rem(h + 2, 4)
    xs = lax.rem(sib + 2, 4)
    return h, y, c, sib, xn, xs


def remote(src, dst, sems, k, dev):
    return pltpu.make_async_remote_copy(src_ref=src, dst_ref=dst, send_sem=sems[0].at[k], recv_sem=sems[1].at[k],
                                        device_id=dev, device_id_type=MESH)


def unit(j, q):
    u0, u1 = CH[j]
    return 4 * u0 + q * (u1 - u0)


def aligned(start, size, tile):
    return pl.ds(pl.multiple_of(start * tile, tile), size * tile)


GCH = ((0, 3), (3, 7), (7, 10))
HT = T // 2
NG = len(GCH)
NLS = 16
N_SEM = {"ud": 2 * NC, "ux": 2 * NC, "mx": 2 * NG, "md": 4 * NG, "gx": NG, "gd": NG, "gf": NG, "fy": 4, "st": 3}
SEM_NAMES = list(N_SEM)


def comm_kernel(x_hbm, w1_ref, b1_hbm, w2_ref, b2_hbm, gam_hbm, dy_hbm,
                m_ref, du_ref, d_ref, dr_ref, nrm_ref, db1_ref, dxp_ref,
                x_ref, b1_ref, b2_ref, gam_ref, dy_ref, w1b, w2b, ub, rb, xsb, xrb, fs, fr, stb, dmb, dmr, u_ref, dmf, pr_ref, acc,
                ls0, ls1, *sem_list):
    sems = {n: (sem_list[2 * i], sem_list[2 * i + 1]) for i, n in enumerate(SEM_NAMES)}
    h, y, c, sib, xn, xs = places()
    dev_sib, dev_x, dev_xs, dev_y = (0, y, sib), (0, y, xn), (0, y, xs), (0, 1 - y, h)
    order = [xs, xn, sib, h]

    load_order = []
    for j in range(NC + 1):
        load_order += [(j, k) for k in (0, 1) if j < NC] + [(j - 1, k) for k in (2, 3) if j > 0]

    def w1_load(j, k):
        u0, u1 = CH[j]
        n = u1 - u0
        return pltpu.make_async_copy(w1_ref.at[:, aligned(unit(j, order[k]), n, 256)], w1b.at[k, :, u0 * 256:u1 * 256],
                                     ls1.at[load_order.index((j, k)) % NLS])

    def w2_load(j):
        rows = slice(4 * 128 * CH[j][0], 4 * 128 * CH[j][1])
        return pltpu.make_async_copy(w2_ref.at[rows, :], w2b.at[rows, :], ls1.at[(4 * NC + j) % NLS])

    ins = [pltpu.make_async_copy(a, b, ls0.at[i]) for i, (a, b) in enumerate(
        ((x_hbm, x_ref), (b1_hbm, b1_ref), (b2_hbm, b2_ref), (gam_hbm, gam_ref), (dy_hbm, dy_ref)))]
    bar = pltpu.get_barrier_semaphore()
    for dev in (dev_sib, dev_x, dev_xs, dev_y):
        pl.semaphore_signal(bar, inc=1, device_id=dev, device_id_type=MESH)
    ins[0].start()
    for j, k in load_order[:6]:
        w1_load(j, k).start()
    loaded = [6]

    def load_more(n):
        for j, k in load_order[loaded[0]:loaded[0] + n]:
            w1_load(j, k).start()
        loaded[0] += n

    ins[0].wait()

    live = []

    def send(src, dst, name, k, dev):
        cp = remote(src, dst, sems[name], k, dev)
        cp.start()
        live.append(cp)
        return cp

    def sent(*cps):
        for cp in cps:
            cp.wait_send()
        live[:] = [cp for cp in live if not any(cp is old for old in cps)]

    def u_parts(*slabs):
        for j, k in slabs:
            w1_load(j, k).wait()
        load_more(4)
        for j, k in slabs:
            u0, u1 = CH[j]
            r = dot(x_ref[...], w1b[k, :, u0 * 256:u1 * 256]).astype(BF)
            for i in range(u1 - u0):
                ub[k, u0 + i] = r[:, i * 256:(i + 1) * 256]
        if slabs[0] == (0, 0):
            pl.semaphore_wait(bar, 4)
            for cp in ins[1:]:
                cp.start()
        for j, k in slabs:
            us = slice(*CH[j])
            if k == 0:
                c_ud[j, 1] = send(ub.at[0, us], rb.at[1, us], "ud", 2 * j + 1, dev_sib)
            if k == 2:
                c_ud[j, 0] = send(ub.at[2, us], rb.at[0, us], "ud", 2 * j, dev_sib)

    def s1(j):
        us = slice(*CH[j])
        c_ud[j, 1].wait_recv()
        xsb[us] = (ub[1, us].astype(F32) + rb[1, us].astype(F32)).astype(BF)
        send_x(0, j)

    def half(a):
        return slice(a * HT, (a + 1) * HT)

    def send_x(a, j):
        us = slice(*CH[j])
        c_ux[a, j] = send(xsb.at[us, half(a)], xrb.at[us, half(a)], "ux", a * NC + j, dev_x)

    def s2(a, j):
        rows = half(a)
        u0, u1 = CH[j]
        if a == 0:
            c_ud[j, 0].wait_recv()
        c_ux[a, j].wait_recv()
        for i in range(u1 - u0):
            n = u0 + i
            u = (ub[3, n, rows].astype(F32) + rb[0, n, rows].astype(F32) + xrb[n, rows].astype(F32)
                 + b1_ref[unit(j, h) + i])
            u = u.astype(BF)
            u_ref[h, n, rows] = u
            u = u.astype(F32)
            val, slope = gelu_both(u[:, PAIR:])
            m_ref[h, n, rows] = (u[:, :PAIR] * val).astype(BF)
            pr_ref[h, n, rows, :PAIR] = val
            pr_ref[h, n, rows, PAIR:] = u[:, :PAIR] * slope
        if j % 2 == 1:
            g = j // 2
            part = m_ref.at[h, slice(*GCH[g]), rows]
            c_mx[a, g] = send(part, part, "mx", a * NG + g, dev_x)
            c_md[a, g] = send(part, part, "md", a * NG + g, dev_sib)

    def s3(a, g):
        c_mx[a, g].wait_recv()
        part = m_ref.at[xn, slice(*GCH[g]), half(a)]
        c_mf[a, g] = send(part, part, "md", (2 + a) * NG + g, dev_sib)

    def s4(a, g):
        rows = half(a)
        c_md[a, g].wait_recv()
        c_mf[a, g].wait_recv()
        if a == 0:
            for j in (2 * g, 2 * g + 1):
                w2_load(j).wait()
        m = jnp.concatenate([m_ref[q, n, rows] for j in (2 * g, 2 * g + 1) for q in range(4) for n in range(*CH[j])], axis=1)
        u0, u1 = GCH[g]
        for n in range(2):
            cols = slice(n * 512, (n + 1) * 512)
            part = dot(m, w2b[4 * 128 * u0:4 * 128 * u1, cols])
            if g > 0:
                part = nrm_ref[rows, cols] + part
            if g < NG - 1:
                nrm_ref[rows, cols] = part
            else:
                fs[a, n] = part.astype(BF)
                c_fy[a, n] = send(fs.at[a, n], fr.at[a, n], "fy", 2 * a + n, dev_y)

    def gather_u(j):
        us = slice(*GCH[j])
        c_gx[j] = send(u_ref.at[h, us], u_ref.at[h, us], "gx", j, dev_x)
        c_gd[j] = send(u_ref.at[h, us], u_ref.at[h, us], "gd", j, dev_sib)

    def forward_u(j):
        us = slice(*GCH[j])
        c_gx[j].wait_recv()
        c_gf[j] = send(u_ref.at[xn, us], u_ref.at[xn, us], "gf", j, dev_sib)
        products(j, xn)

    def products(j, q):
        for a in range(*GCH[j]):
            u = u_ref[q, a].astype(F32)
            val, slope = gelu_both(u[:, PAIR:])
            pr_ref[q, a, :, :PAIR] = val
            pr_ref[q, a, :, PAIR:] = u[:, :PAIR] * slope

    def products_sib(j):
        c_gd[j].wait_recv()
        c_gf[j].wait_recv()
        products(j, sib)
        products(j, xs)

    c_ud, c_ux, c_mx, c_md, c_mf, c_fy, c_gx, c_gd, c_gf = {}, {}, {}, {}, {}, {}, {}, {}, {}
    u_parts((0, 0), (0, 1))
    u_parts((1, 0), (1, 1), (0, 2), (0, 3))
    s1(0)
    u_parts((2, 0), (2, 1), (1, 2), (1, 3))
    s1(1)
    send_x(1, 0)
    u_parts((3, 0), (3, 1), (2, 2), (2, 3))
    s1(2)
    for j in range(NC):
        w2_load(j).start()
    u_parts((4, 0), (4, 1), (3, 2), (3, 3))
    s1(3)
    send_x(1, 1)
    u_parts((5, 0), (5, 1), (4, 2), (4, 3))
    s1(4)
    u_parts((5, 2), (5, 3))
    s1(5)
    for j in range(2, NC):
        send_x(1, j)
    ins[1].wait()
    for a in range(2):
        for j in range(NC):
            s2(a, j)
    for g in range(NG - 1):
        gather_u(g)
    for a in range(2):
        s3(a, 0)
        s3(a, 1)
        s4(a, 0)
        s3(a, 2)
        s4(a, 1)
        s4(a, 2)
    for cp in ins[2:]:
        cp.wait()

    forward_u(0)
    for a in range(2):
        for n in range(2):
            rows, cols = half(a), slice(n * 512, (n + 1) * 512)
            c_fy[a, n].wait_recv()
            f = fs[a, n].astype(F32) + fr[a, n].astype(F32)
            nrm_ref[rows, cols] = ALPHA * x_ref[rows, cols].astype(F32) + f + b2_ref[:, cols]
    r = nrm_ref[...]
    gdy = dy_ref[...].astype(F32) * gam_ref[...]
    m_loc = jnp.sum(r, axis=1, keepdims=True) * (1.0 / H)
    cen = r - m_loc
    m2 = jnp.sum(cen * cen, axis=1, keepdims=True)
    sg = jnp.sum(gdy, axis=1, keepdims=True)
    cg = jnp.sum(gdy * cen, axis=1, keepdims=True)
    lane = lax.broadcasted_iota(jnp.int32, (T, 128), 1)
    pack = jnp.where(lane == 0, m_loc, jnp.where(lane == 1, m2, jnp.where(lane == 2, sg, cg)))
    stb[h] = pack.T[0:8]
    c_st = [send(stb.at[h], stb.at[h], "st", i, dev) for i, dev in enumerate((dev_sib, dev_x, dev_xs))]
    gather_u(NG - 1)
    products_sib(0)
    for cp in c_st:
        cp.wait_recv()
    st = [stb[i] for i in range(4)]
    mu = ((st[0][0:1] + st[1][0:1]) + (st[2][0:1] + st[3][0:1])) * 0.25
    m2t = jnp.zeros_like(mu)
    sgt = jnp.zeros_like(mu)
    cgt = jnp.zeros_like(mu)
    for i in range(4):
        delta = st[i][0:1] - mu
        m2t += st[i][1:2] + (H * delta) * delta
        sgt += st[i][2:3]
        cgt += st[i][3:4] + delta * st[i][2:3]
    rho = lax.rsqrt(m2t * (1.0 / (4 * H)) + LN_EPS)
    rows = jnp.concatenate([mu, rho, sgt * (1.0 / (4 * H)), cgt * rho * (1.0 / (4 * H)), jnp.zeros((124, T), F32)], axis=0)
    colst = rows.T
    mu_c, rho_c, mg_c, mgr_c = (colst[:, i:i + 1] for i in range(4))
    nrm = (r - mu_c) * rho_c
    dr = rho_c * (gdy - mg_c - nrm * mgr_c)
    nrm_ref[...] = nrm
    dr_ref[...] = dr
    d_ref[...] = dr.astype(BF)
    d_t = dr.T.astype(BF)

    c_dd, c_dx, c_df = {}, {}, {}
    mine, mine_k, theirs, theirs_k = (h, xn), (3, 1), (sib, xs), (2, 0)

    def dm_part(j):
        u0, u1 = CH[j]
        n = u1 - u0
        for i, q in enumerate(theirs + mine):
            r = dot(w2b[aligned(unit(j, q), n, 128), :], d_t).astype(BF).T
            for a in range(n):
                dmb[i, u0 + a] = r[:, a * 128:(a + 1) * 128]
            if i == 1:
                sent(c_ud[j, 0], c_ud[j, 1])
                for k in range(2):
                    c_dd[j, k] = send(dmb.at[k, u0:u1], dmr.at[k, u0:u1], "ud", 2 * j + k, dev_sib)

    def dm_sum(j):
        us = slice(*CH[j])
        sent(c_ux[0, j], c_ux[1, j])
        for i in range(2):
            c_dd[j, i].wait_recv()
            xsb[us, :, i * 128:(i + 1) * 128] = (dmb[2 + i, us].astype(F32) + dmr[i, us].astype(F32)).astype(BF)
        c_dx[j] = send(xsb.at[us], xrb.at[us], "ux", j, dev_x)

    def dm_full(j):
        us = slice(*CH[j])
        c_dx[j].wait_recv()
        if j == 0:
            sent(*c_md.values(), *c_mf.values())
        for i in range(2):
            q = mine[i]
            dmf[q, us] = (xsb[us, :, i * 128:(i + 1) * 128].astype(F32)
                          + xrb[us, :, (1 - i) * 128:(2 - i) * 128].astype(F32)).astype(BF)
        for i in range(2):
            q = mine[i]
            c_df[j, i] = send(dmf.at[q, us], dmf.at[q, us], "md", 2 * j + i, dev_sib)

    def grads(j, qs, ks, first):
        u0, u1 = CH[j]
        total = None
        dus = []
        for q in qs:
            parts = []
            for a in range(u0, u1):
                dm = dmf[q, a].astype(F32)
                du_f = pr_ref[q, a] * jnp.concatenate([dm, dm], axis=1)
                db1_ref[unit(j, q) + a - u0] = jnp.sum(du_f, axis=0, keepdims=True)
                du = du_f.astype(BF)
                du_ref[q, a] = du
                parts.append(du)
            dus.append(jnp.concatenate(parts, axis=1).T)
        for du_t, k in zip(dus, ks):
            part = dot(w1b[k, :, u0 * 256:u1 * 256], du_t)
            total = part if total is None else total + part
        acc[...] = total if first else acc[...] + total

    def grads_mine(j):
        grads(j, mine, mine_k, j == 0)

    def grads_theirs(j):
        for i in range(2):
            c_df[j, i].wait_recv()
        grads(j, theirs, theirs_k, False)

    dm_part(0)
    dm_part(1)
    dm_sum(0)
    forward_u(1)
    dm_part(2)
    dm_sum(1)
    products_sib(1)
    dm_part(3)
    dm_sum(2)
    dm_part(4)
    dm_sum(3)
    forward_u(2)
    dm_part(5)
    dm_sum(4)
    dm_sum(5)
    dm_full(0)
    grads_mine(0)
    for j in range(1, NC):
        if j == NC - 1:
            dm_full(j)
        grads_theirs(j - 1)
        if j < NC - 1:
            dm_full(j)
        grads_mine(j)
        if j == 3:
            products_sib(2)
    grads_theirs(NC - 1)
    dxp_ref[...] = acc[...].T.astype(BF)
    for cp in live:
        cp.wait_send()


def comm_call(x, w1, b1, w2, b2, gam, dy):
    scratch = [pltpu.VMEM((T, H), BF), pltpu.VMEM((4 * NU, 1, 256), F32), pltpu.VMEM((1, H), F32), pltpu.VMEM((1, H), F32),
               pltpu.VMEM((T, H), BF),
               pltpu.VMEM((4, H, NU * 256), BF), pltpu.VMEM((4 * NU * 128, H), BF),
               pltpu.VMEM((4, NU, T, 256), BF), pltpu.VMEM((2, NU, T, 256), BF),
               pltpu.VMEM((NU, T, 256), BF), pltpu.VMEM((NU, T, 256), BF),
               pltpu.VMEM((2, 2, HT, 512), BF), pltpu.VMEM((2, 2, HT, 512), BF),
               pltpu.VMEM((4, 8, T), F32),
               pltpu.VMEM((4, NU, T, 128), BF), pltpu.VMEM((2, NU, T, 128), BF),
               pltpu.VMEM((4, NU, T, 256), BF), pltpu.VMEM((4, NU, T, 128), BF), pltpu.VMEM((4, NU, T, 256), F32),
               pltpu.VMEM((H, T), F32),
               pltpu.SemaphoreType.DMA((5,)), pltpu.SemaphoreType.DMA((NLS,))]
    for n in SEM_NAMES:
        scratch += [pltpu.SemaphoreType.DMA((N_SEM[n],)), pltpu.SemaphoreType.DMA((N_SEM[n],))]
    outs = [sds((4, NU, T, 128), BF), sds((4, NU, T, 256), BF), sds((T, H), BF), sds((T, H), F32), sds((T, H), F32),
            sds((4 * NU, 1, 256), F32), sds((T, H), BF)]
    return pl.pallas_call(
        comm_kernel, out_shape=outs, name="comm",
        in_specs=[HBM] * 7, out_specs=[VMEM] * 7, scratch_shapes=scratch,
        compiler_params=pltpu.CompilerParams(collective_id=0, has_side_effects=True, vmem_limit_bytes=COMM_LIM),
        cost_estimate=pl.CostEstimate(flops=8 * 10 ** 9, bytes_accessed=32 << 20, transcendentals=0),
    )(x, w1, b1, w2, b2, gam, dy)


NB2 = 6
NB1 = 6


def grads_kernel(m_ref, du_ref, d_ref, nrm_ref, dr_ref, db1_in, x_ref, gam_ref, beta_ref, dy_ref,
                 dw1_ref, dw2_ref, y_ref, db1_ref, db2_ref, dgam_ref, dbeta_ref,
                 ob2, ob1, xt, yb, db1b, sb, so2, so1, so0):
    tiles = [(j, q) for j in range(NC) for q in range(4)]

    def put2(t):
        j, q = tiles[t]
        n = CH[j][1] - CH[j][0]
        r0 = unit(j, q) * 128
        return pltpu.make_async_copy(ob2.at[t % NB2, :n * 128], dw2_ref.at[r0:r0 + n * 128, :], so2.at[t % NB2])

    def put1(t):
        j, q = tiles[t]
        n = CH[j][1] - CH[j][0]
        c0 = unit(j, q) * 256
        return pltpu.make_async_copy(ob1.at[t % NB1, :, :n * 256], dw1_ref.at[:, c0:c0 + n * 256], so1.at[t % NB1])

    small = [pltpu.make_async_copy(a, b, so0.at[i]) for i, (a, b) in enumerate(
        ((yb, y_ref), (db1b, db1_ref), (sb.at[0], db2_ref), (sb.at[1], dgam_ref), (sb.at[2], dbeta_ref)))]
    for t, (j, q) in enumerate(tiles):
        if t >= NB2:
            put2(t - NB2).wait()
        for i, a in enumerate(range(*CH[j])):
            ob2[t % NB2, i * 128:(i + 1) * 128] = dot(m_ref[q, a].T, d_ref[...])
        put2(t).start()
        if t == 6:
            xt[...] = x_ref[...].T
        if t == 8:
            yb[...] = (gam_ref[...] * nrm_ref[...] + beta_ref[...]).astype(BF)
            for i in range(4 * NU):
                db1b[:, i * 256:(i + 1) * 256] = db1_in[i]
            for cp in small[:2]:
                cp.start()
        if t == 10:
            dy = dy_ref[...].astype(F32)
            sb[0] = jnp.sum(dr_ref[...], axis=0, keepdims=True)
            sb[1] = jnp.sum(dy * nrm_ref[...], axis=0, keepdims=True)
            sb[2] = jnp.sum(dy, axis=0, keepdims=True)
            for cp in small[2:]:
                cp.start()
    for t, (j, q) in enumerate(tiles):
        if t >= NB1:
            put1(t - NB1).wait()
        for i, a in enumerate(range(*CH[j])):
            ob1[t % NB1, :, i * 256:(i + 1) * 256] = dot(xt[...], du_ref[q, a])
        put1(t).start()
    last = len(tiles)
    for t in range(last - NB2, last):
        put2(t).wait()
    for cp in small:
        cp.wait()
    for t in range(last - NB1, last):
        put1(t).wait()


def grads_call(m, du, d, nrm, dr, db1, x, gam, beta, dy):
    outs = [sds((H, 4 * NU * 256), F32), sds((4 * NU * 128, H), F32), sds((T, H), BF), sds((1, 4 * NU * 256), F32),
            sds((1, H), F32), sds((1, H), F32), sds((1, H), F32)]
    return pl.pallas_call(
        grads_kernel, out_shape=outs, name="grads",
        in_specs=[VMEM] * 10, out_specs=[HBM] * 7,
        scratch_shapes=[pltpu.VMEM((NB2, 256, H), F32), pltpu.VMEM((NB1, H, 512), F32), pltpu.VMEM((H, T), BF),
                        pltpu.VMEM((T, H), BF), pltpu.VMEM((1, 4 * NU * 256), F32), pltpu.VMEM((3, 1, H), F32),
                        pltpu.SemaphoreType.DMA((NB2,)), pltpu.SemaphoreType.DMA((NB1,)), pltpu.SemaphoreType.DMA((5,))],
        compiler_params=pltpu.CompilerParams(vmem_limit_bytes=GRADS_LIM),
        cost_estimate=pl.CostEstimate(flops=4 * 10 ** 9, bytes_accessed=66 << 20, transcendentals=0),
    )(m, du, d, nrm, dr, db1, x, gam, beta, dy)


def solution(mesh):
    data_spec = P('dp', 'hd')
    hid_spec = P('hd')
    in_specs = (data_spec, P('hd', 'ff'), P('ff'), P('ff', 'hd'), hid_spec, hid_spec, hid_spec, data_spec)
    out_specs = (data_spec, data_spec, P(('dp', 'hd'), 'ff'), P(('dp', 'ff'), 'hd'), P(('dp', 'ff')), P(('dp', 'hd')), P(('dp', 'hd')), P(('dp', 'hd')))

    def device_step(x, w1, b1, w2, b2, gam, beta, dy):
        b2, gam, beta = (a.reshape(1, H) for a in (b2, gam, beta))
        hbm = [pltpu.with_memory_space_constraint(a, pltpu.HBM) for a in (x, w1, b1.reshape(4 * NU, 1, 256), w2, b2, gam, dy)]
        m, du, d, dr, nrm, db1, dxp = comm_call(*hbm)
        dxr = lax.ppermute(dxp, 'ff', [(0, 1), (1, 0)])
        dw1, dw2, y, db1, db2, dgam, dbeta = grads_call(m, du, d, nrm, dr, db1, x, gam, beta, dy)
        dx = (ALPHA * dr + (dxp.astype(F32) + dxr.astype(F32))).astype(BF)
        return y, dx, dw1, dw2, db1.reshape(-1), db2.reshape(-1), dgam.reshape(-1), dbeta.reshape(-1)

    return jax.shard_map(device_step, mesh=mesh, in_specs=in_specs, out_specs=out_specs, check_vma=False)
```

```python
import functools
import math
import jax
import jax.numpy as jnp
from jax import lax
from jax.experimental import pallas as pl
from jax.experimental.pallas import tpu as pltpu
from jax.sharding import PartitionSpec as P

PAIR = 128
ALPHA = math.sqrt(140.0)
LN_EPS = 1e-5
C0 = math.sqrt(2.0 / math.pi)
C1 = 0.044715
MESH = pl.DeviceIdType.MESH
F32 = jnp.float32
BF = jnp.bfloat16
T = 128
H = 1024
NU = 10
CH = ((0, 1), (1, 3), (3, 5), (5, 7), (7, 9), (9, 10))
NC = len(CH)
COMM_LIM = 48 * 1024 * 1024
GRADS_LIM = 28 * 1024 * 1024

VMEM = pl.BlockSpec(memory_space=pltpu.VMEM)
ANY = pl.BlockSpec(memory_space=pl.ANY)
HBM = pl.BlockSpec(memory_space=pltpu.HBM)


def sds(shape, dtype):
    return jax.ShapeDtypeStruct(shape, dtype)


def dot(a, b):
    return jnp.dot(a, b, preferred_element_type=F32)


def gelu_both(g):
    g2 = g * g
    t = jnp.tanh(C0 * (g + C1 * (g2 * g)))
    cdf = 0.5 * (1.0 + t)
    slope = cdf + (0.5 * g) * (1.0 - t * t) * (C0 * (1.0 + (3.0 * C1) * g2))
    return g * cdf, slope


def places():
    h = lax.axis_index("hd")
    y = lax.axis_index("ff")
    c = lax.rem(h, 2)
    sib = h + 1 - 2 * c
    xn = lax.rem(h + 2, 4)
    xs = lax.rem(sib + 2, 4)
    return h, y, c, sib, xn, xs


def remote(src, dst, sems, k, dev):
    return pltpu.make_async_remote_copy(src_ref=src, dst_ref=dst, send_sem=sems[0].at[k], recv_sem=sems[1].at[k],
                                        device_id=dev, device_id_type=MESH)


def unit(j, q):
    u0, u1 = CH[j]
    return 4 * u0 + q * (u1 - u0)


def aligned(start, size, tile):
    return pl.ds(pl.multiple_of(start * tile, tile), size * tile)


GCH = ((0, 3), (3, 7), (7, 10))
HT = T // 2
NG = len(GCH)
NLS = 16
N_SEM = {"ud": 2 * NC, "ux": 2 * NC, "mx": 2 * NG, "md": 4 * NG, "gx": NG, "gd": NG, "gf": NG, "fy": 4, "st": 3}
SEM_NAMES = list(N_SEM)


def comm_kernel(x_hbm, w1_ref, b1_hbm, w2_ref, b2_hbm, gam_hbm, dy_hbm,
                m_ref, du_ref, d_ref, dr_ref, nrm_ref, db1_ref, dxp_ref,
                x_ref, b1_ref, b2_ref, gam_ref, dy_ref, w1b, w2b, ub, rb, xsb, xrb, fs, fr, stb, dmb, dmr, u_ref, dmf, pr_ref, acc,
                ls0, ls1, *sem_list):
    sems = {n: (sem_list[2 * i], sem_list[2 * i + 1]) for i, n in enumerate(SEM_NAMES)}
    h, y, c, sib, xn, xs = places()
    dev_sib, dev_x, dev_xs, dev_y = (0, y, sib), (0, y, xn), (0, y, xs), (0, 1 - y, h)
    order = [xs, xn, sib, h]

    load_order = []
    for j in range(NC + 1):
        load_order += [(j, k) for k in (0, 1) if j < NC] + [(j - 1, k) for k in (2, 3) if j > 0]

    def w1_load(j, k):
        u0, u1 = CH[j]
        n = u1 - u0
        return pltpu.make_async_copy(w1_ref.at[:, aligned(unit(j, order[k]), n, 256)], w1b.at[k, :, u0 * 256:u1 * 256],
                                     ls1.at[load_order.index((j, k)) % NLS])

    def w2_load(j):
        rows = slice(4 * 128 * CH[j][0], 4 * 128 * CH[j][1])
        return pltpu.make_async_copy(w2_ref.at[rows, :], w2b.at[rows, :], ls1.at[(4 * NC + j) % NLS])

    ins = [pltpu.make_async_copy(a, b, ls0.at[i]) for i, (a, b) in enumerate(
        ((x_hbm, x_ref), (b1_hbm, b1_ref), (b2_hbm, b2_ref), (gam_hbm, gam_ref), (dy_hbm, dy_ref)))]
    bar = pltpu.get_barrier_semaphore()
    for dev in (dev_sib, dev_x, dev_xs, dev_y):
        pl.semaphore_signal(bar, inc=1, device_id=dev, device_id_type=MESH)
    ins[0].start()
    for j, k in load_order[:6]:
        w1_load(j, k).start()
    loaded = [6]

    def load_more(n):
        for j, k in load_order[loaded[0]:loaded[0] + n]:
            w1_load(j, k).start()
        loaded[0] += n

    ins[0].wait()

    live = []

    def send(src, dst, name, k, dev):
        cp = remote(src, dst, sems[name], k, dev)
        cp.start()
        live.append(cp)
        return cp

    def sent(*cps):
        for cp in cps:
            cp.wait_send()
        live[:] = [cp for cp in live if not any(cp is old for old in cps)]

    def u_parts(*slabs):
        for j, k in slabs:
            w1_load(j, k).wait()
        load_more(4)
        for j, k in slabs:
            u0, u1 = CH[j]
            r = dot(x_ref[...], w1b[k, :, u0 * 256:u1 * 256]).astype(BF)
            for i in range(u1 - u0):
                ub[k, u0 + i] = r[:, i * 256:(i + 1) * 256]
        if slabs[0] == (0, 0):
            pl.semaphore_wait(bar, 4)
            for cp in ins[1:]:
                cp.start()
        for j, k in slabs:
            us = slice(*CH[j])
            if k == 0:
                c_ud[j, 1] = send(ub.at[0, us], rb.at[1, us], "ud", 2 * j + 1, dev_sib)
            if k == 2:
                c_ud[j, 0] = send(ub.at[2, us], rb.at[0, us], "ud", 2 * j, dev_sib)

    def s1(j):
        us = slice(*CH[j])
        c_ud[j, 1].wait_recv()
        xsb[us] = (ub[1, us].astype(F32) + rb[1, us].astype(F32)).astype(BF)
        send_x(0, j)

    def half(a):
        return slice(a * HT, (a + 1) * HT)

    def send_x(a, j):
        us = slice(*CH[j])
        c_ux[a, j] = send(xsb.at[us, half(a)], xrb.at[us, half(a)], "ux", a * NC + j, dev_x)

    def s2(a, j):
        rows = half(a)
        u0, u1 = CH[j]
        if a == 0:
            c_ud[j, 0].wait_recv()
        c_ux[a, j].wait_recv()
        for i in range(u1 - u0):
            n = u0 + i
            u = (ub[3, n, rows].astype(F32) + rb[0, n, rows].astype(F32) + xrb[n, rows].astype(F32)
                 + b1_ref[unit(j, h) + i])
            u = u.astype(BF)
            u_ref[h, n, rows] = u
            u = u.astype(F32)
            val, slope = gelu_both(u[:, PAIR:])
            m_ref[h, n, rows] = (u[:, :PAIR] * val).astype(BF)
            pr_ref[h, n, rows, :PAIR] = val
            pr_ref[h, n, rows, PAIR:] = u[:, :PAIR] * slope
        if j % 2 == 1:
            g = j // 2
            part = m_ref.at[h, slice(*GCH[g]), rows]
            c_mx[a, g] = send(part, part, "mx", a * NG + g, dev_x)
            c_md[a, g] = send(part, part, "md", a * NG + g, dev_sib)

    def s3(a, g):
        c_mx[a, g].wait_recv()
        part = m_ref.at[xn, slice(*GCH[g]), half(a)]
        c_mf[a, g] = send(part, part, "md", (2 + a) * NG + g, dev_sib)

    def s4(a, g):
        rows = half(a)
        c_md[a, g].wait_recv()
        c_mf[a, g].wait_recv()
        if a == 0:
            for j in (2 * g, 2 * g + 1):
                w2_load(j).wait()
        m = jnp.concatenate([m_ref[q, n, rows] for j in (2 * g, 2 * g + 1) for q in range(4) for n in range(*CH[j])], axis=1)
        u0, u1 = GCH[g]
        for n in range(2):
            cols = slice(n * 512, (n + 1) * 512)
            part = dot(m, w2b[4 * 128 * u0:4 * 128 * u1, cols])
            if g > 0:
                part = nrm_ref[rows, cols] + part
            if g < NG - 1:
                nrm_ref[rows, cols] = part
            else:
                fs[a, n] = part.astype(BF)
                c_fy[a, n] = send(fs.at[a, n], fr.at[a, n], "fy", 2 * a + n, dev_y)

    def gather_u(j):
        us = slice(*GCH[j])
        c_gx[j] = send(u_ref.at[h, us], u_ref.at[h, us], "gx", j, dev_x)
        c_gd[j] = send(u_ref.at[h, us], u_ref.at[h, us], "gd", j, dev_sib)

    def forward_u(j):
        us = slice(*GCH[j])
        c_gx[j].wait_recv()
        c_gf[j] = send(u_ref.at[xn, us], u_ref.at[xn, us], "gf", j, dev_sib)
        products(j, xn)

    def products(j, q):
        for a in range(*GCH[j]):
            u = u_ref[q, a].astype(F32)
            val, slope = gelu_both(u[:, PAIR:])
            pr_ref[q, a, :, :PAIR] = val
            pr_ref[q, a, :, PAIR:] = u[:, :PAIR] * slope

    def products_sib(j):
        c_gd[j].wait_recv()
        c_gf[j].wait_recv()
        products(j, sib)
        products(j, xs)

    c_ud, c_ux, c_mx, c_md, c_mf, c_fy, c_gx, c_gd, c_gf = {}, {}, {}, {}, {}, {}, {}, {}, {}
    u_parts((0, 0), (0, 1))
    u_parts((1, 0), (1, 1), (0, 2), (0, 3))
    s1(0)
    u_parts((2, 0), (2, 1), (1, 2), (1, 3))
    s1(1)
    send_x(1, 0)
    u_parts((3, 0), (3, 1), (2, 2), (2, 3))
    s1(2)
    for j in range(NC):
        w2_load(j).start()
    u_parts((4, 0), (4, 1), (3, 2), (3, 3))
    s1(3)
    send_x(1, 1)
    u_parts((5, 0), (5, 1), (4, 2), (4, 3))
    s1(4)
    u_parts((5, 2), (5, 3))
    s1(5)
    for j in range(2, NC):
        send_x(1, j)
    ins[1].wait()
    for a in range(2):
        for j in range(NC):
            s2(a, j)
    for g in range(NG - 1):
        gather_u(g)
    for a in range(2):
        s3(a, 0)
        s3(a, 1)
        s4(a, 0)
        s3(a, 2)
        s4(a, 1)
        s4(a, 2)
    for cp in ins[2:]:
        cp.wait()

    gdy = dy_ref[...].astype(F32) * gam_ref[...]
    sg = jnp.sum(gdy, axis=1, keepdims=True)
    dr_ref[...] = gdy
    for n in range(2):
        cols = slice(n * 512, (n + 1) * 512)
        nrm_ref[:, cols] = ALPHA * x_ref[:, cols].astype(F32) + b2_ref[:, cols]
    forward_u(0)
    lane = lax.broadcasted_iota(jnp.int32, (HT, 128), 1)
    packs = []
    for a in range(2):
        rows = half(a)
        for n in range(2):
            cols = slice(n * 512, (n + 1) * 512)
            c_fy[a, n].wait_recv()
            nrm_ref[rows, cols] = nrm_ref[rows, cols] + (fs[a, n].astype(F32) + fr[a, n].astype(F32))
        r = nrm_ref[rows, :]
        m_loc = jnp.sum(r, axis=1, keepdims=True) * (1.0 / H)
        cen = r - m_loc
        m2 = jnp.sum(cen * cen, axis=1, keepdims=True)
        cg = jnp.sum(dr_ref[rows, :] * cen, axis=1, keepdims=True)
        packs.append(jnp.where(lane == 0, m_loc, jnp.where(lane == 1, m2, jnp.where(lane == 2, sg[rows], cg))))
    pack = jnp.concatenate(packs, axis=0)
    stb[h] = pack.T[0:8]
    c_st = [send(stb.at[h], stb.at[h], "st", i, dev) for i, dev in enumerate((dev_sib, dev_x, dev_xs))]
    gather_u(NG - 1)
    products_sib(0)
    for cp in c_st:
        cp.wait_recv()
    st = [stb[i] for i in range(4)]
    mu = ((st[0][0:1] + st[1][0:1]) + (st[2][0:1] + st[3][0:1])) * 0.25
    m2t = jnp.zeros_like(mu)
    sgt = jnp.zeros_like(mu)
    cgt = jnp.zeros_like(mu)
    for i in range(4):
        delta = st[i][0:1] - mu
        m2t += st[i][1:2] + (H * delta) * delta
        sgt += st[i][2:3]
        cgt += st[i][3:4] + delta * st[i][2:3]
    rho = lax.rsqrt(m2t * (1.0 / (4 * H)) + LN_EPS)
    rows = jnp.concatenate([mu, rho, sgt * (1.0 / (4 * H)), cgt * rho * (1.0 / (4 * H)), jnp.zeros((124, T), F32)], axis=0)
    colst = rows.T
    mu_c, rho_c, mg_c, mgr_c = (colst[:, i:i + 1] for i in range(4))
    r = nrm_ref[...]
    gdy = dr_ref[...]
    nrm = (r - mu_c) * rho_c
    dr = rho_c * (gdy - mg_c - nrm * mgr_c)
    nrm_ref[...] = nrm
    dr_ref[...] = dr
    d_ref[...] = dr.astype(BF)
    d_t = dr.T.astype(BF)

    c_dd, c_dx, c_df = {}, {}, {}
    mine, mine_k, theirs, theirs_k = (h, xn), (3, 1), (sib, xs), (2, 0)

    def dm_part(j):
        u0, u1 = CH[j]
        n = u1 - u0
        for i, q in enumerate(theirs + mine):
            r = dot(w2b[aligned(unit(j, q), n, 128), :], d_t).astype(BF).T
            for a in range(n):
                dmb[i, u0 + a] = r[:, a * 128:(a + 1) * 128]
            if i == 1:
                sent(c_ud[j, 0], c_ud[j, 1])
                for k in range(2):
                    c_dd[j, k] = send(dmb.at[k, u0:u1], dmr.at[k, u0:u1], "ud", 2 * j + k, dev_sib)

    def dm_sum(j):
        us = slice(*CH[j])
        sent(c_ux[0, j], c_ux[1, j])
        for i in range(2):
            c_dd[j, i].wait_recv()
            xsb[us, :, i * 128:(i + 1) * 128] = (dmb[2 + i, us].astype(F32) + dmr[i, us].astype(F32)).astype(BF)
        c_dx[j] = send(xsb.at[us], xrb.at[us], "ux", j, dev_x)

    def dm_full(j):
        us = slice(*CH[j])
        c_dx[j].wait_recv()
        if j == 0:
            sent(*c_md.values(), *c_mf.values())
        for i in range(2):
            q = mine[i]
            dmf[q, us] = (xsb[us, :, i * 128:(i + 1) * 128].astype(F32)
                          + xrb[us, :, (1 - i) * 128:(2 - i) * 128].astype(F32)).astype(BF)
        for i in range(2):
            q = mine[i]
            c_df[j, i] = send(dmf.at[q, us], dmf.at[q, us], "md", 2 * j + i, dev_sib)

    def grads(j, qs, ks, first):
        u0, u1 = CH[j]
        total = None
        dus = []
        for q in qs:
            parts = []
            for a in range(u0, u1):
                dm = dmf[q, a].astype(F32)
                du_f = pr_ref[q, a] * jnp.concatenate([dm, dm], axis=1)
                db1_ref[unit(j, q) + a - u0] = jnp.sum(du_f, axis=0, keepdims=True)
                du = du_f.astype(BF)
                du_ref[q, a] = du
                parts.append(du)
            dus.append(jnp.concatenate(parts, axis=1).T)
        for du_t, k in zip(dus, ks):
            part = dot(w1b[k, :, u0 * 256:u1 * 256], du_t)
            total = part if total is None else total + part
        acc[...] = total if first else acc[...] + total

    def grads_mine(j):
        grads(j, mine, mine_k, j == 0)

    def grads_theirs(j):
        for i in range(2):
            c_df[j, i].wait_recv()
        grads(j, theirs, theirs_k, False)

    dm_part(0)
    dm_part(1)
    dm_sum(0)
    forward_u(1)
    dm_part(2)
    dm_sum(1)
    products_sib(1)
    dm_part(3)
    dm_sum(2)
    dm_part(4)
    dm_sum(3)
    forward_u(2)
    dm_part(5)
    dm_sum(4)
    dm_sum(5)
    dm_full(0)
    grads_mine(0)
    for j in range(1, NC):
        if j == NC - 1:
            dm_full(j)
        grads_theirs(j - 1)
        if j < NC - 1:
            dm_full(j)
        grads_mine(j)
        if j == 3:
            products_sib(2)
    grads_theirs(NC - 1)
    dxp_ref[...] = acc[...].T.astype(BF)
    for cp in live:
        cp.wait_send()


def comm_call(x, w1, b1, w2, b2, gam, dy):
    scratch = [pltpu.VMEM((T, H), BF), pltpu.VMEM((4 * NU, 1, 256), F32), pltpu.VMEM((1, H), F32), pltpu.VMEM((1, H), F32),
               pltpu.VMEM((T, H), BF),
               pltpu.VMEM((4, H, NU * 256), BF), pltpu.VMEM((4 * NU * 128, H), BF),
               pltpu.VMEM((4, NU, T, 256), BF), pltpu.VMEM((2, NU, T, 256), BF),
               pltpu.VMEM((NU, T, 256), BF), pltpu.VMEM((NU, T, 256), BF),
               pltpu.VMEM((2, 2, HT, 512), BF), pltpu.VMEM((2, 2, HT, 512), BF),
               pltpu.VMEM((4, 8, T), F32),
               pltpu.VMEM((4, NU, T, 128), BF), pltpu.VMEM((2, NU, T, 128), BF),
               pltpu.VMEM((4, NU, T, 256), BF), pltpu.VMEM((4, NU, T, 128), BF), pltpu.VMEM((4, NU, T, 256), F32),
               pltpu.VMEM((H, T), F32),
               pltpu.SemaphoreType.DMA((5,)), pltpu.SemaphoreType.DMA((NLS,))]
    for n in SEM_NAMES:
        scratch += [pltpu.SemaphoreType.DMA((N_SEM[n],)), pltpu.SemaphoreType.DMA((N_SEM[n],))]
    outs = [sds((4, NU, T, 128), BF), sds((4, NU, T, 256), BF), sds((T, H), BF), sds((T, H), F32), sds((T, H), F32),
            sds((4 * NU, 1, 256), F32), sds((T, H), BF)]
    return pl.pallas_call(
        comm_kernel, out_shape=outs, name="comm",
        in_specs=[HBM] * 7, out_specs=[VMEM] * 7, scratch_shapes=scratch,
        compiler_params=pltpu.CompilerParams(collective_id=0, has_side_effects=True, vmem_limit_bytes=COMM_LIM),
        cost_estimate=pl.CostEstimate(flops=8 * 10 ** 9, bytes_accessed=32 << 20, transcendentals=0),
    )(x, w1, b1, w2, b2, gam, dy)


NB2 = 8
NB1 = 8


def grads_kernel(m_ref, du_ref, d_ref, nrm_ref, dr_ref, db1_in, x_ref, gam_ref, beta_ref, dy_ref,
                 dw1_ref, dw2_ref, y_ref, db1_ref, db2_ref, dgam_ref, dbeta_ref,
                 ob2, ob1, xt, yb, db1b, sb, so2, so1, so0):
    tiles = [(j, q) for j in range(NC) for q in range(4)]

    def put2(t):
        j, q = tiles[t]
        n = CH[j][1] - CH[j][0]
        r0 = unit(j, q) * 128
        return pltpu.make_async_copy(ob2.at[t % NB2, :n * 128], dw2_ref.at[r0:r0 + n * 128, :], so2.at[t % NB2])

    def put1(t):
        j, q = tiles[t]
        n = CH[j][1] - CH[j][0]
        c0 = unit(j, q) * 256
        return pltpu.make_async_copy(ob1.at[t % NB1, :, :n * 256], dw1_ref.at[:, c0:c0 + n * 256], so1.at[t % NB1])

    small = [pltpu.make_async_copy(a, b, so0.at[i]) for i, (a, b) in enumerate(
        ((yb, y_ref), (db1b, db1_ref), (sb.at[0], db2_ref), (sb.at[1], dgam_ref), (sb.at[2], dbeta_ref)))]
    for t, (j, q) in enumerate(tiles):
        if t >= NB2:
            put2(t - NB2).wait()
        for i, a in enumerate(range(*CH[j])):
            ob2[t % NB2, i * 128:(i + 1) * 128] = dot(m_ref[q, a].T, d_ref[...])
        put2(t).start()
        if t == 6:
            xt[...] = x_ref[...].T
        if t == 8:
            yb[...] = (gam_ref[...] * nrm_ref[...] + beta_ref[...]).astype(BF)
            for i in range(4 * NU):
                db1b[:, i * 256:(i + 1) * 256] = db1_in[i]
            for cp in small[:2]:
                cp.start()
        if t == 10:
            dy = dy_ref[...].astype(F32)
            sb[0] = jnp.sum(dr_ref[...], axis=0, keepdims=True)
            sb[1] = jnp.sum(dy * nrm_ref[...], axis=0, keepdims=True)
            sb[2] = jnp.sum(dy, axis=0, keepdims=True)
            for cp in small[2:]:
                cp.start()
    for t, (j, q) in enumerate(tiles):
        if t >= NB1:
            put1(t - NB1).wait()
        for i, a in enumerate(range(*CH[j])):
            ob1[t % NB1, :, i * 256:(i + 1) * 256] = dot(xt[...], du_ref[q, a])
        put1(t).start()
    last = len(tiles)
    for t in range(last - NB2, last):
        put2(t).wait()
    for cp in small:
        cp.wait()
    for t in range(last - NB1, last):
        put1(t).wait()


def grads_call(m, du, d, nrm, dr, db1, x, gam, beta, dy):
    outs = [sds((H, 4 * NU * 256), F32), sds((4 * NU * 128, H), F32), sds((T, H), BF), sds((1, 4 * NU * 256), F32),
            sds((1, H), F32), sds((1, H), F32), sds((1, H), F32)]
    return pl.pallas_call(
        grads_kernel, out_shape=outs, name="grads",
        in_specs=[VMEM] * 10, out_specs=[HBM] * 7,
        scratch_shapes=[pltpu.VMEM((NB2, 256, H), F32), pltpu.VMEM((NB1, H, 512), F32), pltpu.VMEM((H, T), BF),
                        pltpu.VMEM((T, H), BF), pltpu.VMEM((1, 4 * NU * 256), F32), pltpu.VMEM((3, 1, H), F32),
                        pltpu.SemaphoreType.DMA((NB2,)), pltpu.SemaphoreType.DMA((NB1,)), pltpu.SemaphoreType.DMA((5,))],
        compiler_params=pltpu.CompilerParams(vmem_limit_bytes=GRADS_LIM),
        cost_estimate=pl.CostEstimate(flops=4 * 10 ** 9, bytes_accessed=66 << 20, transcendentals=0),
    )(m, du, d, nrm, dr, db1, x, gam, beta, dy)


def solution(mesh):
    data_spec = P('dp', 'hd')
    hid_spec = P('hd')
    in_specs = (data_spec, P('hd', 'ff'), P('ff'), P('ff', 'hd'), hid_spec, hid_spec, hid_spec, data_spec)
    out_specs = (data_spec, data_spec, P(('dp', 'hd'), 'ff'), P(('dp', 'ff'), 'hd'), P(('dp', 'ff')), P(('dp', 'hd')), P(('dp', 'hd')), P(('dp', 'hd')))

    def device_step(x, w1, b1, w2, b2, gam, beta, dy):
        b2, gam, beta = (a.reshape(1, H) for a in (b2, gam, beta))
        hbm = [pltpu.with_memory_space_constraint(a, pltpu.HBM) for a in (x, w1, b1.reshape(4 * NU, 1, 256), w2, b2, gam, dy)]
        m, du, d, dr, nrm, db1, dxp = comm_call(*hbm)
        dxr = lax.ppermute(dxp, 'ff', [(0, 1), (1, 0)])
        dw1, dw2, y, db1, db2, dgam, dbeta = grads_call(m, du, d, nrm, dr, db1, x, gam, beta, dy)
        dx = (ALPHA * dr + (dxp.astype(F32) + dxr.astype(F32))).astype(BF)
        return y, dx, dw1, dw2, db1.reshape(-1), db2.reshape(-1), dgam.reshape(-1), dbeta.reshape(-1)

    return jax.shard_map(device_step, mesh=mesh, in_specs=in_specs, out_specs=out_specs, check_vma=False)
```

```python
import functools
import math
import jax
import jax.numpy as jnp
from jax import lax
from jax.experimental import pallas as pl
from jax.experimental.pallas import tpu as pltpu
from jax.sharding import PartitionSpec as P

PAIR = 128
ALPHA = math.sqrt(140.0)
LN_EPS = 1e-5
C0 = math.sqrt(2.0 / math.pi)
C1 = 0.044715
MESH = pl.DeviceIdType.MESH
F32 = jnp.float32
BF = jnp.bfloat16
T = 128
H = 1024
NU = 10
CH = ((0, 1), (1, 3), (3, 5), (5, 7), (7, 9), (9, 10))
NC = len(CH)
COMM_LIM = 48 * 1024 * 1024
GRADS_LIM = 28 * 1024 * 1024

VMEM = pl.BlockSpec(memory_space=pltpu.VMEM)
ANY = pl.BlockSpec(memory_space=pl.ANY)
HBM = pl.BlockSpec(memory_space=pltpu.HBM)


def sds(shape, dtype):
    return jax.ShapeDtypeStruct(shape, dtype)


def dot(a, b):
    return jnp.dot(a, b, preferred_element_type=F32)


def gelu_both(g):
    g2 = g * g
    t = jnp.tanh(C0 * (g + C1 * (g2 * g)))
    cdf = 0.5 * (1.0 + t)
    slope = cdf + (0.5 * g) * (1.0 - t * t) * (C0 * (1.0 + (3.0 * C1) * g2))
    return g * cdf, slope


def places():
    h = lax.axis_index("hd")
    y = lax.axis_index("ff")
    c = lax.rem(h, 2)
    sib = h + 1 - 2 * c
    xn = lax.rem(h + 2, 4)
    xs = lax.rem(sib + 2, 4)
    return h, y, c, sib, xn, xs


def remote(src, dst, sems, k, dev):
    return pltpu.make_async_remote_copy(src_ref=src, dst_ref=dst, send_sem=sems[0].at[k], recv_sem=sems[1].at[k],
                                        device_id=dev, device_id_type=MESH)


def unit(j, q):
    u0, u1 = CH[j]
    return 4 * u0 + q * (u1 - u0)


def aligned(start, size, tile):
    return pl.ds(pl.multiple_of(start * tile, tile), size * tile)


GCH = ((0, 3), (3, 7), (7, 10))
HT = T // 2
NG = len(GCH)
NLS = 16
N_SEM = {"ud": 2 * NC, "ux": 2 * NC, "mx": 2 * NG, "md": 4 * NG, "gx": NG, "gd": NG, "gf": NG, "fy": 4, "st": 3}
SEM_NAMES = list(N_SEM)


def comm_kernel(x_hbm, w1_ref, b1_hbm, w2_ref, b2_hbm, gam_hbm, dy_hbm,
                m_ref, du_ref, d_ref, dr_ref, nrm_ref, db1_ref, dxp_ref,
                x_ref, b1_ref, b2_ref, gam_ref, dy_ref, w1b, w2b, ub, rb, xsb, xrb, fs, fr, stb, dmb, dmr, u_ref, dmf, pr_ref, acc,
                ls0, ls1, *sem_list):
    sems = {n: (sem_list[2 * i], sem_list[2 * i + 1]) for i, n in enumerate(SEM_NAMES)}
    h, y, c, sib, xn, xs = places()
    dev_sib, dev_x, dev_xs, dev_y = (0, y, sib), (0, y, xn), (0, y, xs), (0, 1 - y, h)
    order = [xs, xn, sib, h]

    load_order = []
    for j in range(NC + 1):
        load_order += [(j, k) for k in (0, 1) if j < NC] + [(j - 1, k) for k in (2, 3) if j > 0]

    def w1_load(j, k):
        u0, u1 = CH[j]
        n = u1 - u0
        return pltpu.make_async_copy(w1_ref.at[:, aligned(unit(j, order[k]), n, 256)], w1b.at[k, :, u0 * 256:u1 * 256],
                                     ls1.at[load_order.index((j, k)) % NLS])

    def w2_load(j):
        rows = slice(4 * 128 * CH[j][0], 4 * 128 * CH[j][1])
        return pltpu.make_async_copy(w2_ref.at[rows, :], w2b.at[rows, :], ls1.at[(4 * NC + j) % NLS])

    ins = [pltpu.make_async_copy(a, b, ls0.at[i]) for i, (a, b) in enumerate(
        ((x_hbm, x_ref), (b1_hbm, b1_ref), (b2_hbm, b2_ref), (gam_hbm, gam_ref), (dy_hbm, dy_ref)))]
    bar = pltpu.get_barrier_semaphore()
    for dev in (dev_sib, dev_x, dev_xs, dev_y):
        pl.semaphore_signal(bar, inc=1, device_id=dev, device_id_type=MESH)
    ins[0].start()
    for j, k in load_order[:6]:
        w1_load(j, k).start()
    loaded = [6]

    def load_more(n):
        for j, k in load_order[loaded[0]:loaded[0] + n]:
            w1_load(j, k).start()
        loaded[0] += n

    ins[0].wait()

    live = []

    def send(src, dst, name, k, dev):
        cp = remote(src, dst, sems[name], k, dev)
        cp.start()
        live.append(cp)
        return cp

    def sent(*cps):
        for cp in cps:
            cp.wait_send()
        live[:] = [cp for cp in live if not any(cp is old for old in cps)]

    def u_parts(*slabs):
        for j, k in slabs:
            w1_load(j, k).wait()
        load_more(4)
        for j, k in slabs:
            u0, u1 = CH[j]
            r = dot(x_ref[...], w1b[k, :, u0 * 256:u1 * 256]).astype(BF)
            for i in range(u1 - u0):
                ub[k, u0 + i] = r[:, i * 256:(i + 1) * 256]
        if slabs[0] == (0, 0):
            pl.semaphore_wait(bar, 4)
            for cp in ins[1:]:
                cp.start()
        for j, k in slabs:
            us = slice(*CH[j])
            if k == 0:
                c_ud[j, 1] = send(ub.at[0, us], rb.at[1, us], "ud", 2 * j + 1, dev_sib)
            if k == 2:
                c_ud[j, 0] = send(ub.at[2, us], rb.at[0, us], "ud", 2 * j, dev_sib)

    def s1(j):
        us = slice(*CH[j])
        c_ud[j, 1].wait_recv()
        xsb[us] = (ub[1, us].astype(F32) + rb[1, us].astype(F32)).astype(BF)
        send_x(0, j)

    def half(a):
        return slice(a * HT, (a + 1) * HT)

    def send_x(a, j):
        us = slice(*CH[j])
        c_ux[a, j] = send(xsb.at[us, half(a)], xrb.at[us, half(a)], "ux", a * NC + j, dev_x)

    def s2(a, j):
        rows = half(a)
        u0, u1 = CH[j]
        if a == 0:
            c_ud[j, 0].wait_recv()
        c_ux[a, j].wait_recv()
        for i in range(u1 - u0):
            n = u0 + i
            u = (ub[3, n, rows].astype(F32) + rb[0, n, rows].astype(F32) + xrb[n, rows].astype(F32)
                 + b1_ref[unit(j, h) + i])
            u = u.astype(BF)
            u_ref[h, n, rows] = u
            u = u.astype(F32)
            val, slope = gelu_both(u[:, PAIR:])
            m_ref[h, n, rows] = (u[:, :PAIR] * val).astype(BF)
            pr_ref[h, n, rows, :PAIR] = val
            pr_ref[h, n, rows, PAIR:] = u[:, :PAIR] * slope
        if j % 2 == 1:
            g = j // 2
            part = m_ref.at[h, slice(*GCH[g]), rows]
            c_mx[a, g] = send(part, part, "mx", a * NG + g, dev_x)
            c_md[a, g] = send(part, part, "md", a * NG + g, dev_sib)

    def s3(a, g):
        c_mx[a, g].wait_recv()
        part = m_ref.at[xn, slice(*GCH[g]), half(a)]
        c_mf[a, g] = send(part, part, "md", (2 + a) * NG + g, dev_sib)

    def s4(a, g):
        rows = half(a)
        c_md[a, g].wait_recv()
        c_mf[a, g].wait_recv()
        if a == 0:
            for j in (2 * g, 2 * g + 1):
                w2_load(j).wait()
        m = jnp.concatenate([m_ref[q, n, rows] for j in (2 * g, 2 * g + 1) for q in range(4) for n in range(*CH[j])], axis=1)
        u0, u1 = GCH[g]
        for n in range(2):
            cols = slice(n * 512, (n + 1) * 512)
            part = dot(m, w2b[4 * 128 * u0:4 * 128 * u1, cols])
            if g > 0:
                part = nrm_ref[rows, cols] + part
            if g < NG - 1:
                nrm_ref[rows, cols] = part
            else:
                fs[a, n] = part.astype(BF)
                c_fy[a, n] = send(fs.at[a, n], fr.at[a, n], "fy", 2 * a + n, dev_y)

    def gather_u(j):
        us = slice(*GCH[j])
        c_gx[j] = send(u_ref.at[h, us], u_ref.at[h, us], "gx", j, dev_x)
        c_gd[j] = send(u_ref.at[h, us], u_ref.at[h, us], "gd", j, dev_sib)

    def forward_u(j):
        us = slice(*GCH[j])
        c_gx[j].wait_recv()
        c_gf[j] = send(u_ref.at[xn, us], u_ref.at[xn, us], "gf", j, dev_sib)
        products(j, xn)

    def products(j, q):
        for a in range(*GCH[j]):
            u = u_ref[q, a].astype(F32)
            val, slope = gelu_both(u[:, PAIR:])
            pr_ref[q, a, :, :PAIR] = val
            pr_ref[q, a, :, PAIR:] = u[:, :PAIR] * slope

    def products_sib(j):
        c_gd[j].wait_recv()
        c_gf[j].wait_recv()
        products(j, sib)
        products(j, xs)

    c_ud, c_ux, c_mx, c_md, c_mf, c_fy, c_gx, c_gd, c_gf = {}, {}, {}, {}, {}, {}, {}, {}, {}
    u_parts((0, 0), (0, 1))
    u_parts((1, 0), (1, 1), (0, 2), (0, 3))
    s1(0)
    send_x(1, 0)
    u_parts((2, 0), (2, 1), (1, 2), (1, 3))
    s1(1)
    u_parts((3, 0), (3, 1), (2, 2), (2, 3))
    s1(2)
    for j in range(NC):
        w2_load(j).start()
    u_parts((4, 0), (4, 1), (3, 2), (3, 3))
    s1(3)
    send_x(1, 1)
    u_parts((5, 0), (5, 1), (4, 2), (4, 3))
    s1(4)
    u_parts((5, 2), (5, 3))
    s1(5)
    for j in range(2, NC):
        send_x(1, j)
    ins[1].wait()
    for a in range(2):
        for j in range(NC):
            s2(a, j)
    for g in range(NG - 1):
        gather_u(g)
    for a in range(2):
        s3(a, 0)
        s3(a, 1)
        s4(a, 0)
        s3(a, 2)
        s4(a, 1)
        s4(a, 2)
    for cp in ins[2:]:
        cp.wait()

    gdy = dy_ref[...].astype(F32) * gam_ref[...]
    sg = jnp.sum(gdy, axis=1, keepdims=True)
    dr_ref[...] = gdy
    for n in range(2):
        cols = slice(n * 512, (n + 1) * 512)
        nrm_ref[:, cols] = ALPHA * x_ref[:, cols].astype(F32) + b2_ref[:, cols]
    forward_u(0)
    lane = lax.broadcasted_iota(jnp.int32, (HT, 128), 1)
    packs = []
    for a in range(2):
        rows = half(a)
        for n in range(2):
            cols = slice(n * 512, (n + 1) * 512)
            c_fy[a, n].wait_recv()
            nrm_ref[rows, cols] = nrm_ref[rows, cols] + (fs[a, n].astype(F32) + fr[a, n].astype(F32))
        r = nrm_ref[rows, :]
        m_loc = jnp.sum(r, axis=1, keepdims=True) * (1.0 / H)
        cen = r - m_loc
        m2 = jnp.sum(cen * cen, axis=1, keepdims=True)
        cg = jnp.sum(dr_ref[rows, :] * cen, axis=1, keepdims=True)
        packs.append(jnp.where(lane == 0, m_loc, jnp.where(lane == 1, m2, jnp.where(lane == 2, sg[rows], cg))))
    pack = jnp.concatenate(packs, axis=0)
    stb[h] = pack.T[0:8]
    c_st = [send(stb.at[h], stb.at[h], "st", i, dev) for i, dev in enumerate((dev_sib, dev_x, dev_xs))]
    gather_u(NG - 1)
    products_sib(0)
    for cp in c_st:
        cp.wait_recv()
    st = [stb[i] for i in range(4)]
    mu = ((st[0][0:1] + st[1][0:1]) + (st[2][0:1] + st[3][0:1])) * 0.25
    m2t = jnp.zeros_like(mu)
    sgt = jnp.zeros_like(mu)
    cgt = jnp.zeros_like(mu)
    for i in range(4):
        delta = st[i][0:1] - mu
        m2t += st[i][1:2] + (H * delta) * delta
        sgt += st[i][2:3]
        cgt += st[i][3:4] + delta * st[i][2:3]
    rho = lax.rsqrt(m2t * (1.0 / (4 * H)) + LN_EPS)
    rows = jnp.concatenate([mu, rho, sgt * (1.0 / (4 * H)), cgt * rho * (1.0 / (4 * H)), jnp.zeros((124, T), F32)], axis=0)
    colst = rows.T
    mu_c, rho_c, mg_c, mgr_c = (colst[:, i:i + 1] for i in range(4))
    r = nrm_ref[...]
    gdy = dr_ref[...]
    nrm = (r - mu_c) * rho_c
    dr = rho_c * (gdy - mg_c - nrm * mgr_c)
    nrm_ref[...] = nrm
    dr_ref[...] = dr
    d_ref[...] = dr.astype(BF)
    d_t = dr.T.astype(BF)

    c_dd, c_dx, c_df = {}, {}, {}
    mine, mine_k, theirs, theirs_k = (h, xn), (3, 1), (sib, xs), (2, 0)

    def dm_part(j):
        u0, u1 = CH[j]
        n = u1 - u0
        for i, q in enumerate(theirs + mine):
            r = dot(w2b[aligned(unit(j, q), n, 128), :], d_t).astype(BF).T
            for a in range(n):
                dmb[i, u0 + a] = r[:, a * 128:(a + 1) * 128]
            if i == 1:
                sent(c_ud[j, 0], c_ud[j, 1])
                for k in range(2):
                    c_dd[j, k] = send(dmb.at[k, u0:u1], dmr.at[k, u0:u1], "ud", 2 * j + k, dev_sib)

    def dm_sum(j):
        us = slice(*CH[j])
        sent(c_ux[0, j], c_ux[1, j])
        for i in range(2):
            c_dd[j, i].wait_recv()
            xsb[us, :, i * 128:(i + 1) * 128] = (dmb[2 + i, us].astype(F32) + dmr[i, us].astype(F32)).astype(BF)
        c_dx[j] = send(xsb.at[us], xrb.at[us], "ux", j, dev_x)

    def dm_full(j):
        us = slice(*CH[j])
        c_dx[j].wait_recv()
        if j == 0:
            sent(*c_md.values(), *c_mf.values())
        for i in range(2):
            q = mine[i]
            dmf[q, us] = (xsb[us, :, i * 128:(i + 1) * 128].astype(F32)
                          + xrb[us, :, (1 - i) * 128:(2 - i) * 128].astype(F32)).astype(BF)
        for i in range(2):
            q = mine[i]
            c_df[j, i] = send(dmf.at[q, us], dmf.at[q, us], "md", 2 * j + i, dev_sib)

    def grads(j, qs, ks, first):
        u0, u1 = CH[j]
        total = None
        dus = []
        for q in qs:
            parts = []
            for a in range(u0, u1):
                dm = dmf[q, a].astype(F32)
                du_f = pr_ref[q, a] * jnp.concatenate([dm, dm], axis=1)
                db1_ref[unit(j, q) + a - u0] = jnp.sum(du_f, axis=0, keepdims=True)
                du = du_f.astype(BF)
                du_ref[q, a] = du
                parts.append(du)
            dus.append(jnp.concatenate(parts, axis=1).T)
        for du_t, k in zip(dus, ks):
            part = dot(w1b[k, :, u0 * 256:u1 * 256], du_t)
            total = part if total is None else total + part
        acc[...] = total if first else acc[...] + total

    def grads_mine(j):
        grads(j, mine, mine_k, j == 0)

    def grads_theirs(j):
        for i in range(2):
            c_df[j, i].wait_recv()
        grads(j, theirs, theirs_k, False)

    dm_part(0)
    dm_part(1)
    dm_sum(0)
    forward_u(1)
    dm_part(2)
    dm_sum(1)
    products_sib(1)
    dm_part(3)
    dm_sum(2)
    dm_part(4)
    dm_sum(3)
    forward_u(2)
    dm_part(5)
    dm_sum(4)
    dm_sum(5)
    dm_full(0)
    grads_mine(0)
    for j in range(1, NC):
        if j == NC - 1:
            dm_full(j)
        grads_theirs(j - 1)
        if j < NC - 1:
            dm_full(j)
        grads_mine(j)
        if j == 3:
            products_sib(2)
    grads_theirs(NC - 1)
    dxp_ref[...] = acc[...].T.astype(BF)
    for cp in live:
        cp.wait_send()


def comm_call(x, w1, b1, w2, b2, gam, dy):
    scratch = [pltpu.VMEM((T, H), BF), pltpu.VMEM((4 * NU, 1, 256), F32), pltpu.VMEM((1, H), F32), pltpu.VMEM((1, H), F32),
               pltpu.VMEM((T, H), BF),
               pltpu.VMEM((4, H, NU * 256), BF), pltpu.VMEM((4 * NU * 128, H), BF),
               pltpu.VMEM((4, NU, T, 256), BF), pltpu.VMEM((2, NU, T, 256), BF),
               pltpu.VMEM((NU, T, 256), BF), pltpu.VMEM((NU, T, 256), BF),
               pltpu.VMEM((2, 2, HT, 512), BF), pltpu.VMEM((2, 2, HT, 512), BF),
               pltpu.VMEM((4, 8, T), F32),
               pltpu.VMEM((4, NU, T, 128), BF), pltpu.VMEM((2, NU, T, 128), BF),
               pltpu.VMEM((4, NU, T, 256), BF), pltpu.VMEM((4, NU, T, 128), BF), pltpu.VMEM((4, NU, T, 256), F32),
               pltpu.VMEM((H, T), F32),
               pltpu.SemaphoreType.DMA((5,)), pltpu.SemaphoreType.DMA((NLS,))]
    for n in SEM_NAMES:
        scratch += [pltpu.SemaphoreType.DMA((N_SEM[n],)), pltpu.SemaphoreType.DMA((N_SEM[n],))]
    outs = [sds((4, NU, T, 128), BF), sds((4, NU, T, 256), BF), sds((T, H), BF), sds((T, H), F32), sds((T, H), F32),
            sds((4 * NU, 1, 256), F32), sds((T, H), BF)]
    return pl.pallas_call(
        comm_kernel, out_shape=outs, name="comm",
        in_specs=[HBM] * 7, out_specs=[VMEM] * 7, scratch_shapes=scratch,
        compiler_params=pltpu.CompilerParams(collective_id=0, has_side_effects=True, vmem_limit_bytes=COMM_LIM),
        cost_estimate=pl.CostEstimate(flops=8 * 10 ** 9, bytes_accessed=32 << 20, transcendentals=0),
    )(x, w1, b1, w2, b2, gam, dy)


NB2 = 8
NB1 = 8


def grads_kernel(m_ref, du_ref, d_ref, nrm_ref, dr_ref, db1_in, x_ref, gam_ref, beta_ref, dy_ref,
                 dw1_ref, dw2_ref, y_ref, db1_ref, db2_ref, dgam_ref, dbeta_ref,
                 ob2, ob1, xt, yb, db1b, sb, so2, so1, so0):
    tiles = [(j, q) for j in range(NC) for q in range(4)]

    def put2(t):
        j, q = tiles[t]
        n = CH[j][1] - CH[j][0]
        r0 = unit(j, q) * 128
        return pltpu.make_async_copy(ob2.at[t % NB2, :n * 128], dw2_ref.at[r0:r0 + n * 128, :], so2.at[t % NB2])

    def put1(t):
        j, q = tiles[t]
        n = CH[j][1] - CH[j][0]
        c0 = unit(j, q) * 256
        return pltpu.make_async_copy(ob1.at[t % NB1, :, :n * 256], dw1_ref.at[:, c0:c0 + n * 256], so1.at[t % NB1])

    small = [pltpu.make_async_copy(a, b, so0.at[i]) for i, (a, b) in enumerate(
        ((yb, y_ref), (db1b, db1_ref), (sb.at[0], db2_ref), (sb.at[1], dgam_ref), (sb.at[2], dbeta_ref)))]
    for t, (j, q) in enumerate(tiles):
        if t >= NB2:
            put2(t - NB2).wait()
        for i, a in enumerate(range(*CH[j])):
            ob2[t % NB2, i * 128:(i + 1) * 128] = dot(m_ref[q, a].T, d_ref[...])
        put2(t).start()
        if t == 6:
            xt[...] = x_ref[...].T
        if t == 8:
            yb[...] = (gam_ref[...] * nrm_ref[...] + beta_ref[...]).astype(BF)
            for i in range(4 * NU):
                db1b[:, i * 256:(i + 1) * 256] = db1_in[i]
            for cp in small[:2]:
                cp.start()
        if t == 10:
            dy = dy_ref[...].astype(F32)
            sb[0] = jnp.sum(dr_ref[...], axis=0, keepdims=True)
            sb[1] = jnp.sum(dy * nrm_ref[...], axis=0, keepdims=True)
            sb[2] = jnp.sum(dy, axis=0, keepdims=True)
            for cp in small[2:]:
                cp.start()
    for t, (j, q) in enumerate(tiles):
        if t >= NB1:
            put1(t - NB1).wait()
        for i, a in enumerate(range(*CH[j])):
            ob1[t % NB1, :, i * 256:(i + 1) * 256] = dot(xt[...], du_ref[q, a])
        put1(t).start()
    last = len(tiles)
    for t in range(last - NB2, last):
        put2(t).wait()
    for cp in small:
        cp.wait()
    for t in range(last - NB1, last):
        put1(t).wait()


def grads_call(m, du, d, nrm, dr, db1, x, gam, beta, dy):
    outs = [sds((H, 4 * NU * 256), F32), sds((4 * NU * 128, H), F32), sds((T, H), BF), sds((1, 4 * NU * 256), F32),
            sds((1, H), F32), sds((1, H), F32), sds((1, H), F32)]
    return pl.pallas_call(
        grads_kernel, out_shape=outs, name="grads",
        in_specs=[VMEM] * 10, out_specs=[HBM] * 7,
        scratch_shapes=[pltpu.VMEM((NB2, 256, H), F32), pltpu.VMEM((NB1, H, 512), F32), pltpu.VMEM((H, T), BF),
                        pltpu.VMEM((T, H), BF), pltpu.VMEM((1, 4 * NU * 256), F32), pltpu.VMEM((3, 1, H), F32),
                        pltpu.SemaphoreType.DMA((NB2,)), pltpu.SemaphoreType.DMA((NB1,)), pltpu.SemaphoreType.DMA((5,))],
        compiler_params=pltpu.CompilerParams(vmem_limit_bytes=GRADS_LIM),
        cost_estimate=pl.CostEstimate(flops=4 * 10 ** 9, bytes_accessed=66 << 20, transcendentals=0),
    )(m, du, d, nrm, dr, db1, x, gam, beta, dy)


def solution(mesh):
    data_spec = P('dp', 'hd')
    hid_spec = P('hd')
    in_specs = (data_spec, P('hd', 'ff'), P('ff'), P('ff', 'hd'), hid_spec, hid_spec, hid_spec, data_spec)
    out_specs = (data_spec, data_spec, P(('dp', 'hd'), 'ff'), P(('dp', 'ff'), 'hd'), P(('dp', 'ff')), P(('dp', 'hd')), P(('dp', 'hd')), P(('dp', 'hd')))

    def device_step(x, w1, b1, w2, b2, gam, beta, dy):
        b2, gam, beta = (a.reshape(1, H) for a in (b2, gam, beta))
        hbm = [pltpu.with_memory_space_constraint(a, pltpu.HBM) for a in (x, w1, b1.reshape(4 * NU, 1, 256), w2, b2, gam, dy)]
        m, du, d, dr, nrm, db1, dxp = comm_call(*hbm)
        dxr = lax.ppermute(dxp, 'ff', [(0, 1), (1, 0)])
        dw1, dw2, y, db1, db2, dgam, dbeta = grads_call(m, du, d, nrm, dr, db1, x, gam, beta, dy)
        dx = (ALPHA * dr + (dxp.astype(F32) + dxr.astype(F32))).astype(BF)
        return y, dx, dw1, dw2, db1.reshape(-1), db2.reshape(-1), dgam.reshape(-1), dbeta.reshape(-1)

    return jax.shard_map(device_step, mesh=mesh, in_specs=in_specs, out_specs=out_specs, check_vma=False)
```
